32 devices in a mesh: seq: 4 (over z), tensor: 2 (over y), fsdp: 4 (over x, core).
Axes of the slice: x: 2, y: 2, z: 4, core: 2. Of those that a mesh axis runs over, the one named last changes fastest.
Arguments:
- hidden_in: bfloat16 [2048, 2048], P(('seq', 'fsdp'), 'tensor'), may hold values from -12 to 12
- out_cotangent: bfloat16 [2048, 2048], P(('seq', 'fsdp'), 'tensor'), may hold values from -6 to 6
- attn_norm_gain: float32 [2048], replicated, may hold values from 0.1 to 1.9
- attn_norm_bias: float32 [2048], replicated, may hold values from -3 to 3
- mlp_norm_gain: float32 [2048], replicated, may hold values from 0.1 to 1.9
- mlp_norm_bias: float32 [2048], replicated, may hold values from -3 to 3
- qkv_weight: bfloat16 [2048, 6144], P(('seq', 'fsdp'), 'tensor'), as said below
- qkv_bias: float32 [6144], P('tensor'), may hold values from -0.6 to 0.6
- proj_weight: bfloat16 [2048, 2048], P(('seq', 'fsdp'), 'tensor'), may hold values from -1.5 to 1.5
- proj_bias: float32 [2048], P('tensor'), may hold values from -3 to 3
- up_weight: bfloat16 [2048, 8192], P(('seq', 'fsdp'), 'tensor'), may hold values from -0.125 to 0.125
- up_bias: float32 [8192], P('tensor'), may hold values from -3 to 3
- down_weight: bfloat16 [2048, 8192], P(('seq', 'fsdp'), 'tensor'), may hold values from -0.0625 to 0.0625
- down_bias: float32 [2048], P('tensor'), may hold values from -3 to 3
Outputs:
- hidden_out: bfloat16 [2048, 2048], P(('seq', 'fsdp'), 'tensor')
- input_grad: bfloat16 [2048, 2048], P(('seq', 'fsdp'), 'tensor')
- attn_gain_grad: float32 [2048], replicated
- attn_bias_grad: float32 [2048], replicated
- mlp_gain_grad: float32 [2048], replicated
- mlp_bias_grad: float32 [2048], replicated
- qkv_weight_grad: float32 [2048, 6144], P(('seq', 'fsdp'), 'tensor')
- qkv_bias_grad: float32 [6144], P('tensor')
- proj_weight_grad: float32 [2048, 2048], P(('seq', 'fsdp'), 'tensor')
- proj_bias_grad: float32 [2048], P('tensor')
- up_weight_grad: float32 [2048, 8192], P(('seq', 'fsdp'), 'tensor')
- up_bias_grad: float32 [8192], P('tensor')
- down_weight_grad: float32 [2048, 8192], P(('seq', 'fsdp'), 'tensor')
- down_bias_grad: float32 [2048], P('tensor')
The draws below stay inside these ranges and needn't reach their ends.
Inputs may be any that keep to these rules, and one draw needn't show every extreme that they name: `qkv_weight`: columns laid out as qkv in the reference program.
All inputs are finite; a program needn't handle non-finite values.
Results may differ from the reference program's by a relative error of at most 0.013.
Values may be sent and summed in bfloat16 or wider, within the bound.
A program may use at most 256 MiB of HBM per device.

```python
import math
import jax
import jax.numpy as jnp
from jax import lax

D = 2048
HEADS = 8
HEAD_DIM = 256
ROT = 64
FF = 8192
SEQ_LEN = 2048


def draw_hidden_in(key, part):
    key_base, key_rows, key_cols = jax.random.split(key, 3)
    row_scale = jnp.exp(jax.random.uniform(key_rows, (SEQ_LEN, 1), jnp.float32, math.log(0.2), math.log(2.0)))
    col_scale = jnp.exp(jax.random.uniform(key_cols, (1, D), jnp.float32, math.log(0.2), math.log(2.0)))
    base_draw = jax.random.truncated_normal(key_base, -3.0, 3.0, (SEQ_LEN, D), jnp.float32)
    values = base_draw * row_scale * col_scale
    return values.astype(jnp.bfloat16)


def draw_qkv_weight(key, part):
    values = jax.random.truncated_normal(key, -4.0, 4.0, (D, 3 * D), jnp.float32) * D ** (-0.5)
    return values.astype(jnp.bfloat16)


def with_spikes(drawn, own_key, source, target, shards_of, factor):
    owner, partner = [(jnp.arange(drawn.shape[dim]) // (drawn.shape[dim] // shards_of)).reshape([-1 if axis == dim else 1 for axis in range(drawn.ndim)]) for dim in (source, target)]
    chosen = jax.random.permutation(own_key, shards_of)[partner]
    strong = (owner == chosen) | (owner == (partner + shards_of // 2) % shards_of)
    return jnp.where(strong, factor * drawn, drawn)


def levels(key, dims, shards, low, top_value):
    factor_of = 1.0
    for dim, shards_of in shards:
        draws = jax.random.uniform(jax.random.fold_in(jax.random.fold_in(key, 6), dim), (shards_of,), jnp.float32, low / len(shards), top_value / len(shards))
        factor_of = factor_of * jnp.repeat(jnp.exp(draws), dims[dim] // shards_of).reshape((-1,) + (1,) * (len(dims) - 1 - dim))
    return factor_of


def gaussian(key, shape, spread, limit, pieces=(), held_as=jnp.bfloat16):
    entries = jax.random.normal(key, shape, jnp.float32) * spread
    if len(pieces) > 0:
        entries = levels(key, shape, pieces, -0.22, 0.18) * entries
    return jnp.clip(entries, min=-limit, max=limit).astype(held_as)


def gaussian_with(own_key, dims, deviation, reach, pieces, heavy, kind=jnp.bfloat16):
    values = deviation * jax.random.normal(own_key, dims, jnp.float32)
    if pieces:
        values = values * levels(own_key, dims, pieces, -0.22, 0.18)
    return jnp.clip(with_spikes(values, jax.random.fold_in(own_key, 3), *heavy), -reach, reach).astype(kind)


def setup_inputs(seed: int = 0) -> dict:
    key_list = jax.random.split(jax.random.key(seed), 15)
    hidden_in = draw_hidden_in(jax.random.fold_in(key_list[14], 71), 0)
    out_cotangent = gaussian_with(key_list[1], (SEQ_LEN, D), 1.0, 6.0, ((0, 16), (1, 2)), (0, 1, 16, 2.0))
    attn_norm_gain = jnp.clip(1.0 + 0.18 * jax.random.normal(key_list[2], (D,), jnp.float32), 0.1, 1.9)
    attn_norm_bias = gaussian(key_list[3], (D,), 0.5, 3.0, (), jnp.float32)
    mlp_norm_gain = jnp.clip(1.0 + 0.18 * jax.random.normal(key_list[4], (D,), jnp.float32), 0.1, 1.9)
    mlp_norm_bias = gaussian(key_list[5], (D,), 0.5, 3.0, (), jnp.float32)
    qkv_weight = draw_qkv_weight(jax.random.fold_in(key_list[14], 71), 0)
    qkv_bias = gaussian(key_list[7], (3 * D,), 0.1, 0.6, ((0, 2),), jnp.float32)
    proj_weight = gaussian(key_list[8], (D, D), (max(D // 128, 1)) ** -0.5, 1.5, ((0, 16), (1, 2)))
    proj_bias = gaussian(key_list[9], (D,), 0.5, 3.0, ((0, 2),), jnp.float32)
    up_weight = gaussian(key_list[10], (D, FF), D ** -0.5, 0.125, ((0, 16), (1, 2)))
    up_bias = gaussian(key_list[11], (FF,), 0.5, 3.0, ((0, 2),), jnp.float32)
    down_weight = gaussian(key_list[12], (D, FF), FF ** -0.5, 0.0625, ((0, 16), (1, 2)))
    down_bias = gaussian(key_list[13], (D,), 0.5, 3.0, ((0, 2),), jnp.float32)
    return dict(hidden_in=hidden_in, out_cotangent=out_cotangent, attn_norm_gain=attn_norm_gain, attn_norm_bias=attn_norm_bias, mlp_norm_gain=mlp_norm_gain, mlp_norm_bias=mlp_norm_bias, qkv_weight=qkv_weight, qkv_bias=qkv_bias, proj_weight=proj_weight, proj_bias=proj_bias, up_weight=up_weight, up_bias=up_bias, down_weight=down_weight, down_bias=down_bias)


norm_eps = 1e-05
rope_base = 10000.0

def gelu_value(pre_act):
    return 0.5 * pre_act * (1.0 + lax.erf(pre_act * 0.7071067811865476))

def gelu_slope(pre_act):
    return 0.5 * (1.0 + lax.erf(pre_act * 0.7071067811865476)) + pre_act * jnp.exp(-0.5 * pre_act * pre_act) * 0.3989422804014327

def layer_norm_parts(row_values):
    centered = row_values - lax.optimization_barrier(jnp.mean(row_values, axis=-1, keepdims=True))
    inv_std = lax.rsqrt(lax.optimization_barrier(jnp.mean(centered * centered, axis=-1, keepdims=True)) + norm_eps)
    return (centered * inv_std, inv_std)

def rotary_tables(positions):
    half_rot = ROT // 2
    exponent = jnp.arange(half_rot, dtype=jnp.float32) * (2.0 / ROT)
    frequency = jnp.exp(-exponent * math.log(rope_base))
    angles = positions.astype(jnp.float32)[:, None] * frequency[None, :]
    return (jnp.cos(angles), jnp.sin(angles))

def rotate_heads(values, cosine_table, sine_table):
    half_rot = ROT // 2
    first_half = values[..., :half_rot]
    second_half = values[..., half_rot:ROT]
    cos_part = cosine_table[:, None, :]
    sin_part = sine_table[:, None, :]
    return jnp.concatenate([first_half * cos_part - second_half * sin_part, second_half * cos_part + first_half * sin_part, values[..., ROT:]], axis=-1)

def heads_first(stacked):
    return jnp.transpose(stacked, (1, 0, 2))

def reference(hidden_in, out_cotangent, attn_norm_gain, attn_norm_bias, mlp_norm_gain, mlp_norm_bias, qkv_weight, qkv_bias, proj_weight, proj_bias, up_weight, up_bias, down_weight, down_bias):
    seq_len = hidden_in.shape[0]
    score_scale = HEAD_DIM ** (-0.5)
    float_rows = hidden_in.astype(jnp.float32)
    normal_rows, inv_std = layer_norm_parts(float_rows)
    attn_in = (normal_rows * attn_norm_gain + attn_norm_bias).astype(jnp.bfloat16)
    mlp_in = (normal_rows * mlp_norm_gain + mlp_norm_bias).astype(jnp.bfloat16)
    qkv_rows = jnp.dot(attn_in, qkv_weight, preferred_element_type=jnp.float32) + qkv_bias
    qkv_rows = qkv_rows.reshape(seq_len, HEADS, 3, HEAD_DIM)
    positions = jnp.arange(seq_len, dtype=jnp.int32)
    cosine_table, sine_table = rotary_tables(positions)
    queries = rotate_heads(qkv_rows[:, :, 0], cosine_table, sine_table).astype(jnp.bfloat16)
    keys_all = rotate_heads(qkv_rows[:, :, 1], cosine_table, sine_table).astype(jnp.bfloat16)
    values_all = qkv_rows[:, :, 2].astype(jnp.bfloat16)
    query_block = math.gcd(seq_len, 1024)
    block_numbers = jnp.arange(seq_len // query_block, dtype=jnp.int32)

    def block_scores(head_query, head_key, start_row):
        query_rows = lax.dynamic_slice_in_dim(head_query, start_row, query_block, 0)
        scores = jnp.dot(query_rows, head_key.T, preferred_element_type=jnp.float32) * score_scale
        query_pos = start_row + jnp.arange(query_block, dtype=jnp.int32)
        allowed = positions[None, :] <= query_pos[:, None]
        return (query_rows, jnp.where(allowed, scores, -1e+30), allowed)

    def head_forward(operands):
        head_query, head_key, head_value = operands

        def block_forward(block_number):
            start_row = block_number * query_block
            ignored, scores, allowed = block_scores(head_query, head_key, start_row)
            row_max = lax.optimization_barrier(jnp.max(scores, axis=-1))
            exp_terms = jnp.where(allowed, jnp.exp(scores - row_max[:, None]), 0.0)
            row_total = lax.optimization_barrier(jnp.sum(exp_terms, axis=-1))
            mixed_rows = jnp.dot(exp_terms.astype(jnp.bfloat16), head_value, preferred_element_type=jnp.float32) / row_total[:, None]
            return (mixed_rows.astype(jnp.bfloat16), row_max + jnp.log(row_total))
        mixed_rows, log_total = lax.map(block_forward, block_numbers)
        return (mixed_rows.reshape(seq_len, HEAD_DIM), log_total.reshape(seq_len))

    def head_backward(operands):
        head_query, head_key, head_value, head_out, head_grad_out, head_log_total = operands
        row_delta = lax.optimization_barrier(jnp.sum(head_grad_out.astype(jnp.float32) * head_out.astype(jnp.float32), axis=-1))

        def block_backward(running, block_number):
            key_acc, value_acc = running
            start_row = block_number * query_block
            query_rows, scores, allowed = block_scores(head_query, head_key, start_row)
            grad_rows = lax.dynamic_slice_in_dim(head_grad_out, start_row, query_block, 0)
            lse_rows = lax.dynamic_slice_in_dim(head_log_total, start_row, query_block, 0)
            delta_rows = lax.dynamic_slice_in_dim(row_delta, start_row, query_block, 0)
            prob_weights = jnp.where(allowed, jnp.exp(scores - lse_rows[:, None]), 0.0)
            prob_grad = jnp.dot(grad_rows, head_value.T, preferred_element_type=jnp.float32)
            score_grad = (prob_weights * (prob_grad - delta_rows[:, None])).astype(jnp.bfloat16)
            query_grad = jnp.dot(score_grad, head_key, preferred_element_type=jnp.float32) * score_scale
            key_acc = key_acc + jnp.dot(score_grad.T, query_rows, preferred_element_type=jnp.float32)
            value_acc = value_acc + jnp.dot(prob_weights.astype(jnp.bfloat16).T, grad_rows, preferred_element_type=jnp.float32)
            return ((key_acc, value_acc), query_grad)
        zero_block = jnp.zeros((seq_len, HEAD_DIM), jnp.float32)
        (key_acc, value_acc), query_grads = lax.scan(block_backward, (zero_block, zero_block), block_numbers)
        return (query_grads.reshape(seq_len, HEAD_DIM), key_acc * score_scale, value_acc)
    head_queries = heads_first(queries)
    head_keys = heads_first(keys_all)
    head_values = heads_first(values_all)
    attn_heads, log_totals = lax.map(head_forward, (head_queries, head_keys, head_values))
    attn_rows = heads_first(attn_heads).reshape(seq_len, D)
    attn_branch = jnp.dot(attn_rows, proj_weight.T, preferred_element_type=jnp.float32)
    token_block = math.gcd(seq_len, 4096)
    token_numbers = jnp.arange(seq_len // token_block, dtype=jnp.int32)

    def mlp_block(running, block_number):
        up_acc, down_acc, bias_acc = running
        start_row = block_number * token_block
        inputs_block = lax.dynamic_slice_in_dim(mlp_in, start_row, token_block, 0)
        grads_block = lax.dynamic_slice_in_dim(out_cotangent, start_row, token_block, 0)
        up_rows = jnp.dot(inputs_block, up_weight, preferred_element_type=jnp.float32) + up_bias
        active = gelu_value(up_rows).astype(jnp.bfloat16)
        mlp_rows = jnp.dot(active, down_weight.T, preferred_element_type=jnp.float32)
        pre_grad = jnp.dot(grads_block, down_weight, preferred_element_type=jnp.float32) * gelu_slope(up_rows)
        pre_rounded = pre_grad.astype(jnp.bfloat16)
        up_acc = up_acc + jnp.dot(inputs_block.T, pre_rounded, preferred_element_type=jnp.float32)
        down_acc = down_acc + jnp.dot(grads_block.T, active, preferred_element_type=jnp.float32)
        bias_acc = bias_acc + lax.optimization_barrier(jnp.sum(pre_grad, axis=0))
        block_in_grad = jnp.dot(pre_rounded, up_weight.T, preferred_element_type=jnp.float32)
        return ((up_acc, down_acc, bias_acc), (mlp_rows, block_in_grad))
    zero_weight = jnp.zeros((D, FF), jnp.float32)
    (up_weight_grad, down_weight_grad, up_bias_grad), (mlp_rows, mlp_in_grad) = lax.scan(mlp_block, (zero_weight, zero_weight, jnp.zeros((FF,), jnp.float32)), token_numbers)
    mlp_rows = mlp_rows.reshape(seq_len, D)
    mlp_in_grad = mlp_in_grad.reshape(seq_len, D)
    hidden_out = (float_rows + attn_branch + mlp_rows + proj_bias + down_bias).astype(jnp.bfloat16)
    grad_float = out_cotangent.astype(jnp.float32)
    proj_bias_grad = lax.optimization_barrier(jnp.sum(grad_float, axis=0))
    down_bias_grad = lax.optimization_barrier(jnp.sum(grad_float, axis=0))
    proj_weight_grad = jnp.dot(out_cotangent.T, attn_rows, preferred_element_type=jnp.float32)
    head_grad = jnp.dot(out_cotangent, proj_weight, preferred_element_type=jnp.float32).astype(jnp.bfloat16)
    head_grads = heads_first(head_grad.reshape(seq_len, HEADS, HEAD_DIM))
    query_grads, key_grads, value_grads = lax.map(head_backward, (head_queries, head_keys, head_values, attn_heads, head_grads, log_totals))
    query_grads = rotate_heads(heads_first(query_grads), cosine_table, -sine_table)
    key_grads = rotate_heads(heads_first(key_grads), cosine_table, -sine_table)
    token_grads = jnp.stack([query_grads, key_grads, heads_first(value_grads)], axis=2).astype(jnp.bfloat16).reshape(seq_len, 3 * D)
    qkv_bias_grad = lax.optimization_barrier(jnp.sum(token_grads.astype(jnp.float32), axis=0))
    qkv_weight_grad = jnp.dot(attn_in.T, token_grads, preferred_element_type=jnp.float32)
    attn_in_grad = jnp.dot(token_grads, qkv_weight.T, preferred_element_type=jnp.float32)
    attn_gain_grad = lax.optimization_barrier(jnp.sum(attn_in_grad * normal_rows, axis=0))
    attn_bias_grad = lax.optimization_barrier(jnp.sum(attn_in_grad, axis=0))
    mlp_gain_grad = lax.optimization_barrier(jnp.sum(mlp_in_grad * normal_rows, axis=0))
    mlp_bias_grad = lax.optimization_barrier(jnp.sum(mlp_in_grad, axis=0))
    spread_grad = attn_in_grad * attn_norm_gain + mlp_in_grad * mlp_norm_gain
    mean_grad = lax.optimization_barrier(jnp.mean(spread_grad, axis=-1, keepdims=True))
    mean_proj = lax.optimization_barrier(jnp.mean(spread_grad * normal_rows, axis=-1, keepdims=True))
    input_grad = (grad_float + inv_std * (spread_grad - mean_grad - normal_rows * mean_proj)).astype(jnp.bfloat16)
    return (hidden_out, input_grad, attn_gain_grad, attn_bias_grad, mlp_gain_grad, mlp_bias_grad, qkv_weight_grad, qkv_bias_grad, proj_weight_grad, proj_bias_grad, up_weight_grad, up_bias_grad, down_weight_grad, down_bias_grad)
```

```python
import math

import jax
import jax.numpy as jnp
from jax import lax
from jax.sharding import PartitionSpec as P

HEAD_DIM = 256
ROT = 64

norm_eps = 1e-05
rope_base = 10000.0


def gelu_parts(pre_act):
    cdf = 0.5 * (1.0 + lax.erf(pre_act * 0.7071067811865476))
    slope = cdf + pre_act * jnp.exp(-0.5 * pre_act * pre_act) * 0.3989422804014327
    return (pre_act * cdf, slope)


def rotary_tables(positions):
    half_rot = ROT // 2
    exponent = jnp.arange(half_rot, dtype=jnp.float32) * (2.0 / ROT)
    frequency = jnp.exp(-exponent * math.log(rope_base))
    angles = positions.astype(jnp.float32)[:, None] * frequency[None, :]
    return (jnp.cos(angles), jnp.sin(angles))


def rotate(values, cos_part, sin_part):
    half_rot = ROT // 2
    first_half = values[:, :half_rot]
    second_half = values[:, half_rot:ROT]
    return jnp.concatenate(
        [
            first_half * cos_part - second_half * sin_part,
            second_half * cos_part + first_half * sin_part,
            values[:, ROT:],
        ],
        axis=-1,
    )


def mm(left, right, left_dim, right_dim):
    return lax.dot_general(
        left, right, (((left_dim,), (right_dim,)), ((), ())), preferred_element_type=jnp.float32
    )


def swap(value, axis, bits):
    size = lax.axis_size(axis)
    return lax.ppermute(value, axis, [(i, i ^ bits) for i in range(size)])


def bits_of(size):
    return [1 << b for b in range(size.bit_length() - 1)]


def gather_blocks(block, axis):
    blocks = [block]
    for bit in reversed(bits_of(lax.axis_size(axis))):
        blocks = blocks + [swap(b, axis, bit) for b in blocks]
    return blocks


def gather_order(size):
    order = [0]
    for bit in reversed(bits_of(size)):
        order = order + [j | bit for j in order]
    return order


def bf(value):
    return value.astype(jnp.bfloat16)


def f32(value):
    return value.astype(jnp.float32)


def per_device(
    hidden_in,
    out_cotangent,
    attn_norm_gain,
    attn_norm_bias,
    mlp_norm_gain,
    mlp_norm_bias,
    qkv_weight,
    qkv_bias,
    proj_weight,
    proj_bias,
    up_weight,
    up_bias,
    down_weight,
    down_bias,
):
    S = lax.axis_size("seq")
    T = lax.axis_size("tensor")
    F = lax.axis_size("fsdp")
    z = lax.axis_index("seq")
    y = lax.axis_index("tensor")
    f = lax.axis_index("fsdp")
    tok, width = hidden_in.shape
    D = width * T
    rows = qkv_weight.shape[0]
    ntok = S * tok
    scale = HEAD_DIM ** (-0.5)
    order = gather_order(F)
    tensor_order = gather_order(T)

    per_half = S // T
    block_from = []
    for j in order:
        for k in range(S):
            zd = z ^ k
            half = (zd // per_half) ^ y
            block_from.append((half * per_half + zd % per_half) * F + (f ^ j))
    place = {j: p for p, j in enumerate(order)}
    place_table = jnp.array([place[j] for j in range(F)], jnp.int32)
    block_to = []
    for i in range(T):
        for zl in range(per_half):
            for fd in range(F):
                zd = (y ^ tensor_order[i]) * per_half + zl
                block_to.append(place_table[f ^ fd] * S + (zd ^ z))

    def shuffle(value, source):
        return jnp.concatenate(
            [
                lax.dynamic_slice_in_dim(value, s * rows, rows, value.ndim - 1)
                for s in source
            ],
            axis=-1,
        )

    def natural_vector(vector):
        halves = [
            lax.dynamic_slice_in_dim(vector, (y ^ i) * width, width, 0) for i in tensor_order
        ]
        return shuffle(jnp.concatenate(halves), block_from)

    def seq_columns(weight):
        cols = weight.shape[1] // S
        return [lax.dynamic_slice_in_dim(weight, (z ^ k) * cols, cols, 1) for k in range(S)]

    def own_columns(vector):
        cols = vector.shape[0] // S
        return lax.dynamic_slice_in_dim(vector, z * cols, cols, 0)

    def gather_tokens(value):
        pieces = [value] + [swap(value, "seq", k) for k in range(1, S)]
        mine = jnp.concatenate(pieces, axis=0)
        halves = gather_blocks(mine, "tensor")
        return shuffle(jnp.concatenate(halves, axis=1), block_from)

    def gather_weight(weight):
        sends = seq_columns(weight)
        block = jnp.concatenate(
            [sends[0]] + [swap(sends[k], "seq", k) for k in range(1, S)], axis=0
        )
        return jnp.concatenate(gather_blocks(block, "fsdp"), axis=0)

    def sum_blocks(left, right):
        half = left.shape[1] // 2
        bits = bits_of(F)
        keep = mm(left[:, :half], right, 0, 0)
        sent = bf(mm(left[:, half:], right, 0, 0))
        total = keep + f32(swap(sent, "fsdp", bits[0]))
        return sum_rows(total, bits[1:])

    def sum_rows(total, bits):
        for bit in bits:
            half = total.shape[0] // 2
            total = total[:half] + f32(swap(bf(total[half:]), "fsdp", bit))
        return total

    def home_weight(total):
        cols = total.shape[1]
        small = bf(total)
        pieces = [total[:rows]] + [
            f32(swap(small[k * rows : (k + 1) * rows], "seq", k)) for k in range(1, S)
        ]
        stacked = jnp.stack(pieces)
        return jnp.concatenate(
            [lax.dynamic_index_in_dim(stacked, z ^ b, 0, keepdims=False) for b in range(S)],
            axis=1,
        )

    def home_tokens(partial):
        natural = shuffle(partial, block_to)
        total = natural
        for bit in bits_of(T):
            half = total.shape[1] // 2
            total = total[:, :half] + f32(swap(bf(total[:, half:]), "tensor", bit))
        small = bf(total)
        out = total[:tok]
        for k in range(1, S):
            out = out + f32(swap(small[k * tok : (k + 1) * tok], "seq", k))
        return out

    rows_in = gather_tokens(hidden_in)
    w_qkv = gather_weight(qkv_weight)
    cot = gather_tokens(out_cotangent)
    w_proj = gather_weight(proj_weight)
    w_up = gather_weight(up_weight)
    w_down = gather_weight(down_weight)

    attn_gain = natural_vector(attn_norm_gain)
    attn_shift = natural_vector(attn_norm_bias)
    mlp_gain = natural_vector(mlp_norm_gain)
    mlp_shift = natural_vector(mlp_norm_bias)

    float_rows = f32(rows_in)
    centered = float_rows - jnp.mean(float_rows, axis=-1, keepdims=True)
    inv_std = lax.rsqrt(jnp.mean(centered * centered, axis=-1, keepdims=True) + norm_eps)
    xhat = centered * inv_std
    attn_in = bf(xhat * attn_gain + attn_shift)
    mlp_in = bf(xhat * mlp_gain + mlp_shift)

    token_row = jnp.arange(tok, dtype=jnp.int32)

    def positions_of(fd):
        return jnp.concatenate([((z ^ k) * F + fd) * tok + token_row for k in range(S)])

    query_pos = positions_of(f)
    key_pos = jnp.concatenate([positions_of(f ^ j) for j in order])
    cos_part, sin_part = rotary_tables(query_pos)
    heads = width // HEAD_DIM // S
    qkv = mm(attn_in, w_qkv, 1, 0) + own_columns(qkv_bias)
    queries, pairs = [], []
    for h in range(heads):
        base = h * 3 * HEAD_DIM
        queries.append(bf(rotate(qkv[:, base : base + HEAD_DIM], cos_part, sin_part)))
        pairs.append(
            bf(rotate(qkv[:, base + HEAD_DIM : base + 2 * HEAD_DIM], cos_part, sin_part))
        )
        pairs.append(bf(qkv[:, base + 2 * HEAD_DIM : base + 3 * HEAD_DIM]))
    pair_all = jnp.concatenate(gather_blocks(jnp.concatenate(pairs, axis=1), "fsdp"), axis=0)
    allowed = key_pos[None, :] <= query_pos[:, None]
    attn_parts, exp_parts, recips = [], [], []
    for h in range(heads):
        keys = pair_all[:, 2 * h * HEAD_DIM : (2 * h + 1) * HEAD_DIM]
        vals = pair_all[:, (2 * h + 1) * HEAD_DIM : (2 * h + 2) * HEAD_DIM]
        scores = jnp.where(allowed, mm(queries[h], keys, 1, 1) * scale, -1e30)
        row_max = jnp.max(scores, axis=-1, keepdims=True)
        exp_terms = jnp.where(allowed, jnp.exp(scores - row_max), 0.0)
        recip = 1.0 / jnp.sum(exp_terms, axis=-1, keepdims=True)
        attn_parts.append(bf(mm(bf(exp_terms), vals, 1, 0) * recip))
        exp_parts.append(exp_terms)
        recips.append(recip)
    attn = jnp.concatenate(attn_parts, axis=1)

    up_rows = mm(mlp_in, w_up, 1, 0) + own_columns(up_bias)
    active, slope = gelu_parts(up_rows)
    active = bf(active)

    attn_grad = bf(mm(cot, w_proj, 1, 0))
    grads, pair_terms = [], []
    for h in range(heads):
        keys = pair_all[:, 2 * h * HEAD_DIM : (2 * h + 1) * HEAD_DIM]
        vals = pair_all[:, (2 * h + 1) * HEAD_DIM : (2 * h + 2) * HEAD_DIM]
        grad_h = attn_grad[:, h * HEAD_DIM : (h + 1) * HEAD_DIM]
        delta = jnp.sum(f32(grad_h) * f32(attn_parts[h]), axis=-1, keepdims=True)
        probs = exp_parts[h] * recips[h]
        score_grad = bf(probs * (mm(grad_h, vals, 1, 1) - delta))
        grads.append(mm(score_grad, keys, 1, 0) * scale)
        pair_terms.append(mm(score_grad, queries[h], 0, 0) * scale)
        pair_terms.append(mm(bf(probs), grad_h, 0, 0))
    pair_grad = sum_rows(jnp.concatenate(pair_terms, axis=1), bits_of(F))
    columns = []
    for h in range(heads):
        columns.append(rotate(grads[h], cos_part, -sin_part))
        columns.append(
            rotate(pair_grad[:, 2 * h * HEAD_DIM : (2 * h + 1) * HEAD_DIM], cos_part, -sin_part)
        )
        columns.append(pair_grad[:, (2 * h + 1) * HEAD_DIM : (2 * h + 2) * HEAD_DIM])
    token_grads = bf(jnp.concatenate(columns, axis=1))

    pre_grad = mm(cot, w_down, 1, 0) * slope
    pre_small = bf(pre_grad)

    down_weight_grad = home_weight(sum_blocks(cot, active))
    proj_weight_grad = home_weight(sum_blocks(cot, attn))
    branch = home_tokens(mm(attn, w_proj, 1, 1) + mm(active, w_down, 1, 1))
    up_weight_grad = home_weight(sum_blocks(mlp_in, pre_small))
    qkv_weight_grad = home_weight(sum_blocks(attn_in, token_grads))

    hidden_out = bf(f32(hidden_in) + branch + proj_bias + down_bias)

    mlp_in_grad = mm(pre_small, w_up, 1, 1)
    attn_in_grad = mm(token_grads, w_qkv, 1, 1)
    spread = attn_in_grad * attn_gain + mlp_in_grad * mlp_gain
    mean_grad = jnp.mean(spread, axis=-1, keepdims=True)
    mean_proj = jnp.mean(spread * xhat, axis=-1, keepdims=True)
    input_term = inv_std * (spread - mean_grad - xhat * mean_proj)
    input_grad = bf(f32(out_cotangent) + home_tokens(input_term))

    def total_over(vector, axis):
        for bit in bits_of(lax.axis_size(axis)):
            vector = vector + swap(vector, axis, bit)
        return vector

    gains = jnp.stack(
        [
            jnp.sum(attn_in_grad * xhat, axis=0),
            jnp.sum(attn_in_grad, axis=0),
            jnp.sum(mlp_in_grad * xhat, axis=0),
            jnp.sum(mlp_in_grad, axis=0),
        ]
    )
    gains = shuffle(gains, block_to)
    gains = jnp.concatenate(
        [lax.dynamic_slice_in_dim(gains, (y ^ i) * width, width, 1) for i in range(T)], axis=1
    )
    gains = total_over(gains, "tensor").reshape(-1)

    def spread_columns(vector):
        cols = vector.shape[0]
        empty = jnp.zeros((S * cols,), jnp.float32)
        return lax.dynamic_update_slice_in_dim(empty, vector, z * cols, 0)

    qkv_bias_part = spread_columns(jnp.sum(f32(token_grads), axis=0))
    up_bias_part = spread_columns(jnp.sum(pre_grad, axis=0))
    out_bias_part = jnp.sum(f32(out_cotangent), axis=0)
    vector = jnp.concatenate([gains, qkv_bias_part, up_bias_part, out_bias_part])
    vector = total_over(total_over(vector, "seq"), "fsdp")
    parts = []
    start = 0
    for length in (D, D, D, D, 3 * width, up_bias.shape[0], width):
        parts.append(vector[start : start + length])
        start += length
    attn_gain_grad, attn_bias_grad, mlp_gain_grad, mlp_bias_grad = parts[:4]
    qkv_bias_grad, up_bias_grad, out_bias_grad = parts[4:]

    return (
        hidden_out,
        input_grad,
        attn_gain_grad,
        attn_bias_grad,
        mlp_gain_grad,
        mlp_bias_grad,
        qkv_weight_grad,
        qkv_bias_grad,
        proj_weight_grad,
        out_bias_grad,
        up_weight_grad,
        up_bias_grad,
        down_weight_grad,
        out_bias_grad,
    )


def solution(mesh):
    matrix = P(("seq", "fsdp"), "tensor")
    vector = P("tensor")
    return jax.shard_map(
        per_device,
        mesh=mesh,
        in_specs=(
            matrix, matrix, P(), P(), P(), P(),
            matrix, vector, matrix, vector, matrix, vector, matrix, vector,
        ),
        out_specs=(
            matrix, matrix, P(), P(), P(), P(),
            matrix, vector, matrix, vector, matrix, vector, matrix, vector,
        ),
        check_vma=False,
    )
```

```python
import functools
import math

import jax
import jax.numpy as jnp
from jax import lax
from jax.experimental import pallas as pl
from jax.experimental.pallas import tpu as pltpu
from jax.sharding import PartitionSpec as P

HEAD_DIM = 256
ROT = 64
MESH = pl.DeviceIdType.MESH

norm_eps = 1e-05
rope_base = 10000.0


def gelu_parts(pre_act):
    cdf = 0.5 * (1.0 + lax.erf(pre_act * 0.7071067811865476))
    slope = cdf + pre_act * jnp.exp(-0.5 * pre_act * pre_act) * 0.3989422804014327
    return (pre_act * cdf, slope)


def rotary_tables(positions):
    half_rot = ROT // 2
    exponent = jnp.arange(half_rot, dtype=jnp.float32) * (2.0 / ROT)
    frequency = jnp.exp(-exponent * math.log(rope_base))
    angles = positions.astype(jnp.float32)[:, None] * frequency[None, :]
    return (jnp.cos(angles), jnp.sin(angles))


def rotate(values, cos_part, sin_part):
    half_rot = ROT // 2
    first_half = values[:, :half_rot]
    second_half = values[:, half_rot:ROT]
    return jnp.concatenate(
        [
            first_half * cos_part - second_half * sin_part,
            second_half * cos_part + first_half * sin_part,
            values[:, ROT:],
        ],
        axis=-1,
    )


def mm(left, right, left_dim, right_dim):
    return lax.dot_general(
        left, right, (((left_dim,), (right_dim,)), ((), ())), preferred_element_type=jnp.float32
    )


def swap(value, axis, bits):
    size = lax.axis_size(axis)
    return lax.ppermute(value, axis, [(i, i ^ bits) for i in range(size)])


def bits_of(size):
    return [1 << b for b in range(size.bit_length() - 1)]


def gather_blocks(block, axis):
    blocks = [block]
    for bit in reversed(bits_of(lax.axis_size(axis))):
        blocks = blocks + [swap(b, axis, bit) for b in blocks]
    return blocks


def gather_order(size):
    order = [0]
    for bit in reversed(bits_of(size)):
        order = order + [j | bit for j in order]
    return order


def bf(value):
    return value.astype(jnp.bfloat16)


def f32(value):
    return value.astype(jnp.float32)


def flip(rank, mask, size):
    out = jnp.int32(0)
    for b in range(size.bit_length() - 1):
        digit = lax.rem(lax.div(rank, jnp.int32(1 << b)), jnp.int32(2))
        out = out + ((1 - digit) if mask >> b & 1 else digit) * (1 << b)
    return out


def low_bit(j, size):
    return j & -j if j else size


def at(index, size):
    return pl.ds(pl.multiple_of(index * size, size), size)


def greet(S, T, F, z, y, f):
    barrier = pltpu.get_barrier_semaphore()
    peers = [{"seq": flip(z, k, S)} for k in range(1, S)]
    peers += [{"tensor": flip(y, t, T)} for t in range(1, T)]
    peers += [{"fsdp": flip(f, b, F)} for b in bits_of(F)]
    for peer in peers:
        pl.semaphore_signal(barrier, inc=1, device_id=peer, device_id_type=MESH)
    pl.semaphore_wait(barrier, len(peers))


def remote(src, dst, send, recv, peer):
    return pltpu.make_async_remote_copy(
        src_ref=src, dst_ref=dst, send_sem=send, recv_sem=recv, device_id=peer, device_id_type=MESH
    )


def gather_kernel(S, T, F, order, *refs):
    n = len(order)
    ins, outs = refs[:n], refs[n : 2 * n]
    own_sem, send_sem, recv_sem = refs[2 * n :]
    z, y, f = lax.axis_index("seq"), lax.axis_index("tensor"), lax.axis_index("fsdp")
    bits = bits_of(F)
    lanes = max(T, F)

    def token_place(a, zd, yd):
        tok, width = ins[a].shape
        return outs[a].at[at(zd, tok), at(yd, width)]

    def row_place(a, zd, fd):
        rows = ins[a].shape[0]
        return outs[a].at[at(zd * F + fd, rows), :]

    def sem(a, k, j):
        return (a * S + k) * lanes + j

    def seq_copy(a, k):
        peer = flip(z, k, S)
        i = sem(a, k, 0)
        if order[a] == "tokens":
            src, dst = ins[a], token_place(a, z, y)
        else:
            cols = outs[a].shape[1]
            src, dst = ins[a].at[:, at(peer, cols)], row_place(a, z, f)
        return remote(src, dst, send_sem.at[i], recv_sem.at[i], {"seq": peer})

    def relay(a, k, j0, step):
        zd = flip(z, k, S)
        i = sem(a, k, j0 | step)
        if order[a] == "tokens":
            dst = token_place(a, zd, y)
            src = ins[a] if k == 0 else dst
            peer = {"tensor": flip(y, step, T)}
        else:
            dst = row_place(a, zd, flip(f, j0, F))
            src = ins[a].at[:, at(z, outs[a].shape[1])] if k == 0 and j0 == 0 else dst
            peer = {"fsdp": flip(f, step, F)}
        return remote(src, dst, send_sem.at[i], recv_sem.at[i], peer)

    def arrival(a, k, j):
        zd = flip(z, k, S)
        i = sem(a, k, j)
        if order[a] == "tokens":
            dst = token_place(a, zd, flip(y, j, T))
        else:
            dst = row_place(a, zd, flip(f, j, F))
        return remote(dst, dst, send_sem.at[i], recv_sem.at[i], {"seq": flip(z, 1, S)})

    def own_copy(a):
        if order[a] == "tokens":
            src, dst = ins[a], token_place(a, z, y)
        else:
            src, dst = ins[a].at[:, at(z, outs[a].shape[1])], row_place(a, z, f)
        return pltpu.make_async_copy(src, dst, own_sem.at[a])

    def steps(a, j):
        if order[a] == "tokens":
            return list(range(1, T)) if j == 0 else []
        return [b for b in reversed(bits) if b < low_bit(j, F)]

    def reach(a):
        if order[a] == "tokens":
            return list(range(1, T))
        return sorted(range(1, F), key=lambda j: (-low_bit(j, F), j))

    greet(S, T, F, z, y, f)
    sends = []

    def start(copy):
        copy.start()
        sends.append(copy)

    for a in range(n):
        for k in range(1, S):
            start(seq_copy(a, k))
        for step in steps(a, 0):
            start(relay(a, 0, 0, step))
        own_copy(a).start()

    def pass_on(a, k, j):
        arrival(a, k, j).wait_recv()
        for step in steps(a, j):
            start(relay(a, k, j, step))

    for a in range(n + 1):
        if a < n:
            for k in range(1, S):
                pass_on(a, k, 0)
        if a > 0:
            for j in reach(a - 1):
                for k in range(S):
                    pass_on(a - 1, k, j)
    for a in range(n):
        own_copy(a).wait()
    for copy in sends:
        copy.wait_send()


def gather_all(S, T, F, tokens, weights):
    order = ("tokens",) * len(tokens) + ("rows",) * len(weights)
    arrays = tuple(tokens) + tuple(weights)
    shapes = [(S * t.shape[0], T * t.shape[1]) for t in tokens]
    shapes += [(S * F * w.shape[0], w.shape[1] // S) for w in weights]
    count = len(arrays) * S * max(T, F)
    return pl.pallas_call(
        functools.partial(gather_kernel, S, T, F, order),
        out_shape=[jax.ShapeDtypeStruct(s, jnp.bfloat16) for s in shapes],
        in_specs=[pl.BlockSpec(memory_space=pltpu.VMEM)] * len(arrays),
        out_specs=[pl.BlockSpec(memory_space=pl.ANY)] * len(arrays),
        scratch_shapes=[
            pltpu.SemaphoreType.DMA((len(arrays),)),
            pltpu.SemaphoreType.DMA((count,)),
            pltpu.SemaphoreType.DMA((count,)),
        ],
        compiler_params=pltpu.CompilerParams(
            collective_id=0, has_side_effects=True, vmem_limit_bytes=16 << 20
        ),
    )(*arrays)


def spread_kernel(S, T, F, units, turned, n_left, n_sum, *refs):
    n = len(units)
    lefts, refs = refs[:n_left], refs[n_left:]
    rights, refs = refs[:n], refs[n:]
    sums, refs = refs[:n_sum], refs[n_sum:]
    grads, refs = refs[:n], refs[n:]
    homes, refs = refs[:n_sum], refs[n_sum:]
    left_v, refs = refs[:n_left], refs[n_left:]
    right_v, refs = refs[:n], refs[n:]
    sum_v, refs = refs[:n_sum], refs[n_sum:]
    out_b, refs = refs[:n], refs[n:]
    in_b, refs = refs[:n], refs[n:]
    seq_b, refs = refs[:n], refs[n:]
    home_v, refs = refs[:n_sum], refs[n_sum:]
    (y_out, y_in, z_out, z_in), refs = refs[:4], refs[4:]
    load_sem, own_sem, out_sem, in_sem, seq_send, seq_recv, y_send, y_recv, z_send, z_recv = refs
    z, y, f = lax.axis_index("seq"), lax.axis_index("tensor"), lax.axis_index("fsdp")
    bits = bits_of(F)
    tok, width = homes[0].shape
    sends = []

    def start(copy):
        copy.start()
        sends.append(copy)

    loads = {}

    def load(name, src, dst):
        copy = pltpu.make_async_copy(src, dst, load_sem.at[len(loads)])
        copy.start()
        loads[name] = copy

    waited = set()

    def need(name):
        if name not in waited:
            waited.add(name)
            loads[name].wait()

    load(("s", 0), sums[0], sum_v[0])
    for u in range(n):
        if ("l", units[u]) not in loads:
            load(("l", units[u]), lefts[units[u]], left_v[units[u]])
        load(("r", u), rights[u], right_v[u])
        if u == 0:
            for s in range(1, n_sum):
                load(("s", s), sums[s], sum_v[s])

    greet(S, T, F, z, y, f)

    def slot(j, bit):
        index = 0
        for jj in range(F):
            for bb in bits:
                if bb < low_bit(jj, F):
                    if (jj, bb) == (j, bit):
                        return index
                    index += 1
        raise ValueError

    def block_sum(u, j):
        need(("l", units[u]))
        need(("r", u))
        left = left_v[units[u]]
        rows = grads[u].shape[0]
        fd = flip(f, j, F)
        if turned:
            block = jnp.concatenate([left[at(zd * F + fd, rows), :] for zd in range(S)], axis=0)
            total = mm(block, right_v[u][...], 1, 0)
        else:
            block = jnp.concatenate([left[:, at(zd * F + fd, rows)] for zd in range(S)], axis=1)
            total = mm(block, right_v[u][...], 0, 0)
        for bit in bits:
            if bit < low_bit(j, F):
                i = u * (F - 1) + slot(j, bit)
                spot = in_b[u].at[slot(j, bit)]
                remote(spot, spot, out_sem.at[i], in_sem.at[i], {"fsdp": flip(f, bit, F)}).wait_recv()
                total = total + f32(in_b[u][slot(j, bit)])
        return total

    def fsdp_stage(u, bit):
        for j in range(1, F):
            if low_bit(j, F) == bit:
                out_b[u][j - 1] = bf(block_sum(u, j))
                there = slot(j - bit, bit)
                start(
                    remote(
                        out_b[u].at[j - 1],
                        in_b[u].at[there],
                        out_sem.at[u * (F - 1) + j - 1],
                        in_sem.at[u * (F - 1) + there],
                        {"fsdp": flip(f, bit, F)},
                    )
                )

    def seq_stage(u):
        rows = grads[u].shape[0]
        cols = seq_b[u].shape[1]
        seq_b[u][...] = bf(block_sum(u, 0))
        for k in range(1, S):
            peer = flip(z, k, S)
            start(
                remote(
                    seq_b[u].at[at(peer, rows), :],
                    grads[u].at[:, at(z, cols)],
                    seq_send.at[u * S + k],
                    seq_recv.at[u * S + k],
                    {"seq": peer},
                )
            )
        own_grad(u).start()

    def own_grad(u):
        rows = grads[u].shape[0]
        cols = seq_b[u].shape[1]
        return pltpu.make_async_copy(
            seq_b[u].at[at(z, rows), :], grads[u].at[:, at(z, cols)], own_sem.at[u]
        )

    def seq_wait(u):
        cols = seq_b[u].shape[1]
        for k in range(1, S):
            spot = grads[u].at[:, at(flip(z, k, S), cols)]
            i = u * S + k
            remote(spot, spot, seq_send.at[i], seq_recv.at[i], {"seq": flip(z, k, S)}).wait_recv()
        own_grad(u).wait()

    def y_index(s, k, t):
        return (s * S + k) * T + t

    def tensor_stage(s):
        need(("s", s))
        for k in [*range(1, S), 0]:
            zd = flip(z, k, S)
            for t in range(1, T):
                i = y_index(s, k, t)
                yd = flip(y, t, T)
                y_out[i] = bf(sum_v[s][at(zd, tok), at(yd, width)])
                start(remote(y_out.at[i], y_in.at[i], y_send.at[i], y_recv.at[i], {"tensor": yd}))

    def token_stage(s):
        for k in [*range(1, S), 0]:
            zd = flip(z, k, S)
            total = sum_v[s][at(zd, tok), at(y, width)]
            for t in range(1, T):
                i = y_index(s, k, t)
                remote(
                    y_in.at[i], y_in.at[i], y_send.at[i], y_recv.at[i], {"tensor": flip(y, t, T)}
                ).wait_recv()
                total = total + f32(y_in[i])
            if k:
                i = s * S + k
                z_out[i] = bf(total)
                start(remote(z_out.at[i], z_in.at[i], z_send.at[i], z_recv.at[i], {"seq": zd}))
            else:
                home_v[s][...] = total

    def token_wait(s):
        total = home_v[s][...]
        for k in range(1, S):
            i = s * S + k
            remote(
                z_in.at[i], z_in.at[i], z_send.at[i], z_recv.at[i], {"seq": flip(z, k, S)}
            ).wait_recv()
            total = total + f32(z_in[i])
        home_v[s][...] = total
        home_copy(s).start()

    def home_copy(s):
        return pltpu.make_async_copy(home_v[s], homes[s], own_sem.at[n + s])

    tensor_stage(0)
    fsdp_stage(0, bits[0])
    token_stage(0)
    tensor_stage(1)
    for u in range(n):
        if u + 1 < n:
            fsdp_stage(u + 1, bits[0])
        for bit in bits[1:]:
            fsdp_stage(u, bit)
        if u == 0:
            token_stage(1)
        seq_stage(u)
    for s in range(n_sum):
        token_wait(s)
    for u in range(n):
        seq_wait(u)
    for s in range(n_sum):
        home_copy(s).wait()
    for copy in sends:
        copy.wait_send()


def spread_all(S, T, F, lefts, units, rights, sums, rows):
    turned = rows % 128 != 0
    if turned:
        lefts = [left.T for left in lefts]
    n, n_left, n_sum = len(rights), len(lefts), len(sums)
    ntok, D = sums[0].shape
    tok, width = ntok // S, D // T
    block = S * rows
    small = jnp.bfloat16
    any_spec = pl.BlockSpec(memory_space=pl.ANY)
    cols = [r.shape[1] for r in rights]
    dma = pltpu.SemaphoreType.DMA
    return pl.pallas_call(
        functools.partial(spread_kernel, S, T, F, units, turned, n_left, n_sum),
        out_shape=[jax.ShapeDtypeStruct((rows, S * c), small) for c in cols]
        + [jax.ShapeDtypeStruct((tok, width), jnp.float32)] * n_sum,
        in_specs=[any_spec] * (n + n_left + n_sum),
        out_specs=[any_spec] * (n + n_sum),
        scratch_shapes=[pltpu.VMEM(left.shape, small) for left in lefts]
        + [pltpu.VMEM(r.shape, small) for r in rights]
        + [pltpu.VMEM(s.shape, jnp.float32) for s in sums]
        + [pltpu.VMEM((F - 1, block, c), small) for c in cols]
        + [pltpu.VMEM((F - 1, block, c), small) for c in cols]
        + [pltpu.VMEM((block, c), small) for c in cols]
        + [pltpu.VMEM((tok, width), jnp.float32)] * n_sum
        + [pltpu.VMEM((n_sum * S * T, tok, width), small)] * 2
        + [pltpu.VMEM((n_sum * S, tok, width), small)] * 2
        + [
            dma((n + n_left + n_sum,)),
            dma((n + n_sum,)),
            dma((n * (F - 1),)),
            dma((n * (F - 1),)),
            dma((n * S,)),
            dma((n * S,)),
            dma((n_sum * S * T,)),
            dma((n_sum * S * T,)),
            dma((n_sum * S,)),
            dma((n_sum * S,)),
        ],
        compiler_params=pltpu.CompilerParams(
            collective_id=1, has_side_effects=True, vmem_limit_bytes=60 << 20
        ),
    )(*lefts, *rights, *sums)


def per_device(
    hidden_in,
    out_cotangent,
    attn_norm_gain,
    attn_norm_bias,
    mlp_norm_gain,
    mlp_norm_bias,
    qkv_weight,
    qkv_bias,
    proj_weight,
    proj_bias,
    up_weight,
    up_bias,
    down_weight,
    down_bias,
):
    S = lax.axis_size("seq")
    T = lax.axis_size("tensor")
    F = lax.axis_size("fsdp")
    z = lax.axis_index("seq")
    f = lax.axis_index("fsdp")
    tok, width = hidden_in.shape
    rows = qkv_weight.shape[0]
    scale = HEAD_DIM ** (-0.5)
    order = gather_order(F)

    def own_columns(vector):
        cols = vector.shape[0] // S
        return lax.dynamic_slice_in_dim(vector, z * cols, cols, 0)

    def sum_rows(total, bits):
        for bit in bits:
            half = total.shape[0] // 2
            total = total[:half] + f32(swap(bf(total[half:]), "fsdp", bit))
        return total

    rows_in, cot, w_qkv, w_proj, w_up, w_down = gather_all(
        S, T, F, (hidden_in, out_cotangent), (qkv_weight, proj_weight, up_weight, down_weight)
    )

    float_rows = f32(rows_in)
    centered = float_rows - jnp.mean(float_rows, axis=-1, keepdims=True)
    inv_std = lax.rsqrt(jnp.mean(centered * centered, axis=-1, keepdims=True) + norm_eps)
    xhat = centered * inv_std
    attn_in = bf(xhat * attn_norm_gain + attn_norm_bias)
    mlp_in = bf(xhat * mlp_norm_gain + mlp_norm_bias)

    token_row = jnp.arange(tok, dtype=jnp.int32)

    def positions_of(fd):
        return jnp.concatenate([(zd * F + fd) * tok + token_row for zd in range(S)])

    query_pos = positions_of(f)
    key_pos = jnp.concatenate([positions_of(f ^ j) for j in order])
    cos_part, sin_part = rotary_tables(query_pos)
    heads = width // HEAD_DIM // S
    qkv = mm(attn_in, w_qkv, 1, 0) + own_columns(qkv_bias)
    queries, pairs = [], []
    for h in range(heads):
        base = h * 3 * HEAD_DIM
        queries.append(bf(rotate(qkv[:, base : base + HEAD_DIM], cos_part, sin_part)))
        pairs.append(
            bf(rotate(qkv[:, base + HEAD_DIM : base + 2 * HEAD_DIM], cos_part, sin_part))
        )
        pairs.append(bf(qkv[:, base + 2 * HEAD_DIM : base + 3 * HEAD_DIM]))
    pair_all = jnp.concatenate(gather_blocks(jnp.concatenate(pairs, axis=1), "fsdp"), axis=0)
    allowed = key_pos[None, :] <= query_pos[:, None]
    attn_parts, exp_parts, recips = [], [], []
    for h in range(heads):
        keys = pair_all[:, 2 * h * HEAD_DIM : (2 * h + 1) * HEAD_DIM]
        vals = pair_all[:, (2 * h + 1) * HEAD_DIM : (2 * h + 2) * HEAD_DIM]
        scores = jnp.where(allowed, mm(queries[h], keys, 1, 1) * scale, -1e30)
        row_max = jnp.max(scores, axis=-1, keepdims=True)
        exp_terms = jnp.where(allowed, jnp.exp(scores - row_max), 0.0)
        recip = 1.0 / jnp.sum(exp_terms, axis=-1, keepdims=True)
        attn_parts.append(bf(mm(bf(exp_terms), vals, 1, 0) * recip))
        exp_parts.append(exp_terms)
        recips.append(recip)
    attn = jnp.concatenate(attn_parts, axis=1)

    up_rows = mm(mlp_in, w_up, 1, 0) + own_columns(up_bias)
    active, slope = gelu_parts(up_rows)
    active = bf(active)

    attn_grad = bf(mm(cot, w_proj, 1, 0))
    grads, pair_terms = [], []
    for h in range(heads):
        keys = pair_all[:, 2 * h * HEAD_DIM : (2 * h + 1) * HEAD_DIM]
        vals = pair_all[:, (2 * h + 1) * HEAD_DIM : (2 * h + 2) * HEAD_DIM]
        grad_h = attn_grad[:, h * HEAD_DIM : (h + 1) * HEAD_DIM]
        delta = jnp.sum(f32(grad_h) * f32(attn_parts[h]), axis=-1, keepdims=True)
        probs = exp_parts[h] * recips[h]
        score_grad = bf(probs * (mm(grad_h, vals, 1, 1) - delta))
        grads.append(mm(score_grad, keys, 1, 0) * scale)
        pair_terms.append(mm(score_grad, queries[h], 0, 0) * scale)
        pair_terms.append(mm(bf(probs), grad_h, 0, 0))
    pair_grad = sum_rows(jnp.concatenate(pair_terms, axis=1), bits_of(F))
    columns = []
    for h in range(heads):
        columns.append(rotate(grads[h], cos_part, -sin_part))
        columns.append(
            rotate(pair_grad[:, 2 * h * HEAD_DIM : (2 * h + 1) * HEAD_DIM], cos_part, -sin_part)
        )
        columns.append(pair_grad[:, (2 * h + 1) * HEAD_DIM : (2 * h + 2) * HEAD_DIM])
    token_grads = bf(jnp.concatenate(columns, axis=1))

    pre_grad = mm(cot, w_down, 1, 0) * slope
    pre_small = bf(pre_grad)
    branch = mm(attn, w_proj, 1, 1) + mm(active, w_down, 1, 1)

    mlp_in_grad = mm(pre_small, w_up, 1, 1)
    attn_in_grad = mm(token_grads, w_qkv, 1, 1)
    spread = attn_in_grad * attn_norm_gain + mlp_in_grad * mlp_norm_gain
    mean_grad = jnp.mean(spread, axis=-1, keepdims=True)
    mean_proj = jnp.mean(spread * xhat, axis=-1, keepdims=True)
    input_term = inv_std * (spread - mean_grad - xhat * mean_proj)

    def total_over(value, axis):
        for bit in bits_of(lax.axis_size(axis)):
            value = value + swap(value, axis, bit)
        return value

    lanes = 128

    def as_rows(value):
        return value.reshape(-1, lanes)

    gains = jnp.stack(
        [
            jnp.sum(attn_in_grad * xhat, axis=0),
            jnp.sum(attn_in_grad, axis=0),
            jnp.sum(mlp_in_grad * xhat, axis=0),
            jnp.sum(mlp_in_grad, axis=0),
        ]
    )
    gains = total_over(as_rows(gains), "tensor")

    def spread_rows(value):
        value = as_rows(value)
        empty = jnp.zeros((S, *value.shape), jnp.float32)
        return lax.dynamic_update_slice_in_dim(empty, value[None], z, 0).reshape(-1, lanes)

    parts = [
        gains,
        spread_rows(jnp.sum(f32(token_grads), axis=0)),
        spread_rows(jnp.sum(pre_grad, axis=0)),
        as_rows(jnp.sum(f32(out_cotangent), axis=0)),
    ]
    total = total_over(total_over(jnp.concatenate(parts), "seq"), "fsdp")
    vectors = []
    start = 0
    for part in parts:
        vectors.append(total[start : start + part.shape[0]])
        start += part.shape[0]
    attn_gain_grad, attn_bias_grad, mlp_gain_grad, mlp_bias_grad = vectors[0].reshape(4, -1)
    qkv_bias_grad, up_bias_grad, out_bias_grad = [v.reshape(-1) for v in vectors[1:]]

    down_grad, up_grad, proj_grad, qkv_grad, branch_home, input_home = spread_all(
        S,
        T,
        F,
        (cot, mlp_in, attn_in),
        (0, 1, 0, 2),
        (active, pre_small, attn, token_grads),
        (branch, input_term),
        rows,
    )
    hidden_out = bf(f32(hidden_in) + branch_home + proj_bias + down_bias)
    input_grad = bf(f32(out_cotangent) + input_home)

    return (
        hidden_out,
        input_grad,
        attn_gain_grad,
        attn_bias_grad,
        mlp_gain_grad,
        mlp_bias_grad,
        f32(qkv_grad),
        qkv_bias_grad,
        f32(proj_grad),
        out_bias_grad,
        f32(up_grad),
        up_bias_grad,
        f32(down_grad),
        out_bias_grad,
    )


def solution(mesh):
    matrix = P(("seq", "fsdp"), "tensor")
    vector = P("tensor")
    return jax.shard_map(
        per_device,
        mesh=mesh,
        in_specs=(
            matrix, matrix, P(), P(), P(), P(),
            matrix, vector, matrix, vector, matrix, vector, matrix, vector,
        ),
        out_specs=(
            matrix, matrix, P(), P(), P(), P(),
            matrix, vector, matrix, vector, matrix, vector, matrix, vector,
        ),
        check_vma=False,
    )
```

```python
import functools
import math

import jax
import jax.numpy as jnp
import numpy as np
from jax import lax
from jax.experimental import pallas as pl
from jax.experimental.pallas import tpu as pltpu
from jax.sharding import PartitionSpec as P

HEAD_DIM = 256
ROT = 64
LANES = 128
STRIP = 256
MESH = pl.DeviceIdType.MESH
VMEM_BYTES = 63 << 20

norm_eps = 1e-05
rope_base = 10000.0


def bits_of(size):
    return [1 << b for b in range(size.bit_length() - 1)]


def bf(value):
    return value.astype(jnp.bfloat16)


def f32(value):
    return value.astype(jnp.float32)


def mm(left, right, left_dim, right_dim):
    return lax.dot_general(
        left, right, (((left_dim,), (right_dim,)), ((), ())), preferred_element_type=jnp.float32
    )


def rotary_tables(tok, blocks):
    half = ROT // 2
    frequency = rope_base ** (-np.arange(half, dtype=np.float64) * 2.0 / ROT)
    lanes = np.zeros(LANES)
    lanes[:half] = frequency
    lanes[half:ROT] = frequency
    inner = np.arange(tok, dtype=np.float64)[:, None] * lanes
    outer = np.arange(blocks, dtype=np.float64)[:, None] * tok * lanes
    pack = lambda a: np.stack([np.cos(a), np.sin(a)]).astype(np.float32)
    return (jnp.asarray(pack(inner)), jnp.asarray(pack(outer)))


def flip(rank, mask, size):
    out = jnp.int32(0)
    for b in range(size.bit_length() - 1):
        digit = lax.rem(lax.div(rank, jnp.int32(1 << b)), jnp.int32(2))
        out = out + ((1 - digit) if mask >> b & 1 else digit) * (1 << b)
    return out


def low_bit(j, size):
    return j & -j if j else size


def line_mask(j):
    mask = 0
    b = 0
    while j >> b:
        if j >> b & 1:
            mask ^= (2 << b) - 1
        b += 1
    return mask


def arrivals(size):
    return sorted(range(1, size), key=lambda j: (-low_bit(j, size), j))


def slot_of(j, bit, size):
    index = 0
    for jj in range(size):
        for bb in bits_of(size):
            if bb < low_bit(jj, size):
                if (jj, bb) == (j, bit):
                    return index
                index += 1
    raise ValueError


def at(index, size):
    return pl.ds(pl.multiple_of(index * size, size), size)


def greet(S, T, F, z, y, f):
    barrier = pltpu.get_barrier_semaphore()
    peers = [{"seq": flip(z, k, S)} for k in range(1, S)]
    peers += [{"tensor": flip(y, t, T)} for t in range(1, T)]
    peers += [{"fsdp": flip(f, b, F)} for b in bits_of(F)]
    for peer in peers:
        pl.semaphore_signal(barrier, inc=1, device_id=peer, device_id_type=MESH)
    pl.semaphore_wait(barrier, len(peers))


def remote(src, dst, send, recv, peer):
    return pltpu.make_async_remote_copy(
        src_ref=src, dst_ref=dst, send_sem=send, recv_sem=recv, device_id=peer, device_id_type=MESH
    )


def repeat(count, body):
    def step(i, carry):
        body(i)
        return carry

    lax.fori_loop(0, count, step, 0)


def turn(value, cos_part, sin_part):
    half = ROT // 2
    head = value[:, :LANES]
    lane = lax.broadcasted_iota(jnp.int32, head.shape, 1)
    other = jnp.where(
        lane < half, -pltpu.roll(head, LANES - half, 1), pltpu.roll(head, half, 1)
    )
    return jnp.concatenate([head * cos_part + other * sin_part, value[:, LANES:]], axis=1)


def first_kernel(S, T, F, *refs):
    hid_in, cot_in, wq_in, wp_in, wu_in, wd_in = refs[:6]
    attn_gain, attn_bias, mlp_gain, mlp_bias, qkv_bias, up_bias, inner, outer = refs[6:14]
    hid_o, cot_o, attn_in_o, mlp_in_o, stat_o, wq_o, wp_o, wu_o, wd_o = refs[14:23]
    attn_o, active_o, slope_o, tg_o = refs[23:27]
    hid, cot, attn_in, mlp_in, stat, wq, wp, wu, wd = refs[27:36]
    attn, active, slope, tg = refs[36:40]
    query, pair, attn_grad, probs, score_grad, row_info, part_in = refs[40:47]
    own_sem, out_sem, tok_send, tok_recv, row_send, row_recv = refs[47:53]
    pair_send, pair_recv, part_send, part_recv = refs[53:57]
    z, y, f = lax.axis_index("seq"), lax.axis_index("tensor"), lax.axis_index("fsdp")
    fbits = bits_of(F)
    tok, width = hid_in.shape
    ntok, D = hid.shape
    rows = wq_in.shape[0]
    keys = pair.shape[0]
    scale = HEAD_DIM ** (-0.5)
    tokens = ((hid_in, hid), (cot_in, cot))
    weights = ((wq_in, wq), (wp_in, wp), (wu_in, wu), (wd_in, wd))
    sends, pair_sends = [], []

    def start(copy):
        copy.start()
        sends.append(copy)

    def tok_sem(a, j, t):
        return (a * S + j) * T + t

    def tok_place(a, j, t):
        return tokens[a][1].at[at(flip(z, line_mask(j), S), tok), at(flip(y, t, T), width)]

    def tok_forward(a, j):
        src = tokens[a][0] if j == 0 else tok_place(a, j, 0)
        dst = tok_place(a, j, 0)
        for b in reversed(bits_of(S)):
            if b < low_bit(j, S):
                i = tok_sem(a, j + b, 0)
                peer = {"seq": flip(z, line_mask(b), S)}
                start(remote(src, dst, tok_send.at[i], tok_recv.at[i], peer))
        for t in range(1, T):
            i = tok_sem(a, j, t)
            peer = {"tensor": flip(y, t, T)}
            start(remote(src, dst, tok_send.at[i], tok_recv.at[i], peer))

    def tok_wait(a, j, t):
        i = tok_sem(a, j, t)
        spot = tok_place(a, j, t)
        remote(spot, spot, tok_send.at[i], tok_recv.at[i], {"tensor": flip(y, 1, T)}).wait_recv()

    def tok_seq(a):
        for j in arrivals(S):
            tok_wait(a, j, 0)
            tok_forward(a, j)

    def tok_rest(a):
        tok_own(a).wait()
        for j in range(S):
            for t in range(1, T):
                tok_wait(a, j, t)

    def tok_own(a):
        return pltpu.make_async_copy(tokens[a][0], tok_place(a, 0, 0), own_sem.at[a])

    def row_sem(m, k, j):
        return (m * S + k) * F + j

    def row_place(m, k, j):
        return weights[m][1].at[at(flip(z, k, S) * F + flip(f, j, F), rows), :]

    def row_source(m, zd):
        src, dst = weights[m]
        return src.at[:, at(zd, dst.shape[1])]

    def row_seq(m):
        for k in range(1, S):
            i = row_sem(m, k, 0)
            zd = flip(z, k, S)
            start(
                remote(
                    row_source(m, zd), row_place(m, 0, 0), row_send.at[i], row_recv.at[i], {"seq": zd}
                )
            )

    def row_forward(m, k, j):
        dst = row_place(m, k, j)
        src = row_source(m, z) if k == 0 and j == 0 else dst
        for b in reversed(fbits):
            if b < low_bit(j, F):
                i = row_sem(m, k, j + b)
                peer = {"fsdp": flip(f, b, F)}
                start(remote(src, dst, row_send.at[i], row_recv.at[i], peer))

    def row_wait(m, k, j):
        i = row_sem(m, k, j)
        spot = row_place(m, k, j)
        remote(spot, spot, row_send.at[i], row_recv.at[i], {"seq": flip(z, 1, S)}).wait_recv()

    def row_own(m):
        return pltpu.make_async_copy(row_source(m, z), row_place(m, 0, 0), own_sem.at[2 + m])

    def row_arrive(m):
        for k in range(1, S):
            row_wait(m, k, 0)
            row_forward(m, k, 0)

    def row_relay(m):
        for j in arrivals(F):
            if low_bit(j, F) > 1:
                for k in range(S):
                    row_wait(m, k, j)
                    row_forward(m, k, j)

    def row_rest(m):
        row_own(m).wait()
        for j in arrivals(F):
            if low_bit(j, F) == 1:
                for k in range(S):
                    row_wait(m, k, j)

    def pair_place(zd, j):
        return pair.at[at(zd * F + flip(f, j, F), tok), :]

    def pair_forward(zd, j):
        spot = pair_place(zd, j)
        for b in reversed(fbits):
            if b < low_bit(j, F):
                i = zd * F + j + b
                peer = {"fsdp": flip(f, b, F)}
                copy = remote(spot, spot, pair_send.at[i], pair_recv.at[i], peer)
                copy.start()
                pair_sends.append(copy)

    def pair_wait(zd, j):
        i = zd * F + j
        spot = pair_place(zd, j)
        remote(spot, spot, pair_send.at[i], pair_recv.at[i], {"fsdp": flip(f, 1, F)}).wait_recv()

    outs = []

    def put(src, dst):
        copy = pltpu.make_async_copy(src, dst, out_sem.at[len(outs)])
        copy.start()
        outs.append(copy)

    greet(S, T, F, z, y, f)
    tok_forward(0, 0)
    tok_own(0).start()
    row_seq(0)
    row_forward(0, 0, 0)
    row_own(0).start()
    tok_forward(1, 0)
    tok_own(1).start()
    for m in range(1, 4):
        row_seq(m)
        row_forward(m, 0, 0)
        row_own(m).start()

    tok_seq(0)
    tok_rest(0)
    put(hid, hid_o)
    chunk = 32

    def norm_chunk(i):
        part = at(i, chunk)
        x = f32(hid[part, :])
        mean = jnp.mean(x, axis=-1, keepdims=True)
        centered = x - mean
        inv_std = lax.rsqrt(jnp.mean(centered * centered, axis=-1, keepdims=True) + norm_eps)
        xhat = centered * inv_std
        attn_in[part, :] = bf(xhat * attn_gain[...] + attn_bias[...])
        mlp_in[part, :] = bf(xhat * mlp_gain[...] + mlp_bias[...])
        stat[0, part, :] = jnp.broadcast_to(mean, (chunk, LANES))
        stat[1, part, :] = jnp.broadcast_to(inv_std, (chunk, LANES))

    repeat(ntok // chunk, norm_chunk)
    put(attn_in, attn_in_o)
    put(mlp_in, mlp_in_o)
    put(stat, stat_o)

    def angles(zd, here=slice(None)):
        block = pl.ds(zd * F + f, 1)
        cos_in, sin_in = inner[0, here, :], inner[1, here, :]
        cos_out, sin_out = outer[0, block, :], outer[1, block, :]
        return (cos_in * cos_out - sin_in * sin_out, sin_in * cos_out + cos_in * sin_out)

    row_arrive(0)
    row_relay(0)
    row_rest(0)
    put(wq, wq_o)
    bias = qkv_bias[:, at(z, 3 * HEAD_DIM)]
    for c in range(3):
        part = mm(attn_in[...], wq[:, c * HEAD_DIM : (c + 1) * HEAD_DIM], 1, 0)
        part = part + bias[:, c * HEAD_DIM : (c + 1) * HEAD_DIM]
        for zd in range(S):
            piece = part[zd * tok : (zd + 1) * tok]
            if c < 2:
                piece = turn(piece, *angles(zd))
            if c == 0:
                query[zd * tok : (zd + 1) * tok, :] = bf(piece)
            else:
                spot = at(zd * F + f, tok)
                pair[spot, (c - 1) * HEAD_DIM : c * HEAD_DIM] = bf(piece)
    for zd in range(S):
        pair_forward(zd, 0)

    tok_seq(1)
    row_arrive(1)
    for j in arrivals(F):
        for zd in range(S):
            pair_wait(zd, j)
            pair_forward(zd, j)
    row_relay(1)

    qc = max(32, min(tok, tok * 2048 // keys))

    def masked_scores(zd, i, n):
        start_row = zd * tok + i * qc
        q = query[pl.ds(pl.multiple_of(start_row, qc), qc), :]
        scores = mm(q, pair[:n, :HEAD_DIM], 1, 1) * scale
        last = (zd * F + f) * tok + i * qc
        ahead = lax.broadcasted_iota(jnp.int32, scores.shape, 1) - lax.broadcasted_iota(
            jnp.int32, scores.shape, 0
        )
        return (scores, ahead <= last)

    for zd in range(S):
        n = (zd + 1) * F * tok

        def forward_chunk(i, zd=zd, n=n):
            here = pl.ds(pl.multiple_of(zd * tok + i * qc, qc), qc)
            scores, allowed = masked_scores(zd, i, n)
            top = jnp.max(jnp.where(allowed, scores, -1e30), axis=-1, keepdims=True)
            terms = jnp.where(allowed, jnp.exp(scores - top), 0.0)
            total = jnp.sum(terms, axis=-1, keepdims=True)
            mixed = mm(bf(terms), pair[:n, HEAD_DIM:], 1, 0) / total
            attn[here, :] = bf(mixed)
            row_info[here, :] = jnp.broadcast_to(top + jnp.log(total), (qc, LANES))

        repeat(tok // qc, forward_chunk)
    put(attn, attn_o)

    tok_rest(1)
    put(cot, cot_o)
    row_rest(1)
    put(wp, wp_o)
    attn_grad[...] = bf(mm(cot[...], wp[...], 1, 0))
    row_arrive(2)
    row_relay(2)
    for zd in range(S):
        n = (zd + 1) * F * tok

        def backward_chunk(i, zd=zd, n=n):
            here = pl.ds(pl.multiple_of(zd * tok + i * qc, qc), qc)
            scores, allowed = masked_scores(zd, i, n)
            weights_here = jnp.where(allowed, jnp.exp(scores - row_info[here, :1]), 0.0)
            grad = attn_grad[here, :]
            delta = jnp.sum(f32(grad) * f32(attn[here, :]), axis=-1, keepdims=True)
            slopes = mm(grad, pair[:n, HEAD_DIM:], 1, 1)
            inner_grad = bf(weights_here * (slopes - delta))
            probs[here, :n] = bf(weights_here)
            score_grad[here, :n] = inner_grad
            if n < keys:
                blank = jnp.zeros((qc, keys - n), jnp.bfloat16)
                probs[here, n:] = blank
                score_grad[here, n:] = blank
            cos_part, sin_part = angles(zd, pl.ds(pl.multiple_of(i * qc, qc), qc))
            grad_here = mm(inner_grad, pair[:n, :HEAD_DIM], 1, 0) * scale
            tg[here, :HEAD_DIM] = bf(turn(grad_here, cos_part, -sin_part))

        repeat(tok // qc, backward_chunk)

    def part_sum(j):
        def lanes(ref):
            return jnp.concatenate(
                [ref[:, at(zd * F + flip(f, j, F), tok)] for zd in range(S)], axis=1
            )

        total = jnp.concatenate(
            [mm(lanes(score_grad), query[...], 0, 0) * scale, mm(lanes(probs), attn_grad[...], 0, 0)],
            axis=1,
        )
        for b in fbits:
            if b < low_bit(j, F):
                i = slot_of(j, b, F)
                spot = part_in.at[i]
                peer = {"fsdp": flip(f, b, F)}
                remote(spot, spot, part_send.at[i], part_recv.at[i], peer).wait_recv()
                total = total + f32(part_in[i])
        return total

    for copy in pair_sends:
        copy.wait_send()

    def part_stage(bit):
        for j in range(1, F):
            if low_bit(j, F) == bit:
                spot = pair.at[(j - 1) * ntok : j * ntok, :]
                pair[(j - 1) * ntok : j * ntok, :] = bf(part_sum(j))
                i = slot_of(j - bit, bit, F)
                peer = {"fsdp": flip(f, bit, F)}
                start(remote(spot, part_in.at[i], part_send.at[j - 1], part_recv.at[i], peer))

    part_stage(fbits[0])
    row_rest(2)
    put(wu, wu_o)

    cols = wu.shape[1]
    for n in range(cols // STRIP):
        strip = slice(n * STRIP, (n + 1) * STRIP)
        mid = mm(mlp_in[...], wu[:, strip], 1, 0) + up_bias[
            :, pl.ds(pl.multiple_of(z * cols + n * STRIP, STRIP), STRIP)
        ]
        cdf = 0.5 * (1.0 + lax.erf(mid * 0.7071067811865476))
        active[:, strip] = bf(mid * cdf)
        slope[:, strip] = cdf + mid * jnp.exp(-0.5 * mid * mid) * 0.3989422804014327
        if n == 0:
            for bit in fbits[1:]:
                part_stage(bit)
    put(active, active_o)
    put(slope, slope_o)
    row_arrive(3)
    total = part_sum(0)
    for zd in range(S):
        here = slice(zd * tok, (zd + 1) * tok)
        cos_part, sin_part = angles(zd)
        tg[here, HEAD_DIM : 2 * HEAD_DIM] = bf(turn(total[here, :HEAD_DIM], cos_part, -sin_part))
        tg[here, 2 * HEAD_DIM :] = bf(total[here, HEAD_DIM:])
    put(tg, tg_o)
    row_relay(3)
    row_rest(3)
    put(wd, wd_o)
    for copy in outs:
        copy.wait()
    for copy in sends:
        copy.wait_send()


def first_call(S, T, F, arrays, vectors):
    hidden, _, wq, wp, wu, _ = arrays
    tok, width = hidden.shape
    rows = wq.shape[0]
    ntok, D, keys = S * tok, T * width, S * F * tok
    if width != S * HEAD_DIM or S * F * rows != D:
        raise ValueError
    small, wide = jnp.bfloat16, jnp.float32
    ff = wu.shape[1] // S
    inner, outer = rotary_tables(tok, S * F)
    outs = [((ntok, D), small)] * 4 + [((2, ntok, LANES), wide)]
    outs += [((D, w.shape[1] // S), small) for w in arrays[2:]]
    outs += [((ntok, HEAD_DIM), small), ((ntok, ff), small), ((ntok, ff), wide)]
    outs += [((ntok, 3 * HEAD_DIM), small)]
    n_part = max(F - 1, 1)
    scratch = outs + [
        ((ntok, HEAD_DIM), small),
        ((keys, 2 * HEAD_DIM), small),
        ((ntok, HEAD_DIM), small),
        ((ntok, keys), small),
        ((ntok, keys), small),
        ((ntok, LANES), wide),
        ((n_part, ntok, 2 * HEAD_DIM), small),
    ]
    dma = pltpu.SemaphoreType.DMA
    any_spec = pl.BlockSpec(memory_space=pl.ANY)
    vmem = pl.BlockSpec(memory_space=pltpu.VMEM)
    return pl.pallas_call(
        functools.partial(first_kernel, S, T, F),
        out_shape=[jax.ShapeDtypeStruct(*o) for o in outs],
        in_specs=[any_spec] * 6 + [vmem] * 8,
        out_specs=[any_spec] * len(outs),
        scratch_shapes=[pltpu.VMEM(*o) for o in scratch]
        + [
            dma((6,)),
            dma((len(outs),)),
            dma((2 * S * T,)),
            dma((2 * S * T,)),
            dma((4 * S * F,)),
            dma((4 * S * F,)),
            dma((S * F,)),
            dma((S * F,)),
            dma((n_part,)),
            dma((n_part,)),
        ],
        compiler_params=pltpu.CompilerParams(
            collective_id=0, has_side_effects=True, vmem_limit_bytes=VMEM_BYTES
        ),
    )(*arrays, *vectors, inner, outer)


def second_kernel(S, T, F, turned, *refs):
    cot_i, hid_i, attn_in_i, mlp_in_i, stat_i, wq_i, wp_i, wu_i, wd_i = refs[:9]
    attn_i, active_i, slope_i, tg_i, own_cot, attn_gain, mlp_gain = refs[9:16]
    grads, refs = refs[16:20], refs[20:]
    homes, (gain_o, qkv_bias_o, up_bias_o, out_bias_o), refs = refs[:2], refs[2:6], refs[6:]
    cot, hid, attn_in, mlp_in, stat, wq, wp, wud, attn, active, tg, pre = refs[:12]
    wide, own_half, sums, vec, vec_in, vec_seq, vec_ten = refs[12:19]
    out_b, in_b, seq_b, refs = refs[19:23], refs[23:27], refs[27:31], refs[31:]
    y_out, y_in, z_out, z_in, home_v = refs[:5]
    load_sem, own_sem, out_sem, in_sem, seq_send, seq_recv = refs[5:11]
    y_send, y_recv, z_send, z_recv, v_send, v_recv = refs[11:17]
    z, y, f = lax.axis_index("seq"), lax.axis_index("tensor"), lax.axis_index("fsdp")
    fbits, sbits = bits_of(F), bits_of(S)
    tok, width = homes[0].shape
    ntok, D = wide.shape
    ff = active.shape[1]
    units = (
        (attn, cot, HEAD_DIM),
        (active, cot, ff),
        (tg, attn_in, 3 * HEAD_DIM),
        (pre, mlp_in, ff),
    )
    sends = []

    def start(copy):
        copy.start()
        sends.append(copy)

    loads = {}

    def load(name, src, dst):
        loads[name] = pltpu.make_async_copy(src, dst, load_sem.at[len(loads)])
        loads[name].start()

    waited = set()

    def need(*names):
        for name in names:
            if name not in waited:
                waited.add(name)
                loads[name].wait()

    load("cot", cot_i, cot)
    load("attn", attn_i, attn)
    load("active", active_i, active)
    load("wd", wd_i, wud)
    load("wp", wp_i, wp)
    load("slope", slope_i, wide.at[:, :ff])
    load("tg", tg_i, tg)
    load("attn_in", attn_in_i, attn_in)
    load("wq", wq_i, wq)
    load("hid", hid_i, hid)
    load("stat", stat_i, stat)
    load("mlp_in", mlp_in_i, mlp_in)

    greet(S, T, F, z, y, f)

    def block_sum(u, j):
        right, left, _ = units[u]
        rows = grads[u].shape[0]
        fd = flip(f, j, F)
        if turned:
            block = jnp.concatenate([left[at(zd * F + fd, rows), :] for zd in range(S)], axis=0)
            total = mm(block, right[...], 1, 0)
        else:
            block = jnp.concatenate([left[:, at(zd * F + fd, rows)] for zd in range(S)], axis=1)
            total = mm(block, right[...], 0, 0)
        for bit in fbits:
            if bit < low_bit(j, F):
                s = slot_of(j, bit, F)
                i = u * (F - 1) + s
                spot = in_b[u].at[s]
                peer = {"fsdp": flip(f, bit, F)}
                remote(spot, spot, out_sem.at[i], in_sem.at[i], peer).wait_recv()
                total = total + f32(in_b[u][s])
        return total

    def fsdp_stage(u, bit):
        for j in range(1, F):
            if low_bit(j, F) == bit:
                out_b[u][j - 1] = bf(block_sum(u, j))
                there = slot_of(j - bit, bit, F)
                start(
                    remote(
                        out_b[u].at[j - 1],
                        in_b[u].at[there],
                        out_sem.at[u * (F - 1) + j - 1],
                        in_sem.at[u * (F - 1) + there],
                        {"fsdp": flip(f, bit, F)},
                    )
                )

    def own_grad(u):
        rows = grads[u].shape[0]
        cols = units[u][2]
        return pltpu.make_async_copy(
            seq_b[u].at[at(z, rows), :], grads[u].at[:, at(z, cols)], own_sem.at[u]
        )

    def seq_stage(u):
        rows = grads[u].shape[0]
        cols = units[u][2]
        seq_b[u][...] = bf(block_sum(u, 0))
        for k in range(1, S):
            peer = flip(z, k, S)
            start(
                remote(
                    seq_b[u].at[at(peer, rows), :],
                    grads[u].at[:, at(z, cols)],
                    seq_send.at[u * S + k],
                    seq_recv.at[u * S + k],
                    {"seq": peer},
                )
            )
        own_grad(u).start()

    def seq_wait(u):
        cols = units[u][2]
        for k in range(1, S):
            spot = grads[u].at[:, at(flip(z, k, S), cols)]
            i = u * S + k
            remote(spot, spot, seq_send.at[i], seq_recv.at[i], {"seq": flip(z, k, S)}).wait_recv()
        own_grad(u).wait()

    def y_index(s, t, zd):
        return (s * max(T - 1, 1) + t - 1) * S + zd

    def y_store(s, t, column, value):
        for zd in range(S):
            y_out[y_index(s, t, zd), :, column] = bf(value[zd * tok : (zd + 1) * tok])

    def tensor_send(s):
        for j in [*sorted(range(1, S), key=lambda j: (low_bit(j, S), j)), 0]:
            zd = flip(z, line_mask(j), S)
            for t in range(1, T):
                i = y_index(s, t, 0) + j
                peer = {"tensor": flip(y, t, T)}
                here = y_out.at[y_index(s, t, zd)]
                start(remote(here, y_in.at[i], y_send.at[i], y_recv.at[i], peer))

    def token_part(s, j):
        zd = flip(z, line_mask(j), S)
        total = own_half[at(zd, tok), :]
        for t in range(1, T):
            i = y_index(s, t, 0) + j
            spot = y_in.at[i]
            remote(spot, spot, y_send.at[i], y_recv.at[i], {"tensor": flip(y, t, T)}).wait_recv()
            total = total + f32(y_in[i])
        for bit in sbits:
            if bit < low_bit(j, S):
                i = s * (S - 1) + slot_of(j, bit, S)
                spot = z_in.at[i]
                peer = {"seq": flip(z, line_mask(bit), S)}
                remote(spot, spot, z_send.at[i], z_recv.at[i], peer).wait_recv()
                total = total + f32(z_in[i])
        return total

    def token_stage(s, bit):
        for j in range(1, S):
            if low_bit(j, S) == bit:
                i = s * (S - 1) + j - 1
                there = s * (S - 1) + slot_of(j - bit, bit, S)
                z_out[i] = bf(token_part(s, j))
                peer = {"seq": flip(z, line_mask(bit), S)}
                start(remote(z_out.at[i], z_in.at[there], z_send.at[i], z_recv.at[there], peer))

    def home_copy(s):
        return pltpu.make_async_copy(home_v.at[s], homes[s], own_sem.at[4 + s])

    def token_home(s):
        home_v[s] = token_part(s, 0)
        home_copy(s).start()

    def vec_exchange(i, dst, peer):
        return remote(vec.at[i], dst, v_send.at[i], v_recv.at[i], peer)

    n_fsdp = len(fbits)

    def vec_fsdp(b):
        start(vec_exchange(b, vec_in.at[b], {"fsdp": flip(f, fbits[b], F)}))

    def vec_fsdp_sum(b):
        vec_exchange(b, vec_in.at[b], {"fsdp": flip(f, fbits[b], F)}).wait_recv()
        vec[b + 1] = vec[b] + vec_in[b]

    def vec_seq_copy(k):
        peer = {"seq": flip(z, k, S)}
        i = n_fsdp + k - 1
        return remote(vec.at[n_fsdp], vec_seq.at[k - 1], v_send.at[i], v_recv.at[i], peer)

    def vec_seq_sum():
        qkv_bias_o[:, at(z, 3 * HEAD_DIM)] = vec[n_fsdp, 4:5, : 3 * HEAD_DIM]
        up_bias_o[:, at(z, ff)] = vec[n_fsdp, 5:6, :ff]
        parts = [vec[n_fsdp]]
        for k in range(1, S):
            vec_seq_copy(k).wait_recv()
            zd = flip(z, k, S)
            qkv_bias_o[:, at(zd, 3 * HEAD_DIM)] = vec_seq[k - 1, 4:5, : 3 * HEAD_DIM]
            up_bias_o[:, at(zd, ff)] = vec_seq[k - 1, 5:6, :ff]
            parts.append(vec_seq[k - 1])
        while len(parts) > 1:
            parts = [a + b for a, b in zip(parts[::2], parts[1::2])]
        out_bias_o[...] = parts[0][6:7, :width]
        vec_ten[0] = parts[0][:4]

    def vec_ten_copy(t):
        peer = {"tensor": flip(y, t, T)}
        i = n_fsdp + S - 1 + t - 1
        return remote(vec_ten.at[0], vec_ten.at[t], v_send.at[i], v_recv.at[i], peer)

    def vec_ten_sum():
        parts = [vec_ten[0]]
        for t in range(1, T):
            vec_ten_copy(t).wait_recv()
            parts.append(vec_ten[t])
        while len(parts) > 1:
            parts = [a + b for a, b in zip(parts[::2], parts[1::2])]
        gain_o[...] = parts[0]

    need("cot", "attn")
    vec[0] = jnp.zeros(vec.shape[1:], jnp.float32)
    fsdp_stage(0, fbits[0])
    need("active", "wd", "wp")

    def branch(column):
        return mm(active[...], wud[column, :], 1, 1) + mm(attn[...], wp[column, :], 1, 1)

    for t in [*range(1, T), 0]:
        for n in range(width // STRIP):
            there = pl.ds(
                pl.multiple_of(flip(y, t, T) * width + n * STRIP, STRIP), STRIP
            )
            here = slice(n * STRIP, (n + 1) * STRIP)
            if t:
                y_store(0, t, here, branch(there))
            else:
                own_half[:, here] = branch(there)
        if t == T - 1:
            tensor_send(0)
    for bit in fbits[1:]:
        fsdp_stage(0, bit)
    fsdp_stage(1, fbits[0])
    seq_stage(0)
    token_stage(0, sbits[0])

    need("slope")
    for n in range(ff // STRIP):
        here = slice(n * STRIP, (n + 1) * STRIP)
        value = mm(cot[...], wud[:, here], 0 if turned else 1, 0) * wide[:, here]
        vec[0, 5:6, here] = jnp.sum(value, axis=0, keepdims=True)
        pre[:, here] = bf(value)
    load("wu", wu_i, wud)
    for bit in fbits[1:]:
        fsdp_stage(1, bit)
    for bit in sbits[1:]:
        token_stage(0, bit)
    need("tg", "attn_in")
    fsdp_stage(2, fbits[0])
    seq_stage(1)
    need("mlp_in")
    fsdp_stage(3, fbits[0])
    token_home(0)

    need("wu", "wq", "hid", "stat")
    lane_parts = range(0, STRIP, LANES)

    def norm_strip(n):
        here = at(n, STRIP)
        a = mm(tg[...], wq[here, :], 1, 1)
        m = mm(pre[...], wud[here, :], 1, 1)
        mean, inv_std = stat[0, :, :1], stat[1, :, :1]
        xhat = (f32(hid[:, here]) - mean) * inv_std
        vec[0, 0:1, here] = jnp.sum(a * xhat, axis=0, keepdims=True)
        vec[0, 1:2, here] = jnp.sum(a, axis=0, keepdims=True)
        vec[0, 2:3, here] = jnp.sum(m * xhat, axis=0, keepdims=True)
        vec[0, 3:4, here] = jnp.sum(m, axis=0, keepdims=True)
        both = a * attn_gain[:, here] + m * mlp_gain[:, here]
        wide[:, here] = both
        scaled = both * xhat
        sums[0] += sum(both[:, c : c + LANES] for c in lane_parts)
        sums[1] += sum(scaled[:, c : c + LANES] for c in lane_parts)

    sums[...] = jnp.zeros_like(sums)
    repeat(D // STRIP, norm_strip)
    vec[0, 4:5, : 3 * HEAD_DIM] = jnp.sum(f32(tg[...]), axis=0, keepdims=True)
    vec[0, 6:7, :width] = jnp.sum(f32(own_cot[...]), axis=0, keepdims=True)
    vec_fsdp(0)
    for bit in fbits[1:]:
        fsdp_stage(2, bit)
    sums[0] = jnp.broadcast_to(jnp.sum(sums[0], axis=-1, keepdims=True) / D, sums.shape[1:])
    sums[1] = jnp.broadcast_to(jnp.sum(sums[1], axis=-1, keepdims=True) / D, sums.shape[1:])

    def input_term(column):
        mean, inv_std = stat[0, :, :1], stat[1, :, :1]
        xhat = (f32(hid[:, column]) - mean) * inv_std
        return inv_std * (wide[:, column] - sums[0, :, :1] - xhat * sums[1, :, :1])

    for t in [*range(1, T), 0]:
        for n in range(width // STRIP):
            there = pl.ds(
                pl.multiple_of(flip(y, t, T) * width + n * STRIP, STRIP), STRIP
            )
            here = slice(n * STRIP, (n + 1) * STRIP)
            if t:
                y_store(1, t, here, input_term(there))
            else:
                own_half[:, here] = input_term(there)
        if t == T - 1:
            tensor_send(1)
    vec_fsdp_sum(0)
    for b in range(1, n_fsdp):
        vec_fsdp(b)
        if b == 1:
            seq_stage(2)
            for bit in fbits[1:]:
                fsdp_stage(3, bit)
        vec_fsdp_sum(b)
    for k in range(1, S):
        start(vec_seq_copy(k))
    token_stage(1, sbits[0])
    seq_stage(3)
    vec_seq_sum()
    for t in range(1, T):
        start(vec_ten_copy(t))
    for bit in sbits[1:]:
        token_stage(1, bit)
    vec_ten_sum()
    token_home(1)
    for u in range(4):
        seq_wait(u)
    for s in range(2):
        home_copy(s).wait()
    for copy in sends:
        copy.wait_send()


def second_call(S, T, F, first, own_cot, attn_gain, mlp_gain, rows):
    hid, cot, attn_in, mlp_in, stat, wq, wp, wu, wd, attn, active, slope, tg = first
    turned = rows % LANES != 0
    if turned:
        cot, attn_in, mlp_in = cot.T, attn_in.T, mlp_in.T
    tok, width = own_cot.shape
    ntok, D = hid.shape
    ff = active.shape[1]
    small, wide = jnp.bfloat16, jnp.float32
    cols = (HEAD_DIM, ff, 3 * HEAD_DIM, ff)
    parts, block, n_f = max(F - 1, 1), S * rows, F.bit_length() - 1
    ins = (cot, hid, attn_in, mlp_in, stat, wq, wp, wu, wd, attn, active, slope, tg)
    any_spec = pl.BlockSpec(memory_space=pl.ANY)
    vmem = pl.BlockSpec(memory_space=pltpu.VMEM)
    dma = pltpu.SemaphoreType.DMA
    shape = jax.ShapeDtypeStruct
    scratch = [(a.shape, small) for a in (cot, hid, attn_in, mlp_in)] + [(stat.shape, wide)]
    scratch += [(a.shape, small) for a in (wq, wp, wu, attn, active, tg)]
    scratch += [
        ((ntok, ff), small),
        ((ntok, D), wide),
        ((ntok, width), wide),
        ((2, ntok, LANES), wide),
        ((n_f + 1, 8, D), wide),
        ((n_f, 8, D), wide),
        ((max(S - 1, 1), 8, D), wide),
        ((T, 4, D), wide),
    ]
    scratch += [((parts, block, c), small) for c in cols] * 2
    scratch += [((block, c), small) for c in cols]
    n_y, n_z, n_v = 2 * max(T - 1, 1) * S, 2 * max(S - 1, 1), n_f + S + T
    scratch += [((n_y, tok, width), small)] * 2 + [((n_z, tok, width), small)] * 2
    scratch += [((2, tok, width), wide)]
    return pl.pallas_call(
        functools.partial(second_kernel, S, T, F, turned),
        out_shape=[shape((rows, S * c), small) for c in cols]
        + [shape((tok, width), wide)] * 2
        + [shape((4, D), wide), shape((1, 3 * width), wide)]
        + [shape((1, S * ff), wide), shape((1, width), wide)],
        in_specs=[any_spec] * len(ins) + [vmem] * 3,
        out_specs=[any_spec] * 6 + [vmem] * 4,
        scratch_shapes=[pltpu.VMEM(*s) for s in scratch]
        + [
            dma((len(ins),)),
            dma((6,)),
            dma((4 * parts,)),
            dma((4 * parts,)),
            dma((4 * S,)),
            dma((4 * S,)),
            dma((n_y,)),
            dma((n_y,)),
            dma((n_z,)),
            dma((n_z,)),
            dma((n_v,)),
            dma((n_v,)),
        ],
        compiler_params=pltpu.CompilerParams(
            collective_id=1, has_side_effects=True, vmem_limit_bytes=VMEM_BYTES
        ),
    )(*ins, own_cot, attn_gain, mlp_gain)


def per_device(
    hidden_in,
    out_cotangent,
    attn_norm_gain,
    attn_norm_bias,
    mlp_norm_gain,
    mlp_norm_bias,
    qkv_weight,
    qkv_bias,
    proj_weight,
    proj_bias,
    up_weight,
    up_bias,
    down_weight,
    down_bias,
):
    sizes = [lax.axis_size(a) for a in ("seq", "tensor", "fsdp")]
    flat = [
        v.reshape(1, -1)
        for v in (attn_norm_gain, attn_norm_bias, mlp_norm_gain, mlp_norm_bias, qkv_bias, up_bias)
    ]
    first = first_call(
        *sizes,
        (hidden_in, out_cotangent, qkv_weight, proj_weight, up_weight, down_weight),
        flat,
    )
    proj, down, qkv, up, branch, norm, gains, qkv_bias_grad, up_bias_grad, out_bias_grad = (
        second_call(*sizes, first, out_cotangent, flat[0], flat[2], qkv_weight.shape[0])
    )
    hidden_out = bf(f32(hidden_in) + branch + proj_bias + down_bias)
    input_grad = bf(f32(out_cotangent) + norm)
    out_bias_grad = out_bias_grad.reshape(-1)
    return (
        hidden_out,
        input_grad,
        gains[0],
        gains[1],
        gains[2],
        gains[3],
        f32(qkv),
        qkv_bias_grad.reshape(-1),
        f32(proj),
        out_bias_grad,
        f32(up),
        up_bias_grad.reshape(-1),
        f32(down),
        out_bias_grad,
    )


def solution(mesh):
    matrix = P(("seq", "fsdp"), "tensor")
    vector = P("tensor")
    return jax.shard_map(
        per_device,
        mesh=mesh,
        in_specs=(
            matrix, matrix, P(), P(), P(), P(),
            matrix, vector, matrix, vector, matrix, vector, matrix, vector,
        ),
        out_specs=(
            matrix, matrix, P(), P(), P(), P(),
            matrix, vector, matrix, vector, matrix, vector, matrix, vector,
        ),
        check_vma=False,
    )
```

```python
import functools
import math

import jax
import jax.numpy as jnp
import numpy as np
from jax import lax
from jax.experimental import pallas as pl
from jax.experimental.pallas import tpu as pltpu
from jax.sharding import PartitionSpec as P

HEAD_DIM = 256
ROT = 64
LANES = 128
STRIP = 256
TOKEN_PARTS = 4
MESH = pl.DeviceIdType.MESH
VMEM_BYTES = 67_043_328

norm_eps = 1e-05
rope_base = 10000.0


def bits_of(size):
    return [1 << b for b in range(size.bit_length() - 1)]


def bf(value):
    return value.astype(jnp.bfloat16)


def f32(value):
    return value.astype(jnp.float32)


def mm(left, right, left_dim, right_dim):
    return lax.dot_general(
        left, right, (((left_dim,), (right_dim,)), ((), ())), preferred_element_type=jnp.float32
    )


def rotary_tables(tok, blocks):
    half = ROT // 2
    frequency = rope_base ** (-np.arange(half, dtype=np.float64) * 2.0 / ROT)
    lanes = np.zeros(LANES)
    lanes[:half] = frequency
    lanes[half:ROT] = frequency
    inner = np.arange(tok, dtype=np.float64)[:, None] * lanes
    outer = np.arange(blocks, dtype=np.float64)[:, None] * tok * lanes
    pack = lambda a: np.stack([np.cos(a), np.sin(a)]).astype(np.float32)
    return (jnp.asarray(pack(inner)), jnp.asarray(pack(outer)))


def flip(rank, mask, size):
    out = jnp.int32(0)
    for b in range(size.bit_length() - 1):
        digit = lax.rem(lax.div(rank, jnp.int32(1 << b)), jnp.int32(2))
        out = out + ((1 - digit) if mask >> b & 1 else digit) * (1 << b)
    return out


def low_bit(j, size):
    return j & -j if j else size


def line_mask(j):
    mask = 0
    b = 0
    while j >> b:
        if j >> b & 1:
            mask ^= (2 << b) - 1
        b += 1
    return mask


def arrivals(size):
    return sorted(range(1, size), key=lambda j: (-low_bit(j, size), j))


def slot_of(j, bit, size):
    index = 0
    for jj in range(size):
        for bb in bits_of(size):
            if bb < low_bit(jj, size):
                if (jj, bb) == (j, bit):
                    return index
                index += 1
    raise ValueError


def at(index, size):
    return pl.ds(pl.multiple_of(index * size, size), size)


def greet(S, T, F, z, y, f):
    barrier = pltpu.get_barrier_semaphore()
    peers = [{"seq": flip(z, k, S)} for k in range(1, S)]
    peers += [{"tensor": flip(y, t, T)} for t in range(1, T)]
    peers += [{"fsdp": flip(f, b, F)} for b in bits_of(F)]
    for peer in peers:
        pl.semaphore_signal(barrier, inc=1, device_id=peer, device_id_type=MESH)
    pl.semaphore_wait(barrier, len(peers))


def remote(src, dst, send, recv, peer):
    return pltpu.make_async_remote_copy(
        src_ref=src, dst_ref=dst, send_sem=send, recv_sem=recv, device_id=peer, device_id_type=MESH
    )


def repeat(count, body):
    def step(i, carry):
        body(i)
        return carry

    lax.fori_loop(0, count, step, 0)


def turn(value, cos_part, sin_part):
    half = ROT // 2
    head = value[:, :LANES]
    lane = lax.broadcasted_iota(jnp.int32, head.shape, 1)
    other = jnp.where(
        lane < half, -pltpu.roll(head, LANES - half, 1), pltpu.roll(head, half, 1)
    )
    return jnp.concatenate([head * cos_part + other * sin_part, value[:, LANES:]], axis=1)


def first_kernel(S, T, F, *refs):
    hid_in, cot_in, wq_in, wp_in, wu_in, wd_in = refs[:6]
    attn_gain, attn_bias, mlp_gain, mlp_bias, qkv_bias, up_bias, inner, outer = refs[6:14]
    hid_o, cot_o, attn_in_o, mlp_in_o, stat_o, wq_o, wp_o, wu_o, wd_o = refs[14:23]
    attn_o, active_o, slope_o, tg_o, proj_o = refs[23:28]
    hid, cot, attn_in, mlp_in, stat, wq, wp, wu, wd = refs[28:37]
    attn, active, slope, tg, proj = refs[37:42]
    query, pair, attn_grad, probs, score_grad, row_info, part_in = refs[42:49]
    proj_full, proj_out, proj_in = refs[49:52]
    own_sem, out_sem, tok_send, tok_recv, row_send, row_recv = refs[52:58]
    pair_send, pair_recv, part_send, part_recv, proj_send, proj_recv = refs[58:64]
    z, y, f = lax.axis_index("seq"), lax.axis_index("tensor"), lax.axis_index("fsdp")
    fbits = bits_of(F)
    tok, width = hid_in.shape
    ntok, D = hid.shape
    rows = wq_in.shape[0]
    keys = pair.shape[0]
    scale = HEAD_DIM ** (-0.5)
    tokens = ((hid_in, hid), (cot_in, cot))
    half = wu.shape[1] // 2
    parts = TOKEN_PARTS
    weights = (
        (wq_in, wq, 0, wq.shape[1]),
        (wp_in, wp, 0, wp.shape[1]),
        (wu_in, wu, 0, half),
        (wu_in, wu, half, half),
        (wd_in, wd, 0, half),
        (wd_in, wd, half, half),
    )
    sends, pair_sends = [], []

    def start(copy):
        copy.start()
        sends.append(copy)

    def tok_sem(a, j, t, part):
        return ((a * S + j) * T + t) * parts + part

    def tok_place(a, j, t):
        return tokens[a][1].at[at(flip(z, line_mask(j), S), tok), at(flip(y, t, T), width)]

    def tok_split(j, t):
        size = tok // parts if t == 0 else tok
        return [(p, slice(p * size, (p + 1) * size)) for p in range(tok // size)]

    def tok_seq(a, j):
        src = tokens[a][0] if j == 0 else tok_place(a, j, 0)
        dst = tok_place(a, j, 0)
        for b in reversed(bits_of(S)):
            if b < low_bit(j, S):
                peer = {"seq": flip(z, line_mask(b), S)}
                for p, here in tok_split(j + b, 0):
                    i = tok_sem(a, j + b, 0, p)
                    start(remote(src.at[here], dst.at[here], tok_send.at[i], tok_recv.at[i], peer))

    def tok_forward(a, j):
        tok_seq(a, j)
        tok_tensor(a, j)

    def tok_tensor(a, j):
        src = tokens[a][0] if j == 0 else tok_place(a, j, 0)
        dst = tok_place(a, j, 0)
        for t in range(1, T):
            i = tok_sem(a, j, t, 0)
            peer = {"tensor": flip(y, t, T)}
            start(remote(src, dst, tok_send.at[i], tok_recv.at[i], peer))

    def tok_wait(a, j, t):
        spot = tok_place(a, j, t)
        for p, here in tok_split(j, t):
            i = tok_sem(a, j, t, p)
            part = spot.at[here]
            peer = {"tensor": flip(y, 1, T)}
            remote(part, part, tok_send.at[i], tok_recv.at[i], peer).wait_recv()

    def tok_direct(a):
        for j in sorted(bits_of(S)):
            tok_wait(a, j, 0)
            tok_forward(a, j)

    def tok_passed(a):
        for j in arrivals(S):
            if j not in bits_of(S):
                tok_wait(a, j, 0)
                tok_forward(a, j)

    def tok_rest(a):
        tok_own(a).wait()
        for j in range(S):
            for t in range(1, T):
                tok_wait(a, j, t)

    def tok_own(a):
        return pltpu.make_async_copy(tokens[a][0], tok_place(a, 0, 0), own_sem.at[a])

    def row_sem(m, k, j):
        return (m * S + k) * F + j

    def row_place(m, k, j):
        _, dst, first, size = weights[m]
        return dst.at[at(flip(z, k, S) * F + flip(f, j, F), rows), first : first + size]

    def row_source(m, zd):
        src, dst, first, size = weights[m]
        return src.at[:, pl.ds(pl.multiple_of(zd * dst.shape[1] + first, LANES), size)]

    def row_seq(m):
        for k in range(1, S):
            i = row_sem(m, k, 0)
            zd = flip(z, k, S)
            start(
                remote(
                    row_source(m, zd), row_place(m, 0, 0), row_send.at[i], row_recv.at[i], {"seq": zd}
                )
            )

    def row_forward(m, k, j):
        dst = row_place(m, k, j)
        src = row_source(m, z) if k == 0 and j == 0 else dst
        for b in reversed(fbits):
            if b < low_bit(j, F):
                i = row_sem(m, k, j + b)
                peer = {"fsdp": flip(f, b, F)}
                start(remote(src, dst, row_send.at[i], row_recv.at[i], peer))

    def row_wait(m, k, j):
        i = row_sem(m, k, j)
        spot = row_place(m, k, j)
        remote(spot, spot, row_send.at[i], row_recv.at[i], {"seq": flip(z, 1, S)}).wait_recv()

    def row_own(m):
        return pltpu.make_async_copy(row_source(m, z), row_place(m, 0, 0), own_sem.at[2 + m])

    def row_arrive(m):
        for k in range(1, S):
            row_wait(m, k, 0)
            row_forward(m, k, 0)

    def row_relay(m):
        for j in arrivals(F):
            if low_bit(j, F) > 1:
                for k in range(S):
                    row_wait(m, k, j)
                    row_forward(m, k, j)

    def row_rest(m):
        row_own(m).wait()
        for j in arrivals(F):
            if low_bit(j, F) == 1:
                for k in range(S):
                    row_wait(m, k, j)

    def pair_place(zd, j):
        return pair.at[at(zd * F + flip(f, j, F), tok), :]

    def pair_forward(zd, j):
        spot = pair_place(zd, j)
        for b in reversed(fbits):
            if b < low_bit(j, F):
                i = zd * F + j + b
                peer = {"fsdp": flip(f, b, F)}
                copy = remote(spot, spot, pair_send.at[i], pair_recv.at[i], peer)
                copy.start()
                pair_sends.append(copy)

    def pair_wait(zd, j):
        i = zd * F + j
        spot = pair_place(zd, j)
        remote(spot, spot, pair_send.at[i], pair_recv.at[i], {"fsdp": flip(f, 1, F)}).wait_recv()

    outs = []

    def put(src, dst):
        copy = pltpu.make_async_copy(src, dst, out_sem.at[len(outs)])
        copy.start()
        outs.append(copy)

    greet(S, T, F, z, y, f)
    tok_seq(0, 0)
    tok_tensor(0, 0)
    for m in range(4):
        row_forward(m, 0, 0)
    for a in range(2):
        tok_own(a).start()
    for m in range(6):
        row_own(m).start()

    tok_direct(0)
    row_seq(0)
    tok_passed(0)
    row_seq(2)
    tok_tensor(1, 0)
    for m in (4, 5):
        row_forward(m, 0, 0)
    tok_rest(0)
    put(hid, hid_o)
    chunk = 32

    def norm_chunk(i):
        part = at(i, chunk)
        x = f32(hid[part, :])
        mean = jnp.mean(x, axis=-1, keepdims=True)
        centered = x - mean
        inv_std = lax.rsqrt(jnp.mean(centered * centered, axis=-1, keepdims=True) + norm_eps)
        xhat = centered * inv_std
        attn_in[part, :] = bf(xhat * attn_gain[...] + attn_bias[...])
        mlp_in[part, :] = bf(xhat * mlp_gain[...] + mlp_bias[...])
        stat[0, part, :] = jnp.broadcast_to(mean, (chunk, LANES))
        stat[1, part, :] = jnp.broadcast_to(inv_std, (chunk, LANES))

    repeat(ntok // chunk, norm_chunk)
    put(attn_in, attn_in_o)
    put(mlp_in, mlp_in_o)
    put(stat, stat_o)

    def angles(zd, here=slice(None)):
        block = pl.ds(zd * F + f, 1)
        cos_in, sin_in = inner[0, here, :], inner[1, here, :]
        cos_out, sin_out = outer[0, block, :], outer[1, block, :]
        return (cos_in * cos_out - sin_in * sin_out, sin_in * cos_out + cos_in * sin_out)

    row_arrive(0)
    tok_seq(1, 0)
    row_relay(0)
    row_rest(0)
    put(wq, wq_o)
    bias = qkv_bias[:, at(z, 3 * HEAD_DIM)]
    for c in range(3):
        part = mm(attn_in[...], wq[:, c * HEAD_DIM : (c + 1) * HEAD_DIM], 1, 0)
        part = part + bias[:, c * HEAD_DIM : (c + 1) * HEAD_DIM]
        for zd in range(S):
            piece = part[zd * tok : (zd + 1) * tok]
            if c < 2:
                piece = turn(piece, *angles(zd))
            if c == 0:
                query[zd * tok : (zd + 1) * tok, :] = bf(piece)
            else:
                spot = at(zd * F + f, tok)
                pair[spot, (c - 1) * HEAD_DIM : c * HEAD_DIM] = bf(piece)
    for zd in range(S):
        pair_forward(zd, 0)

    row_arrive(2)
    row_seq(3)
    tok_direct(1)
    row_seq(1)
    row_relay(2)
    for j in arrivals(F):
        if low_bit(j, F) > 1:
            for zd in range(S):
                pair_wait(zd, j)
                pair_forward(zd, j)
    tok_passed(1)
    row_seq(4)
    row_arrive(3)
    row_arrive(1)
    for j in arrivals(F):
        if low_bit(j, F) == 1:
            for zd in range(S):
                pair_wait(zd, j)

    qc = max(32, min(tok, tok * 2048 // keys))

    def masked_scores(zd, i, n):
        start_row = zd * tok + i * qc
        q = query[pl.ds(pl.multiple_of(start_row, qc), qc), :]
        scores = mm(q, pair[:n, :HEAD_DIM], 1, 1) * scale
        last = (zd * F + f) * tok + i * qc
        ahead = lax.broadcasted_iota(jnp.int32, scores.shape, 1) - lax.broadcasted_iota(
            jnp.int32, scores.shape, 0
        )
        return (scores, ahead <= last)

    for zd in range(S):
        n = (zd + 1) * F * tok

        def forward_chunk(i, zd=zd, n=n):
            here = pl.ds(pl.multiple_of(zd * tok + i * qc, qc), qc)
            scores, allowed = masked_scores(zd, i, n)
            top = jnp.max(jnp.where(allowed, scores, -1e30), axis=-1, keepdims=True)
            terms = jnp.where(allowed, jnp.exp(scores - top), 0.0)
            total = jnp.sum(terms, axis=-1, keepdims=True)
            mixed = mm(bf(terms), pair[:n, HEAD_DIM:], 1, 0) / total
            attn[here, :] = bf(mixed)
            row_info[here, :] = jnp.broadcast_to(top + jnp.log(total), (qc, LANES))

        repeat(tok // qc, forward_chunk)
    put(attn, attn_o)

    row_seq(5)
    row_relay(1)
    tok_rest(1)
    put(cot, cot_o)
    row_rest(1)
    put(wp, wp_o)
    attn_grad[...] = bf(mm(cot[...], wp[...], 1, 0))
    for zd in range(S):
        n = (zd + 1) * F * tok

        def backward_chunk(i, zd=zd, n=n):
            here = pl.ds(pl.multiple_of(zd * tok + i * qc, qc), qc)
            scores, allowed = masked_scores(zd, i, n)
            weights_here = jnp.where(allowed, jnp.exp(scores - row_info[here, :1]), 0.0)
            grad = attn_grad[here, :]
            delta = jnp.sum(f32(grad) * f32(attn[here, :]), axis=-1, keepdims=True)
            slopes = mm(grad, pair[:n, HEAD_DIM:], 1, 1)
            inner_grad = bf(weights_here * (slopes - delta))
            probs[here, :n] = bf(weights_here)
            score_grad[here, :n] = inner_grad
            if n < keys:
                blank = jnp.zeros((qc, keys - n), jnp.bfloat16)
                probs[here, n:] = blank
                score_grad[here, n:] = blank
            cos_part, sin_part = angles(zd, pl.ds(pl.multiple_of(i * qc, qc), qc))
            grad_here = mm(inner_grad, pair[:n, :HEAD_DIM], 1, 0) * scale
            tg[here, :HEAD_DIM] = bf(turn(grad_here, cos_part, -sin_part))

        repeat(tok // qc, backward_chunk)

    def part_sum(j):
        def lanes(ref):
            return jnp.concatenate(
                [ref[:, at(zd * F + flip(f, j, F), tok)] for zd in range(S)], axis=1
            )

        total = jnp.concatenate(
            [mm(lanes(score_grad), query[...], 0, 0) * scale, mm(lanes(probs), attn_grad[...], 0, 0)],
            axis=1,
        )
        for b in fbits:
            if b < low_bit(j, F):
                i = slot_of(j, b, F)
                spot = part_in.at[i]
                peer = {"fsdp": flip(f, b, F)}
                remote(spot, spot, part_send.at[i], part_recv.at[i], peer).wait_recv()
                total = total + f32(part_in[i])
        return total

    for copy in pair_sends:
        copy.wait_send()

    def part_stage(bit):
        for j in range(1, F):
            if low_bit(j, F) == bit:
                spot = pair.at[(j - 1) * ntok : j * ntok, :]
                pair[(j - 1) * ntok : j * ntok, :] = bf(part_sum(j))
                i = slot_of(j - bit, bit, F)
                peer = {"fsdp": flip(f, bit, F)}
                start(remote(spot, part_in.at[i], part_send.at[j - 1], part_recv.at[i], peer))

    def proj_sum(j):
        total = jnp.concatenate(
            [proj_full[at(zd * F + flip(f, j, F), rows), :] for zd in range(S)], axis=0
        )
        for b in fbits:
            if b < low_bit(j, F):
                i = slot_of(j, b, F)
                spot = proj_in.at[i]
                peer = {"fsdp": flip(f, b, F)}
                remote(spot, spot, proj_send.at[i], proj_recv.at[i], peer).wait_recv()
                total = total + f32(proj_in[i])
        return total

    def proj_stage(bit):
        for j in range(1, F):
            if low_bit(j, F) == bit:
                proj_out[j - 1] = bf(proj_sum(j))
                i = slot_of(j - bit, bit, F)
                peer = {"fsdp": flip(f, bit, F)}
                there = proj_in.at[i]
                start(remote(proj_out.at[j - 1], there, proj_send.at[j - 1], proj_recv.at[i], peer))

    part_stage(fbits[0])
    proj_full[...] = mm(cot[...], attn[...], 0, 0)
    proj_stage(fbits[0])
    row_arrive(4)
    for bit in fbits[1:]:
        part_stage(bit)
    for bit in fbits[1:]:
        proj_stage(bit)
    row_rest(2)

    cols = wu.shape[1]

    def up_strips(first):
        for n in range(first // STRIP, (first + half) // STRIP):
            strip = slice(n * STRIP, (n + 1) * STRIP)
            mid = mm(mlp_in[...], wu[:, strip], 1, 0) + up_bias[
                :, pl.ds(pl.multiple_of(z * cols + n * STRIP, STRIP), STRIP)
            ]
            cdf = 0.5 * (1.0 + lax.erf(mid * 0.7071067811865476))
            active[:, strip] = bf(mid * cdf)
            slope[:, strip] = cdf + mid * jnp.exp(-0.5 * mid * mid) * 0.3989422804014327

    up_strips(0)
    row_relay(3)
    row_arrive(5)
    row_rest(3)
    put(wu, wu_o)
    up_strips(half)
    put(active, active_o)
    put(slope, slope_o)
    total = part_sum(0)
    for zd in range(S):
        here = slice(zd * tok, (zd + 1) * tok)
        cos_part, sin_part = angles(zd)
        tg[here, HEAD_DIM : 2 * HEAD_DIM] = bf(turn(total[here, :HEAD_DIM], cos_part, -sin_part))
        tg[here, 2 * HEAD_DIM :] = bf(total[here, HEAD_DIM:])
    put(tg, tg_o)
    row_relay(4)
    proj[...] = bf(proj_sum(0))
    put(proj, proj_o)
    row_rest(4)
    row_relay(5)
    row_rest(5)
    put(wd, wd_o)
    for copy in outs:
        copy.wait()
    for copy in sends:
        copy.wait_send()


def first_call(S, T, F, arrays, vectors):
    hidden, _, wq, wp, wu, _ = arrays
    tok, width = hidden.shape
    rows = wq.shape[0]
    ntok, D, keys = S * tok, T * width, S * F * tok
    if width != S * HEAD_DIM or S * F * rows != D:
        raise ValueError
    small, wide = jnp.bfloat16, jnp.float32
    ff = wu.shape[1] // S
    inner, outer = rotary_tables(tok, S * F)
    outs = [((ntok, D), small)] * 4 + [((2, ntok, LANES), wide)]
    outs += [((D, w.shape[1] // S), small) for w in arrays[2:]]
    outs += [((ntok, HEAD_DIM), small), ((ntok, ff), small), ((ntok, ff), wide)]
    outs += [((ntok, 3 * HEAD_DIM), small), ((S * rows, HEAD_DIM), small)]
    n_part = max(F - 1, 1)
    scratch = outs + [
        ((ntok, HEAD_DIM), small),
        ((keys, 2 * HEAD_DIM), small),
        ((ntok, HEAD_DIM), small),
        ((ntok, keys), small),
        ((ntok, keys), small),
        ((ntok, LANES), wide),
        ((n_part, ntok, 2 * HEAD_DIM), small),
        ((D, HEAD_DIM), wide),
        ((n_part, S * rows, HEAD_DIM), small),
        ((n_part, S * rows, HEAD_DIM), small),
    ]
    dma = pltpu.SemaphoreType.DMA
    any_spec = pl.BlockSpec(memory_space=pl.ANY)
    vmem = pl.BlockSpec(memory_space=pltpu.VMEM)
    return pl.pallas_call(
        functools.partial(first_kernel, S, T, F),
        out_shape=[jax.ShapeDtypeStruct(*o) for o in outs],
        in_specs=[any_spec] * 6 + [vmem] * 8,
        out_specs=[any_spec] * len(outs),
        scratch_shapes=[pltpu.VMEM(*o) for o in scratch]
        + [
            dma((8,)),
            dma((len(outs),)),
            dma((2 * S * T * TOKEN_PARTS,)),
            dma((2 * S * T * TOKEN_PARTS,)),
            dma((6 * S * F,)),
            dma((6 * S * F,)),
            dma((S * F,)),
            dma((S * F,)),
            dma((n_part,)),
            dma((n_part,)),
            dma((n_part,)),
            dma((n_part,)),
        ],
        compiler_params=pltpu.CompilerParams(
            collective_id=0, has_side_effects=True, vmem_limit_bytes=VMEM_BYTES
        ),
    )(*arrays, *vectors, inner, outer)


def second_units(ff):
    half = ff // 2
    return (
        (0, 0, HEAD_DIM),
        (1, 0, half),
        (1, half, half),
        (2, 0, 3 * HEAD_DIM),
        (3, 0, half),
        (3, half, half),
    )


def second_kernel(S, T, F, turned, *refs):
    cot_i, hid_i, attn_in_i, mlp_in_i, stat_i, wq_i, wp_i, wu_i, wd_i = refs[:9]
    attn_i, active_i, slope_i, tg_i, proj_i, own_cot, attn_gain, mlp_gain = refs[9:17]
    grads, refs = refs[17:21], refs[21:]
    homes, (gain_o, qkv_bias_o, up_bias_o, out_bias_o), refs = refs[:2], refs[2:6], refs[6:]
    cot, hid, attn_in, mlp_in, stat, wq, wp, wud, attn, active, tg, pre = refs[:12]
    wide, own_half, sums, vec, vec_in, vec_seq, vec_ten = refs[12:19]
    n_u = len(second_units(1))
    out_b, in_b = (None, *refs[19 : 18 + n_u]), (None, *refs[18 + n_u : 17 + 2 * n_u])
    seq_b, refs = refs[17 + 2 * n_u : 17 + 3 * n_u], refs[17 + 3 * n_u :]
    y_out, y_in, z_out, z_in, home_v = refs[:5]
    load_sem, own_sem, out_sem, in_sem, seq_send, seq_recv = refs[5:11]
    y_send, y_recv, z_send, z_recv, v_send, v_recv = refs[11:17]
    z, y, f = lax.axis_index("seq"), lax.axis_index("tensor"), lax.axis_index("fsdp")
    fbits, sbits = bits_of(F), bits_of(S)
    tok, width = homes[0].shape
    ntok, D = wide.shape
    ff = active.shape[1]
    rights, lefts = (attn, active, tg, pre), (cot, cot, attn_in, mlp_in)
    units = second_units(ff)
    P1, D1, D2, Q1, U1, U2 = range(n_u)
    sends = []

    def start(copy):
        copy.start()
        sends.append(copy)

    loads = {}

    def load(name, src, dst):
        loads[name] = pltpu.make_async_copy(src, dst, load_sem.at[len(loads)])
        loads[name].start()

    waited = set()

    def need(*names):
        for name in names:
            if name not in waited:
                waited.add(name)
                loads[name].wait()

    load("proj", proj_i, seq_b[0])
    load("active", active_i, active)
    load("wd", wd_i, wud)
    load("attn", attn_i, attn)
    load("wp", wp_i, wp)
    load("cot", cot_i, cot)
    load("slope", slope_i, wide.at[:, :ff])
    load("tg", tg_i, tg)
    load("attn_in", attn_in_i, attn_in)
    load("wq", wq_i, wq)
    load("hid", hid_i, hid)
    load("stat", stat_i, stat)
    load("mlp_in", mlp_in_i, mlp_in)

    greet(S, T, F, z, y, f)

    def block_sum(u, j):
        g, first, size = units[u]
        right, left = rights[g].at[:, first : first + size], lefts[g]
        rows = grads[g].shape[0]
        fd = flip(f, j, F)
        if turned:
            block = jnp.concatenate([left[at(zd * F + fd, rows), :] for zd in range(S)], axis=0)
            total = mm(block, right[...], 1, 0)
        else:
            block = jnp.concatenate([left[:, at(zd * F + fd, rows)] for zd in range(S)], axis=1)
            total = mm(block, right[...], 0, 0)
        for bit in fbits:
            if bit < low_bit(j, F):
                s = slot_of(j, bit, F)
                i = u * (F - 1) + s
                spot = in_b[u].at[s]
                peer = {"fsdp": flip(f, bit, F)}
                remote(spot, spot, out_sem.at[i], in_sem.at[i], peer).wait_recv()
                total = total + f32(in_b[u][s])
        return total

    def fsdp_stage(u, bit):
        for j in range(1, F):
            if low_bit(j, F) == bit:
                out_b[u][j - 1] = bf(block_sum(u, j))
                there = slot_of(j - bit, bit, F)
                start(
                    remote(
                        out_b[u].at[j - 1],
                        in_b[u].at[there],
                        out_sem.at[u * (F - 1) + j - 1],
                        in_sem.at[u * (F - 1) + there],
                        {"fsdp": flip(f, bit, F)},
                    )
                )

    def grad_place(u, zd):
        g, first, size = units[u]
        start_col = zd * rights[g].shape[1] + first
        return grads[g].at[:, pl.ds(pl.multiple_of(start_col, LANES), size)]

    def own_grad(u):
        rows = grads[0].shape[0]
        return pltpu.make_async_copy(seq_b[u].at[at(z, rows), :], grad_place(u, z), own_sem.at[u])

    def seq_stage(u):
        rows = grads[0].shape[0]
        if u == P1:
            need("proj")
        else:
            seq_b[u][...] = bf(block_sum(u, 0))
        for k in range(1, S):
            peer = flip(z, k, S)
            start(
                remote(
                    seq_b[u].at[at(peer, rows), :],
                    grad_place(u, z),
                    seq_send.at[u * S + k],
                    seq_recv.at[u * S + k],
                    {"seq": peer},
                )
            )
        own_grad(u).start()

    def seq_wait(u):
        for k in range(1, S):
            spot = grad_place(u, flip(z, k, S))
            i = u * S + k
            remote(spot, spot, seq_send.at[i], seq_recv.at[i], {"seq": flip(z, k, S)}).wait_recv()
        own_grad(u).wait()

    def y_index(s, t, zd):
        return (s * max(T - 1, 1) + t - 1) * S + zd

    def y_store(s, t, column, value):
        for zd in range(S):
            y_out[y_index(s, t, zd), :, column] = bf(value[zd * tok : (zd + 1) * tok])

    def tensor_send(s):
        for j in [*sorted(range(1, S), key=lambda j: (low_bit(j, S), j)), 0]:
            zd = flip(z, line_mask(j), S)
            for t in range(1, T):
                i = y_index(s, t, 0) + j
                peer = {"tensor": flip(y, t, T)}
                here = y_out.at[y_index(s, t, zd)]
                start(remote(here, y_in.at[i], y_send.at[i], y_recv.at[i], peer))

    def token_part(s, j):
        zd = flip(z, line_mask(j), S)
        total = own_half[s, at(zd, tok), :]
        for t in range(1, T):
            i = y_index(s, t, 0) + j
            spot = y_in.at[i]
            remote(spot, spot, y_send.at[i], y_recv.at[i], {"tensor": flip(y, t, T)}).wait_recv()
            total = total + f32(y_in[i])
        for bit in sbits:
            if bit < low_bit(j, S):
                i = s * (S - 1) + slot_of(j, bit, S)
                spot = z_in.at[i]
                peer = {"seq": flip(z, line_mask(bit), S)}
                remote(spot, spot, z_send.at[i], z_recv.at[i], peer).wait_recv()
                total = total + f32(z_in[i])
        return total

    def token_stage(s, bit):
        for j in range(1, S):
            if low_bit(j, S) == bit:
                i = s * (S - 1) + j - 1
                there = s * (S - 1) + slot_of(j - bit, bit, S)
                z_out[i] = bf(token_part(s, j))
                peer = {"seq": flip(z, line_mask(bit), S)}
                start(remote(z_out.at[i], z_in.at[there], z_send.at[i], z_recv.at[there], peer))

    def home_copy(s):
        return pltpu.make_async_copy(home_v.at[s], homes[s], own_sem.at[n_u + s])

    def token_home(s):
        home_v[s] = token_part(s, 0)
        home_copy(s).start()

    def vec_exchange(i, dst, peer):
        return remote(vec.at[i], dst, v_send.at[i], v_recv.at[i], peer)

    n_fsdp = len(fbits)

    def vec_fsdp(b):
        start(vec_exchange(b, vec_in.at[b], {"fsdp": flip(f, fbits[b], F)}))

    def vec_fsdp_sum(b):
        vec_exchange(b, vec_in.at[b], {"fsdp": flip(f, fbits[b], F)}).wait_recv()
        vec[b + 1] = vec[b] + vec_in[b]

    def vec_seq_copy(k):
        peer = {"seq": flip(z, k, S)}
        i = n_fsdp + k - 1
        return remote(vec.at[n_fsdp], vec_seq.at[k - 1], v_send.at[i], v_recv.at[i], peer)

    def vec_seq_sum():
        qkv_bias_o[:, at(z, 3 * HEAD_DIM)] = vec[n_fsdp, 4:5, : 3 * HEAD_DIM]
        up_bias_o[:, at(z, ff)] = vec[n_fsdp, 5:6, :ff]
        parts = [vec[n_fsdp]]
        for k in range(1, S):
            vec_seq_copy(k).wait_recv()
            zd = flip(z, k, S)
            qkv_bias_o[:, at(zd, 3 * HEAD_DIM)] = vec_seq[k - 1, 4:5, : 3 * HEAD_DIM]
            up_bias_o[:, at(zd, ff)] = vec_seq[k - 1, 5:6, :ff]
            parts.append(vec_seq[k - 1])
        while len(parts) > 1:
            parts = [a + b for a, b in zip(parts[::2], parts[1::2])]
        out_bias_o[...] = parts[0][6:7, :width]
        vec_ten[0] = parts[0][:4]

    def vec_ten_copy(t):
        peer = {"tensor": flip(y, t, T)}
        i = n_fsdp + S - 1 + t - 1
        return remote(vec_ten.at[0], vec_ten.at[t], v_send.at[i], v_recv.at[i], peer)

    def vec_ten_sum():
        parts = [vec_ten[0]]
        for t in range(1, T):
            vec_ten_copy(t).wait_recv()
            parts.append(vec_ten[t])
        while len(parts) > 1:
            parts = [a + b for a, b in zip(parts[::2], parts[1::2])]
        gain_o[...] = parts[0]

    first_stage = lambda u: fsdp_stage(u, fbits[0])

    def later_stages(u):
        for bit in fbits[1:]:
            fsdp_stage(u, bit)

    def later_tokens(s):
        for bit in sbits[1:]:
            token_stage(s, bit)

    def half_strips(s, t, term):
        for n in range(width // STRIP):
            there = pl.ds(pl.multiple_of(flip(y, t, T) * width + n * STRIP, STRIP), STRIP)
            here = slice(n * STRIP, (n + 1) * STRIP)
            if t:
                y_store(s, t, here, term(there))
            else:
                own_half[s, :, here] = term(there)

    seq_stage(P1)
    vec[0] = jnp.zeros(vec.shape[1:], jnp.float32)
    need("active", "wd", "attn", "wp")

    def branch(column):
        return mm(active[...], wud[column, :], 1, 1) + mm(attn[...], wp[column, :], 1, 1)

    for t in range(1, T):
        half_strips(0, t, branch)
    tensor_send(0)
    need("cot")
    first_stage(D1)
    half_strips(0, 0, branch)
    later_stages(D1)
    first_stage(D2)

    need("slope")
    for n in range(ff // STRIP):
        here = slice(n * STRIP, (n + 1) * STRIP)
        value = mm(cot[...], wud[:, here], 0 if turned else 1, 0) * wide[:, here]
        vec[0, 5:6, here] = jnp.sum(value, axis=0, keepdims=True)
        pre[:, here] = bf(value)
    load("wu", wu_i, wud)
    token_stage(0, sbits[0])
    need("tg", "attn_in")
    first_stage(Q1)
    later_stages(D2)
    need("mlp_in")
    first_stage(U1)
    first_stage(U2)

    need("wu", "wq", "hid", "stat")
    lane_parts = range(0, STRIP, LANES)

    def norm_strip(n):
        here = at(n, STRIP)
        a = mm(tg[...], wq[here, :], 1, 1)
        m = mm(pre[...], wud[here, :], 1, 1)
        mean, inv_std = stat[0, :, :1], stat[1, :, :1]
        xhat = (f32(hid[:, here]) - mean) * inv_std
        vec[0, 0:1, here] = jnp.sum(a * xhat, axis=0, keepdims=True)
        vec[0, 1:2, here] = jnp.sum(a, axis=0, keepdims=True)
        vec[0, 2:3, here] = jnp.sum(m * xhat, axis=0, keepdims=True)
        vec[0, 3:4, here] = jnp.sum(m, axis=0, keepdims=True)
        both = a * attn_gain[:, here] + m * mlp_gain[:, here]
        wide[:, here] = both
        scaled = both * xhat
        sums[0] += sum(both[:, c : c + LANES] for c in lane_parts)
        sums[1] += sum(scaled[:, c : c + LANES] for c in lane_parts)

    sums[...] = jnp.zeros_like(sums)
    repeat(D // STRIP, norm_strip)
    vec[0, 4:5, : 3 * HEAD_DIM] = jnp.sum(f32(tg[...]), axis=0, keepdims=True)
    vec[0, 6:7, :width] = jnp.sum(f32(own_cot[...]), axis=0, keepdims=True)
    vec_fsdp(0)
    seq_stage(D1)
    later_stages(Q1)
    sums[0] = jnp.broadcast_to(jnp.sum(sums[0], axis=-1, keepdims=True) / D, sums.shape[1:])
    sums[1] = jnp.broadcast_to(jnp.sum(sums[1], axis=-1, keepdims=True) / D, sums.shape[1:])

    def input_term(column):
        mean, inv_std = stat[0, :, :1], stat[1, :, :1]
        xhat = (f32(hid[:, column]) - mean) * inv_std
        return inv_std * (wide[:, column] - sums[0, :, :1] - xhat * sums[1, :, :1])

    for t in range(1, T):
        half_strips(1, t, input_term)
    tensor_send(1)
    half_strips(1, 0, input_term)
    later_tokens(0)
    seq_stage(D2)
    later_stages(U1)
    vec_fsdp_sum(0)
    for b in range(1, n_fsdp):
        vec_fsdp(b)
        if b < n_fsdp - 1:
            vec_fsdp_sum(b)
    seq_stage(Q1)
    later_stages(U2)
    token_stage(1, sbits[0])
    token_home(0)
    seq_stage(U1)
    if n_fsdp > 1:
        vec_fsdp_sum(n_fsdp - 1)
    for k in range(1, S):
        start(vec_seq_copy(k))
    seq_stage(U2)
    later_tokens(1)
    vec_seq_sum()
    for t in range(1, T):
        start(vec_ten_copy(t))
    vec_ten_sum()
    token_home(1)
    for u in range(n_u):
        seq_wait(u)
    for s in range(2):
        home_copy(s).wait()
    for copy in sends:
        copy.wait_send()


def second_call(S, T, F, first, own_cot, attn_gain, mlp_gain, rows):
    hid, cot, attn_in, mlp_in, stat, wq, wp, wu, wd, attn, active, slope, tg, proj = first
    turned = rows % LANES != 0
    if turned:
        cot, attn_in, mlp_in = cot.T, attn_in.T, mlp_in.T
    tok, width = own_cot.shape
    ntok, D = hid.shape
    ff = active.shape[1]
    small, wide = jnp.bfloat16, jnp.float32
    cols = (HEAD_DIM, ff, 3 * HEAD_DIM, ff)
    parts, block, n_f = max(F - 1, 1), S * rows, F.bit_length() - 1
    ins = (cot, hid, attn_in, mlp_in, stat, wq, wp, wu, wd, attn, active, slope, tg, proj)
    any_spec = pl.BlockSpec(memory_space=pl.ANY)
    vmem = pl.BlockSpec(memory_space=pltpu.VMEM)
    dma = pltpu.SemaphoreType.DMA
    shape = jax.ShapeDtypeStruct
    scratch = [(a.shape, small) for a in (cot, hid, attn_in, mlp_in)] + [(stat.shape, wide)]
    scratch += [(a.shape, small) for a in (wq, wp, wu, attn, active, tg)]
    scratch += [
        ((ntok, ff), small),
        ((ntok, D), wide),
        ((2, ntok, width), wide),
        ((2, ntok, LANES), wide),
        ((n_f + 1, 8, D), wide),
        ((n_f, 8, D), wide),
        ((max(S - 1, 1), 8, D), wide),
        ((T, 4, D), wide),
    ]
    chunks = [size for _, _, size in second_units(ff)]
    n_u = len(chunks)
    scratch += [((parts, block, c), small) for c in chunks[1:]] * 2
    scratch += [((block, c), small) for c in chunks]
    n_y, n_z, n_v = 2 * max(T - 1, 1) * S, 2 * max(S - 1, 1), n_f + S + T
    scratch += [((n_y, tok, width), small)] * 2 + [((n_z, tok, width), small)] * 2
    scratch += [((2, tok, width), wide)]
    return pl.pallas_call(
        functools.partial(second_kernel, S, T, F, turned),
        out_shape=[shape((rows, S * c), small) for c in cols]
        + [shape((tok, width), wide)] * 2
        + [shape((4, D), wide), shape((1, 3 * width), wide)]
        + [shape((1, S * ff), wide), shape((1, width), wide)],
        in_specs=[any_spec] * len(ins) + [vmem] * 3,
        out_specs=[any_spec] * 6 + [vmem] * 4,
        scratch_shapes=[pltpu.VMEM(*s) for s in scratch]
        + [
            dma((len(ins),)),
            dma((n_u + 2,)),
            dma((n_u * parts,)),
            dma((n_u * parts,)),
            dma((n_u * S,)),
            dma((n_u * S,)),
            dma((n_y,)),
            dma((n_y,)),
            dma((n_z,)),
            dma((n_z,)),
            dma((n_v,)),
            dma((n_v,)),
        ],
        compiler_params=pltpu.CompilerParams(
            collective_id=1, has_side_effects=True, vmem_limit_bytes=VMEM_BYTES
        ),
    )(*ins, own_cot, attn_gain, mlp_gain)


def per_device(
    hidden_in,
    out_cotangent,
    attn_norm_gain,
    attn_norm_bias,
    mlp_norm_gain,
    mlp_norm_bias,
    qkv_weight,
    qkv_bias,
    proj_weight,
    proj_bias,
    up_weight,
    up_bias,
    down_weight,
    down_bias,
):
    sizes = [lax.axis_size(a) for a in ("seq", "tensor", "fsdp")]
    flat = [
        v.reshape(1, -1)
        for v in (attn_norm_gain, attn_norm_bias, mlp_norm_gain, mlp_norm_bias, qkv_bias, up_bias)
    ]
    first = first_call(
        *sizes,
        (hidden_in, out_cotangent, qkv_weight, proj_weight, up_weight, down_weight),
        flat,
    )
    proj, down, qkv, up, branch, norm, gains, qkv_bias_grad, up_bias_grad, out_bias_grad = (
        second_call(*sizes, first, out_cotangent, flat[0], flat[2], qkv_weight.shape[0])
    )
    hidden_out = bf(f32(hidden_in) + branch + proj_bias + down_bias)
    input_grad = bf(f32(out_cotangent) + norm)
    out_bias_grad = out_bias_grad.reshape(-1)
    return (
        hidden_out,
        input_grad,
        gains[0],
        gains[1],
        gains[2],
        gains[3],
        f32(qkv),
        qkv_bias_grad.reshape(-1),
        f32(proj),
        out_bias_grad,
        f32(up),
        up_bias_grad.reshape(-1),
        f32(down),
        out_bias_grad,
    )


def solution(mesh):
    matrix = P(("seq", "fsdp"), "tensor")
    vector = P("tensor")
    return jax.shard_map(
        per_device,
        mesh=mesh,
        in_specs=(
            matrix, matrix, P(), P(), P(), P(),
            matrix, vector, matrix, vector, matrix, vector, matrix, vector,
        ),
        out_specs=(
            matrix, matrix, P(), P(), P(), P(),
            matrix, vector, matrix, vector, matrix, vector, matrix, vector,
        ),
        check_vma=False,
    )
```

```python
import functools
import types

import jax
import jax.numpy as jnp
import numpy as np
from jax import lax
from jax.experimental import pallas as pl
from jax.experimental.pallas import tpu as pltpu
from jax.sharding import PartitionSpec as P

HEAD_DIM = 256
ROT = 64
LANES = 128
STRIP = 256
MESH = pl.DeviceIdType.MESH
VMEM_BYTES = 67_043_328
SMALL, WIDE = jnp.bfloat16, jnp.float32

norm_eps = 1e-05
rope_base = 10000.0

WQ, WP, WU1, WU2, WD1, WD2 = range(6)
P1, D1, D2, Q1, U1, U2 = range(6)


def bits_of(size):
    return [1 << b for b in range(size.bit_length() - 1)]


def bf(value):
    return value.astype(jnp.bfloat16)


def f32(value):
    return value.astype(jnp.float32)


def mm(left, right, left_dim, right_dim):
    return lax.dot_general(
        left, right, (((left_dim,), (right_dim,)), ((), ())), preferred_element_type=jnp.float32
    )


def rotary_tables(tok, blocks):
    half = ROT // 2
    frequency = rope_base ** (-np.arange(half, dtype=np.float64) * 2.0 / ROT)
    lanes = np.zeros(LANES)
    lanes[:half] = frequency
    lanes[half:ROT] = frequency
    inner = np.arange(tok, dtype=np.float64)[:, None] * lanes
    outer = np.arange(blocks, dtype=np.float64)[:, None] * tok * lanes
    pack = lambda a: np.stack([np.cos(a), np.sin(a)]).astype(np.float32)
    return (jnp.asarray(pack(inner)), jnp.asarray(pack(outer)))


def flip(rank, mask, size):
    out = jnp.int32(0)
    for b in range(size.bit_length() - 1):
        digit = lax.rem(lax.div(rank, jnp.int32(1 << b)), jnp.int32(2))
        out = out + ((1 - digit) if mask >> b & 1 else digit) * (1 << b)
    return out


def low_bit(j, size):
    return j & -j if j else size


def line_mask(j):
    mask = 0
    b = 0
    while j >> b:
        if j >> b & 1:
            mask ^= (2 << b) - 1
        b += 1
    return mask


def arrivals(size):
    return sorted(range(1, size), key=lambda j: (-low_bit(j, size), j))


def slot_of(j, bit, size):
    index = 0
    for jj in range(size):
        for bb in bits_of(size):
            if bb < low_bit(jj, size):
                if (jj, bb) == (j, bit):
                    return index
                index += 1
    raise ValueError


def at(index, size):
    return pl.ds(pl.multiple_of(index * size, size), size)


def remote(src, dst, send, recv, peer):
    return pltpu.make_async_remote_copy(
        src_ref=src, dst_ref=dst, send_sem=send, recv_sem=recv, device_id=peer, device_id_type=MESH
    )


def repeat(count, body):
    def step(i, carry):
        body(i)
        return carry

    lax.fori_loop(0, count, step, 0)


def turn(value, cos_part, sin_part):
    half = ROT // 2
    head = value[:, :LANES]
    lane = lax.broadcasted_iota(jnp.int32, head.shape, 1)
    other = jnp.where(
        lane < half, -pltpu.roll(head, LANES - half, 1), pltpu.roll(head, half, 1)
    )
    return jnp.concatenate([head * cos_part + other * sin_part, value[:, LANES:]], axis=1)


def make_core(S, T, F):
    c = types.SimpleNamespace(S=S, T=T, F=F)
    c.z, c.y, c.f = lax.axis_index("seq"), lax.axis_index("tensor"), lax.axis_index("fsdp")
    c.fbits, c.sbits = bits_of(F), bits_of(S)
    sends, busy = [], {}

    def start(copy, key=None):
        copy.start()
        sends.append(copy)
        if key is not None:
            busy.setdefault(key, []).append(copy)

    def free(key):
        done = busy.pop(key, [])
        for copy in done:
            copy.wait_send()
        sends[:] = [s for s in sends if not any(s is copy for copy in done)]

    def finish():
        for copy in sends:
            copy.wait_send()

    def greet():
        barrier = pltpu.get_barrier_semaphore()
        peers = [{"seq": flip(c.z, k, S)} for k in range(1, S)]
        peers += [{"tensor": flip(c.y, t, T)} for t in range(1, T)]
        peers += [{"fsdp": flip(c.f, b, F)} for b in c.fbits]
        for peer in peers:
            pl.semaphore_signal(barrier, inc=1, device_id=peer, device_id_type=MESH)
        pl.semaphore_wait(barrier, len(peers))

    c.start, c.free, c.finish, c.greet = start, free, finish, greet
    return c


def gather_ops(c, e):
    S, T, F, z, y, f = c.S, c.T, c.F, c.z, c.y, c.f
    tok, width = e.hid_in.shape
    rows = e.wq_in.shape[0]
    half = e.wu.shape[1] // 2
    tokens = ((e.hid_in, e.hid), (e.cot_in, e.cot))
    weights = (
        (e.wq_in, e.wq, 0, e.wq.shape[1]),
        (e.wp_in, e.wp, 0, e.wp.shape[1]),
        (e.wu_in, e.wu, 0, half),
        (e.wu_in, e.wu, half, half),
        (e.wd_in, e.wd, 0, half),
        (e.wd_in, e.wd, half, half),
    )
    g = types.SimpleNamespace()

    def tok_sem(a, j, t):
        return (a * S + j) * T + t

    def tok_place(a, j, t):
        return tokens[a][1].at[at(flip(z, line_mask(j), S), tok), at(flip(y, t, T), width)]

    def tok_seq(a, j):
        src = tokens[a][0] if j == 0 else tok_place(a, j, 0)
        dst = tok_place(a, j, 0)
        for b in reversed(c.sbits):
            if b < low_bit(j, S):
                i = tok_sem(a, j + b, 0)
                peer = {"seq": flip(z, line_mask(b), S)}
                c.start(remote(src, dst, e.tok_send.at[i], e.tok_recv.at[i], peer))

    def tok_tensor(a, j):
        src = tokens[a][0] if j == 0 else tok_place(a, j, 0)
        dst = tok_place(a, j, 0)
        for t in range(1, T):
            i = tok_sem(a, j, t)
            peer = {"tensor": flip(y, t, T)}
            c.start(remote(src, dst, e.tok_send.at[i], e.tok_recv.at[i], peer))

    def tok_wait(a, j, t):
        i = tok_sem(a, j, t)
        spot = tok_place(a, j, t)
        peer = {"tensor": flip(y, 1, T)}
        remote(spot, spot, e.tok_send.at[i], e.tok_recv.at[i], peer).wait_recv()

    def tok_own(a):
        return pltpu.make_async_copy(tokens[a][0], tok_place(a, 0, 0), e.own_sem.at[a])

    def tok_direct(a):
        for j in c.sbits:
            tok_wait(a, j, 0)
            tok_seq(a, j)
            tok_tensor(a, j)

    def tok_passed(a):
        for j in arrivals(S):
            if j not in c.sbits:
                tok_wait(a, j, 0)
                tok_seq(a, j)
                tok_tensor(a, j)

    def tok_rest(a):
        tok_own(a).wait()
        for j in range(S):
            for t in range(1, T):
                tok_wait(a, j, t)

    def row_sem(m, k, j):
        return (m * S + k) * F + j

    def row_place(m, k, j):
        _, dst, first, size = weights[m]
        return dst.at[at(flip(z, k, S) * F + flip(f, j, F), rows), first : first + size]

    def row_source(m, zd):
        src, dst, first, size = weights[m]
        return src.at[:, pl.ds(pl.multiple_of(zd * dst.shape[1] + first, LANES), size)]

    def row_seq(m):
        for k in range(1, S):
            i = row_sem(m, k, 0)
            zd = flip(z, k, S)
            src = row_source(m, zd)
            dst = row_place(m, 0, 0)
            c.start(remote(src, dst, e.row_send.at[i], e.row_recv.at[i], {"seq": zd}))

    def row_forward(m, k, j):
        dst = row_place(m, k, j)
        src = row_source(m, z) if k == 0 and j == 0 else dst
        for b in reversed(c.fbits):
            if b < low_bit(j, F):
                i = row_sem(m, k, j + b)
                peer = {"fsdp": flip(f, b, F)}
                c.start(remote(src, dst, e.row_send.at[i], e.row_recv.at[i], peer))

    def row_wait(m, k, j):
        i = row_sem(m, k, j)
        spot = row_place(m, k, j)
        peer = {"seq": flip(z, 1, S)}
        remote(spot, spot, e.row_send.at[i], e.row_recv.at[i], peer).wait_recv()

    def row_own(m):
        return pltpu.make_async_copy(row_source(m, z), row_place(m, 0, 0), e.own_sem.at[2 + m])

    def row_arrive(m):
        for k in range(1, S):
            row_wait(m, k, 0)
            row_forward(m, k, 0)

    def row_relay(m):
        for j in arrivals(F):
            if low_bit(j, F) > 1:
                for k in range(S):
                    row_wait(m, k, j)
                    row_forward(m, k, j)

    def row_rest(m):
        row_own(m).wait()
        for j in arrivals(F):
            if low_bit(j, F) == 1:
                for k in range(S):
                    row_wait(m, k, j)

    def begin_own():
        for a in range(2):
            tok_own(a).start()
        for m in range(6):
            row_own(m).start()

    g.tok_seq, g.tok_tensor, g.tok_direct, g.tok_passed = tok_seq, tok_tensor, tok_direct, tok_passed
    g.tok_rest, g.row_seq, g.row_forward, g.row_arrive = tok_rest, row_seq, row_forward, row_arrive
    g.row_relay, g.row_rest, g.begin_own = row_relay, row_rest, begin_own
    return g


def attention_ops(c, e):
    S, T, F, z, y, f = c.S, c.T, c.F, c.z, c.y, c.f
    tok = e.hid_in.shape[0]
    ntok = e.hid.shape[0]
    keys = e.pair.shape[0]
    scale = HEAD_DIM ** (-0.5)
    chunk = 32
    qc = max(32, min(tok, tok * 1024 // keys))
    o = types.SimpleNamespace()

    def norm():
        def norm_chunk(i):
            part = at(i, chunk)
            x = f32(e.hid[part, :])
            mean = jnp.mean(x, axis=-1, keepdims=True)
            centered = x - mean
            inv_std = lax.rsqrt(jnp.mean(centered * centered, axis=-1, keepdims=True) + norm_eps)
            xhat = centered * inv_std
            e.attn_in[part, :] = bf(xhat * e.attn_gain[...] + e.attn_bias[...])
            e.mlp_in[part, :] = bf(xhat * e.mlp_gain[...] + e.mlp_bias[...])
            e.stat[0, part, :] = jnp.broadcast_to(mean, (chunk, LANES))
            e.stat[1, part, :] = jnp.broadcast_to(inv_std, (chunk, LANES))

        repeat(ntok // chunk, norm_chunk)

    def angles(zd, here=slice(None)):
        block = pl.ds(zd * F + f, 1)
        cos_in, sin_in = e.inner[0, here, :], e.inner[1, here, :]
        cos_out, sin_out = e.outer[0, block, :], e.outer[1, block, :]
        return (cos_in * cos_out - sin_in * sin_out, sin_in * cos_out + cos_in * sin_out)

    def qkv():
        bias = e.qkv_bias[:, at(z, 3 * HEAD_DIM)]
        for n in range(3):
            columns = slice(n * HEAD_DIM, (n + 1) * HEAD_DIM)
            part = mm(e.attn_in[...], e.wq[:, columns], 1, 0) + bias[:, columns]
            for zd in range(S):
                piece = part[zd * tok : (zd + 1) * tok]
                if n < 2:
                    piece = turn(piece, *angles(zd))
                if n == 0:
                    e.query[zd * tok : (zd + 1) * tok, :] = bf(piece)
                else:
                    spot = at(zd * F + f, tok)
                    e.pair[spot, (n - 1) * HEAD_DIM : n * HEAD_DIM] = bf(piece)

    def pair_place(zd, j):
        return e.pair.at[at(zd * F + flip(f, j, F), tok), :]

    def pair_forward(zd, j):
        spot = pair_place(zd, j)
        for b in reversed(c.fbits):
            if b < low_bit(j, F):
                i = zd * F + j + b
                peer = {"fsdp": flip(f, b, F)}
                c.start(remote(spot, spot, e.pair_send.at[i], e.pair_recv.at[i], peer), "pair")

    def pair_wait(zd, j):
        i = zd * F + j
        spot = pair_place(zd, j)
        peer = {"fsdp": flip(f, 1, F)}
        remote(spot, spot, e.pair_send.at[i], e.pair_recv.at[i], peer).wait_recv()

    def pair_own():
        for zd in range(S):
            pair_forward(zd, 0)

    def pair_relay():
        for j in arrivals(F):
            if low_bit(j, F) > 1:
                for zd in range(S):
                    pair_wait(zd, j)
                    pair_forward(zd, j)

    def pair_rest():
        for j in arrivals(F):
            if low_bit(j, F) == 1:
                for zd in range(S):
                    pair_wait(zd, j)

    def masked_scores(zd, i, n):
        start_row = zd * tok + i * qc
        q = e.query[pl.ds(pl.multiple_of(start_row, qc), qc), :]
        scores = mm(q, e.pair[:n, :HEAD_DIM], 1, 1) * scale
        last = (zd * F + f) * tok + i * qc
        ahead = lax.broadcasted_iota(jnp.int32, scores.shape, 1) - lax.broadcasted_iota(
            jnp.int32, scores.shape, 0
        )
        return (scores, ahead <= last)

    def forward():
        for zd in range(S):
            n = (zd + 1) * F * tok

            def forward_chunk(i, zd=zd, n=n):
                here = pl.ds(pl.multiple_of(zd * tok + i * qc, qc), qc)
                scores, allowed = masked_scores(zd, i, n)
                top = jnp.max(jnp.where(allowed, scores, -1e30), axis=-1, keepdims=True)
                terms = jnp.where(allowed, jnp.exp(scores - top), 0.0)
                total = jnp.sum(terms, axis=-1, keepdims=True)
                mixed = mm(bf(terms), e.pair[:n, HEAD_DIM:], 1, 0) / total
                e.attn[here, :] = bf(mixed)
                e.row_info[here, :] = jnp.broadcast_to(top + jnp.log(total), (qc, LANES))

            repeat(tok // qc, forward_chunk)

    def backward():
        e.attn_grad[...] = bf(mm(e.cot[...], e.wp[...], 1, 0))
        for zd in range(S):
            n = (zd + 1) * F * tok

            def backward_chunk(i, zd=zd, n=n):
                here = pl.ds(pl.multiple_of(zd * tok + i * qc, qc), qc)
                scores, allowed = masked_scores(zd, i, n)
                weights_here = jnp.where(allowed, jnp.exp(scores - e.row_info[here, :1]), 0.0)
                grad = e.attn_grad[here, :]
                delta = jnp.sum(f32(grad) * f32(e.attn[here, :]), axis=-1, keepdims=True)
                slopes = mm(grad, e.pair[:n, HEAD_DIM:], 1, 1)
                inner_grad = bf(weights_here * (slopes - delta))
                e.probs[here, :n] = bf(weights_here)
                e.score_grad[here, :n] = inner_grad
                if n < keys:
                    blank = jnp.zeros((qc, keys - n), jnp.bfloat16)
                    e.probs[here, n:] = blank
                    e.score_grad[here, n:] = blank
                cos_part, sin_part = angles(zd, pl.ds(pl.multiple_of(i * qc, qc), qc))
                grad_here = mm(inner_grad, e.pair[:n, :HEAD_DIM], 1, 0) * scale
                e.tg[here, :HEAD_DIM] = bf(turn(grad_here, cos_part, -sin_part))

            repeat(tok // qc, backward_chunk)

    def part_sum(j):
        def lanes(ref):
            return jnp.concatenate(
                [ref[:, at(zd * F + flip(f, j, F), tok)] for zd in range(S)], axis=1
            )

        total = jnp.concatenate(
            [
                mm(lanes(e.score_grad), e.query[...], 0, 0) * scale,
                mm(lanes(e.probs), e.attn_grad[...], 0, 0),
            ],
            axis=1,
        )
        for b in c.fbits:
            if b < low_bit(j, F):
                i = slot_of(j, b, F)
                spot = e.part_in.at[i]
                peer = {"fsdp": flip(f, b, F)}
                remote(spot, spot, e.part_send.at[i], e.part_recv.at[i], peer).wait_recv()
                total = total + f32(e.part_in[i])
        return total

    def part_stage(bit):
        c.free("pair")
        for j in range(1, F):
            if low_bit(j, F) == bit:
                spot = e.pair.at[(j - 1) * ntok : j * ntok, :]
                e.pair[(j - 1) * ntok : j * ntok, :] = bf(part_sum(j))
                i = slot_of(j - bit, bit, F)
                peer = {"fsdp": flip(f, bit, F)}
                here = e.part_in.at[i]
                c.start(remote(spot, here, e.part_send.at[j - 1], e.part_recv.at[i], peer))

    def part_later():
        for bit in c.fbits[1:]:
            part_stage(bit)

    def part_home():
        total = part_sum(0)
        for zd in range(S):
            here = slice(zd * tok, (zd + 1) * tok)
            cos_part, sin_part = angles(zd)
            key_part = turn(total[here, :HEAD_DIM], cos_part, -sin_part)
            e.tg[here, HEAD_DIM : 2 * HEAD_DIM] = bf(key_part)
            e.tg[here, 2 * HEAD_DIM :] = bf(total[here, HEAD_DIM:])

    def up(first, size):
        cols = e.wu.shape[1]
        for n in range(first // STRIP, (first + size) // STRIP):
            strip = slice(n * STRIP, (n + 1) * STRIP)
            bias = e.up_bias[:, pl.ds(pl.multiple_of(z * cols + n * STRIP, STRIP), STRIP)]
            mid = mm(e.mlp_in[...], e.wu[:, strip], 1, 0) + bias
            cdf = 0.5 * (1.0 + lax.erf(mid * 0.7071067811865476))
            e.active[:, strip] = bf(mid * cdf)
            e.slope[:, strip] = cdf + mid * jnp.exp(-0.5 * mid * mid) * 0.3989422804014327

    o.norm, o.qkv, o.pair_own, o.pair_relay, o.pair_rest = norm, qkv, pair_own, pair_relay, pair_rest
    o.forward, o.backward, o.part_stage, o.part_later = forward, backward, part_stage, part_later
    o.part_home, o.up = part_home, up
    return o


def grad_units(ff):
    half = ff // 2
    return (
        (0, 0, HEAD_DIM),
        (1, 0, half),
        (1, half, half),
        (2, 0, 3 * HEAD_DIM),
        (3, 0, half),
        (3, half, half),
    )


def spread_ops(c, e, turned):
    S, T, F, z, y, f = c.S, c.T, c.F, c.z, c.y, c.f
    tok, width = e.homes[0].shape
    ntok, D = e.wide.shape
    ff = e.active.shape[1]
    rows = e.grads[0].shape[0]
    rights, lefts = (e.attn, e.active, e.tg, e.pre), (e.cot, e.cot, e.attn_in, e.mlp_in)
    units = grad_units(ff)
    n_u = len(units)
    p = types.SimpleNamespace()

    def block_sum(u, j):
        g, first, size = units[u]
        right, left = rights[g].at[:, first : first + size], lefts[g]
        fd = flip(f, j, F)
        if turned:
            block = jnp.concatenate([left[at(zd * F + fd, rows), :] for zd in range(S)], axis=0)
            total = mm(block, right[...], 1, 0)
        else:
            block = jnp.concatenate([left[:, at(zd * F + fd, rows)] for zd in range(S)], axis=1)
            total = mm(block, right[...], 0, 0)
        for bit in c.fbits:
            if bit < low_bit(j, F):
                s = slot_of(j, bit, F)
                i = u * (F - 1) + s
                spot = e.in_b[u].at[s]
                peer = {"fsdp": flip(f, bit, F)}
                remote(spot, spot, e.out_sem.at[i], e.in_sem.at[i], peer).wait_recv()
                total = total + f32(e.in_b[u][s])
        return total

    def fsdp_stage(u, bit):
        for j in range(1, F):
            if low_bit(j, F) == bit:
                key, spot = e.out_spot(u, j)
                c.free(key)
                spot[...] = bf(block_sum(u, j))
                there = slot_of(j - bit, bit, F)
                send = e.out_sem.at[u * (F - 1) + j - 1]
                recv = e.in_sem.at[u * (F - 1) + there]
                peer = {"fsdp": flip(f, bit, F)}
                c.start(remote(spot, e.in_b[u].at[there], send, recv, peer), key)

    def first(u):
        fsdp_stage(u, c.fbits[0])

    def later(u):
        for bit in c.fbits[1:]:
            fsdp_stage(u, bit)

    def grad_place(u, zd):
        g, first_col, size = units[u]
        start_col = zd * rights[g].shape[1] + first_col
        return e.grads[g].at[:, pl.ds(pl.multiple_of(start_col, LANES), size)]

    def own_grad(u):
        src = e.seq_b[u].at[at(z, rows), :]
        return pltpu.make_async_copy(src, grad_place(u, z), e.home_sem.at[u])

    def seq(u):
        e.seq_b[u][...] = bf(block_sum(u, 0))
        for k in range(1, S):
            peer = flip(z, k, S)
            src, dst = e.seq_b[u].at[at(peer, rows), :], grad_place(u, z)
            i = u * S + k
            c.start(remote(src, dst, e.seq_send.at[i], e.seq_recv.at[i], {"seq": peer}))
        own_grad(u).start()

    def seq_wait():
        for u in range(n_u):
            for k in range(1, S):
                peer = flip(z, k, S)
                spot = grad_place(u, peer)
                i = u * S + k
                remote(spot, spot, e.seq_send.at[i], e.seq_recv.at[i], {"seq": peer}).wait_recv()
            own_grad(u).wait()

    def half_strips(s, t, term):
        for n in range(width // STRIP):
            there = pl.ds(pl.multiple_of(flip(y, t, T) * width + n * STRIP, STRIP), STRIP)
            here = slice(n * STRIP, (n + 1) * STRIP)
            value = term(there)
            if t:
                for zd in range(S):
                    e.y_out[(t - 1) * S + zd, :, here] = bf(value[zd * tok : (zd + 1) * tok])
            elif s == 0:
                e.own_half[:, here] = value
            else:
                e.wide[:, there] = value

    def y_index(s, t, j):
        return (s * max(T - 1, 1) + t - 1) * S + j

    def tensor_send(s):
        for j in [*sorted(range(1, S), key=lambda j: (low_bit(j, S), j)), 0]:
            zd = flip(z, line_mask(j), S)
            for t in range(1, T):
                i = y_index(s, t, j)
                peer = {"tensor": flip(y, t, T)}
                here = e.y_out.at[(t - 1) * S + zd]
                c.start(remote(here, e.y_in.at[i], e.y_send.at[i], e.y_recv.at[i], peer), "y")

    def token_own(s, zd):
        if s == 0:
            return e.own_half.at[at(zd, tok), :]
        return e.wide.at[at(zd, tok), at(y, width)]

    def token_part(s, j):
        total = token_own(s, flip(z, line_mask(j), S))[...]
        for t in range(1, T):
            i = y_index(s, t, j)
            spot = e.y_in.at[i]
            peer = {"tensor": flip(y, t, T)}
            remote(spot, spot, e.y_send.at[i], e.y_recv.at[i], peer).wait_recv()
            total = total + f32(e.y_in[i])
        for bit in c.sbits:
            if bit < low_bit(j, S):
                i = s * (S - 1) + slot_of(j, bit, S)
                spot = e.z_in.at[i]
                peer = {"seq": flip(z, line_mask(bit), S)}
                remote(spot, spot, e.z_send.at[i], e.z_recv.at[i], peer).wait_recv()
                total = total + f32(e.z_in[i])
        return total

    def token_stage(s, bit):
        for j in range(1, S):
            if low_bit(j, S) == bit:
                i = s * (S - 1) + j - 1
                there = s * (S - 1) + slot_of(j - bit, bit, S)
                c.free(("z", j))
                e.z_out[j - 1] = bf(token_part(s, j))
                peer = {"seq": flip(z, line_mask(bit), S)}
                here = e.z_out.at[j - 1]
                copy = remote(here, e.z_in.at[there], e.z_send.at[i], e.z_recv.at[there], peer)
                c.start(copy, ("z", j))

    def token_first(s):
        token_stage(s, c.sbits[0])

    def token_later(s):
        for bit in c.sbits[1:]:
            token_stage(s, bit)

    def home_copy(s):
        return pltpu.make_async_copy(token_own(s, z), e.homes[s], e.home_sem.at[n_u + s])

    def token_home(s):
        total = token_part(s, 0)
        token_own(s, z)[...] = total
        home_copy(s).start()

    def home_wait():
        for s in range(2):
            home_copy(s).wait()

    n_f = len(c.fbits)
    vec = e.vec

    def vec_copy(b):
        peer = {"fsdp": flip(f, c.fbits[b], F)}
        return remote(vec.at[b], e.vec_in.at[b], e.v_send.at[b], e.v_recv.at[b], peer)

    def vec_start(b):
        c.start(vec_copy(b))

    def vec_sum(b):
        vec_copy(b).wait_recv()
        vec[b + 1] = vec[b] + e.vec_in[b]

    def vec_fsdp():
        for b in range(n_f - 1):
            vec_sum(b)
            vec_start(b + 1)

    def vec_seq_copy(k):
        peer = {"seq": flip(z, k, S)}
        i = n_f + k - 1
        return remote(vec.at[n_f], e.vec_seq.at[k - 1], e.v_send.at[i], e.v_recv.at[i], peer)

    def vec_seq_start():
        vec_sum(n_f - 1)
        for k in range(1, S):
            c.start(vec_seq_copy(k))

    def tree(parts):
        while len(parts) > 1:
            parts = [a + b for a, b in zip(parts[::2], parts[1::2])]
        return parts[0]

    def vec_seq_sum():
        parts = []
        for k in range(S):
            if k:
                vec_seq_copy(k).wait_recv()
            value = vec[n_f] if k == 0 else e.vec_seq[k - 1]
            zd = flip(z, k, S)
            e.qkv_bias_o[:, at(zd, 3 * HEAD_DIM)] = value[4:5, : 3 * HEAD_DIM]
            e.up_bias_o[:, at(zd, ff)] = value[5:6, :ff]
            parts.append(value)
        total = tree(parts)
        e.out_bias_o[...] = total[6:7, :width]
        e.vec_ten[0] = total[:4]
        for t in range(1, T):
            c.start(vec_ten_copy(t))

    def vec_ten_copy(t):
        peer = {"tensor": flip(y, t, T)}
        i = n_f + S - 1 + t - 1
        return remote(e.vec_ten.at[0], e.vec_ten.at[t], e.v_send.at[i], e.v_recv.at[i], peer)

    def vec_ten_sum():
        parts = [e.vec_ten[0]]
        for t in range(1, T):
            vec_ten_copy(t).wait_recv()
            parts.append(e.vec_ten[t])
        e.gain_o[...] = tree(parts)

    def branch():
        def term(column):
            return mm(e.active[...], e.wd[column, :], 1, 1) + mm(e.attn[...], e.wp[column, :], 1, 1)

        for t in range(1, T):
            half_strips(0, t, term)
        tensor_send(0)
        return lambda: half_strips(0, 0, term)

    def hidden_grad():
        vec[0] = jnp.zeros(vec.shape[1:], jnp.float32)
        for n in range(ff // STRIP):
            here = slice(n * STRIP, (n + 1) * STRIP)
            value = mm(e.cot[...], e.wd[:, here], 0 if turned else 1, 0) * e.slope[:, here]
            vec[0, 5:6, here] = jnp.sum(value, axis=0, keepdims=True)
            e.pre[:, here] = bf(value)

    def unit_rows(column):
        mean, inv_std = e.stat[0, :, :1], e.stat[1, :, :1]
        return ((f32(e.hid[:, column]) - mean) * inv_std, inv_std)

    def norm_strips():
        lane_parts = range(0, STRIP, LANES)

        def norm_strip(n):
            here = at(n, STRIP)
            a = mm(e.tg[...], e.wq[here, :], 1, 1)
            m = mm(e.pre[...], e.wu[here, :], 1, 1)
            xhat, _ = unit_rows(here)
            vec[0, 0:1, here] = jnp.sum(a * xhat, axis=0, keepdims=True)
            vec[0, 1:2, here] = jnp.sum(a, axis=0, keepdims=True)
            vec[0, 2:3, here] = jnp.sum(m * xhat, axis=0, keepdims=True)
            vec[0, 3:4, here] = jnp.sum(m, axis=0, keepdims=True)
            both = a * e.attn_gain[:, here] + m * e.mlp_gain[:, here]
            e.wide[:, here] = both
            scaled = both * xhat
            e.sums[0] += sum(both[:, i : i + LANES] for i in lane_parts)
            e.sums[1] += sum(scaled[:, i : i + LANES] for i in lane_parts)

        e.sums[...] = jnp.zeros_like(e.sums)
        repeat(D // STRIP, norm_strip)
        vec[0, 4:5, : 3 * HEAD_DIM] = jnp.sum(f32(e.tg[...]), axis=0, keepdims=True)
        vec[0, 6:7, :width] = jnp.sum(f32(e.own_cot()), axis=0, keepdims=True)
        vec_start(0)
        for i in range(2):
            mean = jnp.sum(e.sums[i], axis=-1, keepdims=True) / D
            e.sums[i] = jnp.broadcast_to(mean, e.sums.shape[1:])

    def input_strips():
        def term(column):
            xhat, inv_std = unit_rows(column)
            return inv_std * (e.wide[:, column] - e.sums[0, :, :1] - xhat * e.sums[1, :, :1])

        c.free("y")
        for t in range(1, T):
            half_strips(1, t, term)
        tensor_send(1)
        return lambda: half_strips(1, 0, term)

    p.first, p.later, p.seq, p.seq_wait = first, later, seq, seq_wait
    p.token_first, p.token_later, p.token_home = token_first, token_later, token_home
    p.home_wait, p.vec_fsdp = home_wait, vec_fsdp
    p.vec_seq_start, p.vec_seq_sum, p.vec_ten_sum = vec_seq_start, vec_seq_sum, vec_ten_sum
    p.branch, p.hidden_grad, p.norm_strips, p.input_strips = (
        branch,
        hidden_grad,
        norm_strips,
        input_strips,
    )
    return p


def gather_buffers(S, T, F, tok, width, rows, ff):
    ntok, D, keys = S * tok, T * width, S * F * tok
    kept = {
        "hid": ((ntok, D), SMALL),
        "cot": ((ntok, D), SMALL),
        "attn_in": ((ntok, D), SMALL),
        "mlp_in": ((ntok, D), SMALL),
        "stat": ((2, ntok, LANES), WIDE),
        "wq": ((D, 3 * HEAD_DIM), SMALL),
        "wp": ((D, HEAD_DIM), SMALL),
        "wu": ((D, ff), SMALL),
        "wd": ((D, ff), SMALL),
        "attn": ((ntok, HEAD_DIM), SMALL),
        "active": ((ntok, ff), SMALL),
        "tg": ((ntok, 3 * HEAD_DIM), SMALL),
    }
    passing = {
        "query": ((ntok, HEAD_DIM), SMALL),
        "pair": ((keys, 2 * HEAD_DIM), SMALL),
        "attn_grad": ((ntok, HEAD_DIM), SMALL),
        "probs": ((ntok, keys), SMALL),
        "score_grad": ((ntok, keys), SMALL),
        "row_info": ((ntok, LANES), WIDE),
        "part_in": ((max(F - 1, 1), ntok, 2 * HEAD_DIM), SMALL),
    }
    sems = {
        "own_sem": 8,
        "tok_send": 2 * S * T,
        "tok_recv": 2 * S * T,
        "row_send": 6 * S * F,
        "row_recv": 6 * S * F,
        "pair_send": S * F,
        "pair_recv": S * F,
        "part_send": max(F - 1, 1),
        "part_recv": max(F - 1, 1),
    }
    return kept, passing, sems


def spread_buffers(S, T, F, tok, width, rows, ff):
    ntok, D = S * tok, T * width
    n_f, n_y, parts = len(bits_of(F)), max(T - 1, 1) * S, max(F - 1, 1)
    held = {
        "pre": ((ntok, ff), SMALL),
        "wide": ((ntok, D), WIDE),
        "own_half": ((ntok, width), WIDE),
        "sums": ((2, ntok, LANES), WIDE),
        "vec": ((n_f + 1, 8, D), WIDE),
        "vec_in": ((n_f, 8, D), WIDE),
        "vec_seq": ((max(S - 1, 1), 8, D), WIDE),
        "vec_ten": ((T, 4, D), WIDE),
        "y_out": ((n_y, tok, width), SMALL),
        "y_in": ((2 * n_y, tok, width), SMALL),
        "z_out": ((max(S - 1, 1), tok, width), SMALL),
        "z_in": ((2 * max(S - 1, 1), tok, width), SMALL),
    }
    for u, (_, _, size) in enumerate(grad_units(ff)):
        held[f"in_b{u}"] = ((parts, S * rows, size), SMALL)
        held[f"seq_b{u}"] = ((S * rows, size), SMALL)
    sems = {
        "home_sem": 8,
        "out_sem": 6 * parts,
        "in_sem": 6 * parts,
        "seq_send": 6 * S,
        "seq_recv": 6 * S,
        "y_send": 2 * n_y,
        "y_recv": 2 * n_y,
        "z_send": 2 * max(S - 1, 1),
        "z_recv": 2 * max(S - 1, 1),
        "v_send": n_f + S + T,
        "v_recv": n_f + S + T,
    }
    outs = {f"grad{g}": ((rows, S * n), SMALL) for g, n in enumerate((HEAD_DIM, ff, 3 * HEAD_DIM, ff))}
    outs |= {f"home{s}": ((tok, width), WIDE) for s in range(2)}
    vectors = {
        "gain_o": ((4, D), WIDE),
        "qkv_bias_o": ((1, 3 * width), WIDE),
        "up_bias_o": ((1, S * ff), WIDE),
        "out_bias_o": ((1, width), WIDE),
    }
    return held, sems, outs, vectors


def send_buffers(S, F, rows, ff, units):
    sizes = [size for _, _, size in grad_units(ff)]
    return {f"out_b{u}": ((max(F - 1, 1), S * rows, sizes[u]), SMALL) for u in units}


def gather_lists(e):
    e.in_b = [getattr(e, f"in_b{u}") for u in range(6)]
    e.seq_b = [getattr(e, f"seq_b{u}") for u in range(6)]
    e.grads = [getattr(e, f"grad{g}") for g in range(4)]
    e.homes = [e.home0, e.home1]


def launch(body, sizes, collective, far, near, outs, near_outs, scratch, sems):
    names = [*far, *near, *outs, *near_outs, *scratch, *sems]

    def kernel(*refs):
        body(types.SimpleNamespace(**dict(zip(names, refs))), *sizes)

    kernel.__name__ = body.__name__
    any_spec = pl.BlockSpec(memory_space=pl.ANY)
    vmem = pl.BlockSpec(memory_space=pltpu.VMEM)
    results = pl.pallas_call(
        kernel,
        out_shape=[jax.ShapeDtypeStruct(*o) for o in [*outs.values(), *near_outs.values()]],
        in_specs=[any_spec] * len(far) + [vmem] * len(near),
        out_specs=[any_spec] * len(outs) + [vmem] * len(near_outs),
        scratch_shapes=[pltpu.VMEM(*s) for s in scratch.values()]
        + [pltpu.SemaphoreType.DMA((n,)) for n in sems.values()],
        compiler_params=pltpu.CompilerParams(
            collective_id=collective, has_side_effects=True, vmem_limit_bytes=VMEM_BYTES
        ),
    )(*far.values(), *near.values())
    return dict(zip([*outs, *near_outs], results))


def whole_kernel(e, S, T, F):
    c = make_core(S, T, F)
    width = e.hid_in.shape[1]
    tok = e.hid_in.shape[0]
    ff = e.active.shape[1]
    half = ff // 2
    gather_lists(e)
    e.slope = e.wide.at[:, :ff]
    e.row_info = e.sums.at[0]
    e.own_cot = lambda: e.cot[at(c.z, tok), at(c.y, width)]
    wide_q = 3 * HEAD_DIM
    lent = [e.probs.at[:, :wide_q], e.probs.at[:, wide_q : 2 * wide_q], e.score_grad.at[:, :wide_q]]

    def out_spot(u, j):
        if u == Q1:
            return (("out", u, j), lent[j - 1])
        shared = {U1: D1, U2: D2}.get(u, u)
        return (("out", shared, j), getattr(e, f"out_b{shared}").at[j - 1])

    e.out_spot = out_spot
    g, o, p = gather_ops(c, e), attention_ops(c, e), spread_ops(c, e, False)

    c.greet()
    g.tok_seq(0, 0)
    g.tok_direct(0)
    g.row_seq(WQ)
    g.row_forward(WU2, 0, 0)
    g.row_forward(WQ, 0, 0)
    g.row_arrive(WQ)
    g.begin_own()
    g.row_seq(WU1)
    g.tok_tensor(0, 0)
    g.row_forward(WD2, 0, 0)
    g.row_relay(WQ)
    g.row_rest(WQ)
    g.row_seq(WU2)
    g.tok_passed(0)
    g.row_arrive(WU1)
    g.tok_rest(0)
    g.tok_seq(1, 0)
    g.row_arrive(WU2)
    g.row_forward(WP, 0, 0)
    g.row_forward(WU1, 0, 0)
    g.tok_tensor(1, 0)
    o.norm()
    o.qkv()
    o.pair_own()
    g.row_seq(WP)
    g.tok_direct(1)
    g.row_relay(WU2)
    g.row_rest(WU2)
    g.row_forward(WD1, 0, 0)
    g.row_relay(WU1)
    g.row_arrive(WP)
    g.row_rest(WU1)
    g.row_seq(WD1)
    g.tok_passed(1)
    o.pair_relay()
    o.up(half, half)
    o.up(0, half)
    g.row_arrive(WD1)
    g.row_seq(WD2)
    g.tok_rest(1)
    p.first(D2)
    o.pair_rest()
    g.row_relay(WP)
    p.later(D2)
    g.row_rest(WP)
    o.forward()
    g.row_relay(WD1)
    g.row_arrive(WD2)
    p.first(P1)
    p.first(D1)
    o.backward()
    p.seq(D2)
    o.part_stage(c.fbits[0])
    p.later(P1)
    g.row_rest(WD1)
    g.row_relay(WD2)
    p.later(D1)
    g.row_rest(WD2)
    own_strips = p.branch()
    p.hidden_grad()
    o.part_later()
    p.seq(P1)
    p.first(U2)
    own_strips()
    p.token_first(0)
    p.seq(D1)
    p.later(U2)
    o.part_home()
    p.first(Q1)
    p.token_later(0)
    p.norm_strips()
    p.vec_fsdp()
    p.later(Q1)
    p.seq(U2)
    own_terms = p.input_strips()
    own_terms()
    p.token_first(1)
    p.vec_seq_start()
    p.seq(Q1)
    p.first(U1)
    p.token_later(1)
    p.vec_seq_sum()
    p.token_home(0)
    p.later(U1)
    p.seq(U1)
    p.token_home(1)
    p.vec_ten_sum()
    p.seq_wait()
    p.home_wait()
    c.finish()


KEPT = ("hid", "cot", "attn_in", "mlp_in", "stat", "wq", "wp", "wu", "wd", "attn", "active", "tg")


def first_kernel(e, S, T, F):
    c = make_core(S, T, F)
    half = e.active.shape[1] // 2
    g, o = gather_ops(c, e), attention_ops(c, e)
    names = [*KEPT, "slope"]

    def out_copy(name):
        i = names.index(name)
        return pltpu.make_async_copy(getattr(e, name), getattr(e, name + "_o"), e.put_sem.at[i])

    c.greet()
    g.tok_seq(0, 0)
    g.tok_tensor(0, 0)
    for m in range(6):
        g.row_forward(m, 0, 0)
    g.begin_own()
    g.tok_direct(0)
    g.row_seq(WQ)
    g.tok_passed(0)
    g.row_seq(WU1)
    g.tok_tensor(1, 0)
    g.tok_rest(0)
    o.norm()
    g.row_arrive(WQ)
    g.tok_seq(1, 0)
    g.row_relay(WQ)
    g.row_rest(WQ)
    o.qkv()
    o.pair_own()
    g.row_arrive(WU1)
    for m in (WP, WU2, WD1, WD2):
        g.row_seq(m)
    g.tok_direct(1)
    g.row_relay(WU1)
    o.pair_relay()
    g.tok_passed(1)
    g.row_rest(WU1)
    o.up(0, half)
    g.row_arrive(WP)
    o.pair_rest()
    o.forward()
    g.row_arrive(WU2)
    g.tok_rest(1)
    g.row_relay(WP)
    g.row_rest(WP)
    o.backward()
    o.part_stage(c.fbits[0])
    g.row_relay(WU2)
    g.row_rest(WU2)
    o.up(half, half)
    o.part_later()
    g.row_arrive(WD1)
    g.row_arrive(WD2)
    o.part_home()
    for m in (WD1, WD2):
        g.row_relay(m)
        g.row_rest(m)
    for name in names:
        out_copy(name).start()
    for name in names:
        out_copy(name).wait()
    c.finish()


def second_kernel(e, S, T, F, turned):
    c = make_core(S, T, F)
    gather_lists(e)
    ff = e.active.shape[1]
    e.slope = e.wide.at[:, :ff]
    e.own_cot = lambda: e.own_cot_in[...]
    e.out_spot = lambda u, j: (("out", u, j), getattr(e, f"out_b{u}").at[j - 1])
    e.wd = e.wu = e.wud
    p = spread_ops(c, e, turned)
    names = [*KEPT, "slope"]

    def load(name):
        i = names.index(name)
        return pltpu.make_async_copy(getattr(e, name + "_i"), getattr(e, name), e.load_sem.at[i])

    for name in names:
        if name != "wu":
            load(name).start()
    c.greet()
    for name in names:
        if name != "wu":
            load(name).wait()
    p.first(P1)
    p.first(D1)
    p.first(D2)
    own_strips = p.branch()
    p.later(P1)
    own_strips()
    p.later(D1)
    p.hidden_grad()
    load("wu").start()
    p.seq(P1)
    p.later(D2)
    p.token_first(0)
    p.first(Q1)
    p.first(U1)
    p.first(U2)
    load("wu").wait()
    p.norm_strips()
    p.seq(D1)
    p.later(Q1)
    own_terms = p.input_strips()
    own_terms()
    p.token_later(0)
    p.seq(D2)
    p.later(U1)
    p.vec_fsdp()
    p.seq(Q1)
    p.later(U2)
    p.token_first(1)
    p.token_home(0)
    p.vec_seq_start()
    p.seq(U1)
    p.seq(U2)
    p.token_later(1)
    p.vec_seq_sum()
    p.vec_ten_sum()
    p.token_home(1)
    p.seq_wait()
    p.home_wait()
    c.finish()


def per_device(
    hidden_in,
    out_cotangent,
    attn_norm_gain,
    attn_norm_bias,
    mlp_norm_gain,
    mlp_norm_bias,
    qkv_weight,
    qkv_bias,
    proj_weight,
    proj_bias,
    up_weight,
    up_bias,
    down_weight,
    down_bias,
):
    S, T, F = [lax.axis_size(a) for a in ("seq", "tensor", "fsdp")]
    tok, width = hidden_in.shape
    rows, ff = qkv_weight.shape[0], up_weight.shape[1] // S
    if width != S * HEAD_DIM or S * F * rows != T * width:
        raise ValueError
    shape = (S, T, F, tok, width, rows, ff)
    inner, outer = rotary_tables(tok, S * F)
    far = {
        "hid_in": hidden_in,
        "cot_in": out_cotangent,
        "wq_in": qkv_weight,
        "wp_in": proj_weight,
        "wu_in": up_weight,
        "wd_in": down_weight,
    }
    row = lambda v: v.reshape(1, -1)
    gains = {"attn_gain": row(attn_norm_gain), "mlp_gain": row(mlp_norm_gain)}
    near = gains | {
        "attn_bias": row(attn_norm_bias),
        "mlp_bias": row(mlp_norm_bias),
        "qkv_bias": row(qkv_bias),
        "up_bias": row(up_bias),
        "inner": inner,
        "outer": outer,
    }
    kept, passing, gather_sems = gather_buffers(*shape)
    held, spread_sems, outs, vectors = spread_buffers(*shape)
    if rows % LANES == 0 and F <= 4:
        scratch = kept | passing | held | send_buffers(S, F, rows, ff, (P1, D1, D2))
        del scratch["row_info"]
        sems = gather_sems | spread_sems
        res = launch(whole_kernel, (S, T, F), 0, far, near, outs, vectors, scratch, sems)
    else:
        slope = {"slope": ((S * tok, ff), WIDE)}
        saved = {k + "_o": v for k, v in (kept | slope).items()}
        sems = gather_sems | {"put_sem": len(saved)}
        scratch = kept | slope | passing
        mid = launch(first_kernel, (S, T, F), 0, far, near, saved, {}, scratch, sems)
        turned = rows % LANES != 0
        if turned:
            for k in ("cot_o", "attn_in_o", "mlp_in_o"):
                mid[k] = mid[k].T
        ins = {k[:-2] + "_i": v for k, v in mid.items()}
        scratch = {k: (ins[k + "_i"].shape, t) for k, (_, t) in kept.items() if k not in ("wu", "wd")}
        scratch |= {"wud": kept["wu"]} | held | send_buffers(S, F, rows, ff, range(6))
        near = gains | {"own_cot_in": out_cotangent}
        sems = spread_sems | {"load_sem": len(ins)}
        res = launch(
            second_kernel, (S, T, F, turned), 1, ins, near, outs, vectors, scratch, sems
        )
    hidden_out = bf(f32(hidden_in) + res["home0"] + proj_bias + down_bias)
    input_grad = bf(f32(out_cotangent) + res["home1"])
    out_bias_grad = res["out_bias_o"].reshape(-1)
    norm_grads = res["gain_o"]
    return (
        hidden_out,
        input_grad,
        norm_grads[0],
        norm_grads[1],
        norm_grads[2],
        norm_grads[3],
        f32(res["grad2"]),
        res["qkv_bias_o"].reshape(-1),
        f32(res["grad0"]),
        out_bias_grad,
        f32(res["grad3"]),
        res["up_bias_o"].reshape(-1),
        f32(res["grad1"]),
        out_bias_grad,
    )


def solution(mesh):
    matrix = P(("seq", "fsdp"), "tensor")
    vector = P("tensor")
    return jax.shard_map(
        per_device,
        mesh=mesh,
        in_specs=(
            matrix, matrix, P(), P(), P(), P(),
            matrix, vector, matrix, vector, matrix, vector, matrix, vector,
        ),
        out_specs=(
            matrix, matrix, P(), P(), P(), P(),
            matrix, vector, matrix, vector, matrix, vector, matrix, vector,
        ),
        check_vma=False,
    )
```

```python
import functools
import types

import jax
import jax.numpy as jnp
import numpy as np
from jax import lax
from jax.experimental import pallas as pl
from jax.experimental.pallas import tpu as pltpu
from jax.sharding import PartitionSpec as P

HEAD_DIM = 256
ROT = 64
LANES = 128
STRIP = 256
MESH = pl.DeviceIdType.MESH
VMEM_BYTES = 67_043_328
SMALL, WIDE = jnp.bfloat16, jnp.float32

norm_eps = 1e-05
rope_base = 10000.0

WQ, WP, WU1, WU2, WD1, WD2 = range(6)
P1, D1, D2, Q1, U1, U2 = range(6)


def bits_of(size):
    return [1 << b for b in range(size.bit_length() - 1)]


def bf(value):
    return value.astype(jnp.bfloat16)


def f32(value):
    return value.astype(jnp.float32)


def mm(left, right, left_dim, right_dim):
    return lax.dot_general(
        left, right, (((left_dim,), (right_dim,)), ((), ())), preferred_element_type=jnp.float32
    )


def rotary_tables(tok, blocks):
    half = ROT // 2
    frequency = rope_base ** (-np.arange(half, dtype=np.float64) * 2.0 / ROT)
    lanes = np.zeros(LANES)
    lanes[:half] = frequency
    lanes[half:ROT] = frequency
    inner = np.arange(tok, dtype=np.float64)[:, None] * lanes
    outer = np.arange(blocks, dtype=np.float64)[:, None] * tok * lanes
    pack = lambda a: np.stack([np.cos(a), np.sin(a)]).astype(np.float32)
    return (jnp.asarray(pack(inner)), jnp.asarray(pack(outer)))


def flip(rank, mask, size):
    out = jnp.int32(0)
    for b in range(size.bit_length() - 1):
        digit = lax.rem(lax.div(rank, jnp.int32(1 << b)), jnp.int32(2))
        out = out + ((1 - digit) if mask >> b & 1 else digit) * (1 << b)
    return out


def low_bit(j, size):
    return j & -j if j else size


def line_mask(j):
    mask = 0
    b = 0
    while j >> b:
        if j >> b & 1:
            mask ^= (2 << b) - 1
        b += 1
    return mask


def arrivals(size):
    return sorted(range(1, size), key=lambda j: (-low_bit(j, size), j))


def slot_of(j, bit, size):
    index = 0
    for jj in range(size):
        for bb in bits_of(size):
            if bb < low_bit(jj, size):
                if (jj, bb) == (j, bit):
                    return index
                index += 1
    raise ValueError


def at(index, size):
    return pl.ds(pl.multiple_of(index * size, size), size)


def remote(src, dst, send, recv, peer):
    return pltpu.make_async_remote_copy(
        src_ref=src, dst_ref=dst, send_sem=send, recv_sem=recv, device_id=peer, device_id_type=MESH
    )


def repeat(count, body):
    def step(i, carry):
        body(i)
        return carry

    lax.fori_loop(0, count, step, 0)


def turn(value, cos_part, sin_part):
    half = ROT // 2
    head = value[:, :LANES]
    lane = lax.broadcasted_iota(jnp.int32, head.shape, 1)
    other = jnp.where(
        lane < half, -pltpu.roll(head, LANES - half, 1), pltpu.roll(head, half, 1)
    )
    return jnp.concatenate([head * cos_part + other * sin_part, value[:, LANES:]], axis=1)


def make_core(S, T, F):
    c = types.SimpleNamespace(S=S, T=T, F=F)
    c.z, c.y, c.f = lax.axis_index("seq"), lax.axis_index("tensor"), lax.axis_index("fsdp")
    c.fbits, c.sbits = bits_of(F), bits_of(S)
    sends, busy = [], {}

    def start(copy, key=None):
        copy.start()
        sends.append(copy)
        if key is not None:
            busy.setdefault(key, []).append(copy)

    def free(key):
        done = busy.pop(key, [])
        for copy in done:
            copy.wait_send()
        sends[:] = [s for s in sends if not any(s is copy for copy in done)]

    def finish():
        for copy in sends:
            copy.wait_send()

    def greet():
        barrier = pltpu.get_barrier_semaphore()
        peers = [dict(seq=flip(c.z, k, S)) for k in range(1, S)]
        peers += [dict(tensor=flip(c.y, t, T)) for t in range(1, T)]
        peers += [dict(fsdp=flip(c.f, b, F)) for b in c.fbits]
        for peer in peers:
            pl.semaphore_signal(barrier, inc=1, device_id=peer, device_id_type=MESH)
        pl.semaphore_wait(barrier, len(peers))

    c.start, c.free, c.finish, c.greet = start, free, finish, greet
    return c


def gather_ops(c, e):
    S, T, F, z, y, f = c.S, c.T, c.F, c.z, c.y, c.f
    tok, width = e.hid_in.shape
    rows = e.wq_in.shape[0]
    half = e.wu.shape[1] // 2
    tokens = ((e.hid_in, e.hid), (e.cot_in, e.cot))
    weights = (
        (e.wq_in, e.wq, 0, e.wq.shape[1]),
        (e.wp_in, e.wp, 0, e.wp.shape[1]),
        (e.wu_in, e.wu, 0, half),
        (e.wu_in, e.wu, half, half),
        (e.wd_in, e.wd, 0, half),
        (e.wd_in, e.wd, half, half),
    )
    g = types.SimpleNamespace()

    def tok_sem(a, j, t):
        return (a * S + j) * T + t

    def tok_place(a, j, t):
        return tokens[a][1].at[at(flip(z, line_mask(j), S), tok), at(flip(y, t, T), width)]

    def tok_seq(a, j):
        src = tokens[a][0] if j == 0 else tok_place(a, j, 0)
        dst = tok_place(a, j, 0)
        for b in reversed(c.sbits):
            if b < low_bit(j, S):
                i = tok_sem(a, j + b, 0)
                peer = dict(seq=flip(z, line_mask(b), S))
                c.start(remote(src, dst, e.tok_send.at[i], e.tok_recv.at[i], peer))

    def tok_tensor(a, j):
        src = tokens[a][0] if j == 0 else tok_place(a, j, 0)
        dst = tok_place(a, j, 0)
        for t in range(1, T):
            i = tok_sem(a, j, t)
            peer = dict(tensor=flip(y, t, T))
            c.start(remote(src, dst, e.tok_send.at[i], e.tok_recv.at[i], peer))

    def tok_wait(a, j, t):
        i = tok_sem(a, j, t)
        spot = tok_place(a, j, t)
        peer = dict(tensor=flip(y, 1, T))
        remote(spot, spot, e.tok_send.at[i], e.tok_recv.at[i], peer).wait_recv()

    def tok_own(a):
        return pltpu.make_async_copy(tokens[a][0], tok_place(a, 0, 0), e.own_sem.at[a])

    def tok_direct(a, j):
        tok_wait(a, j, 0)
        tok_seq(a, j)
        tok_tensor(a, j)

    def tok_passed(a):
        for j in arrivals(S):
            if j not in c.sbits:
                tok_wait(a, j, 0)
                tok_seq(a, j)
                tok_tensor(a, j)

    def tok_rest(a):
        tok_own(a).wait()
        for j in range(S):
            for t in range(1, T):
                tok_wait(a, j, t)

    def row_sem(m, k, j):
        return (m * S + k) * F + j

    def row_place(m, k, j):
        _, dst, first, size = weights[m]
        return dst.at[at(flip(z, k, S) * F + flip(f, j, F), rows), first : first + size]

    def row_source(m, zd):
        src, dst, first, size = weights[m]
        return src.at[:, pl.ds(pl.multiple_of(zd * dst.shape[1] + first, LANES), size)]

    def row_seq(m, *peers):
        for k in peers or range(1, S):
            i = row_sem(m, k, 0)
            zd = flip(z, k, S)
            src = row_source(m, zd)
            dst = row_place(m, 0, 0)
            c.start(remote(src, dst, e.row_send.at[i], e.row_recv.at[i], dict(seq=zd)))

    def row_forward(m, k, j):
        dst = row_place(m, k, j)
        src = row_source(m, z) if k == 0 and j == 0 else dst
        for b in reversed(c.fbits):
            if b < low_bit(j, F):
                i = row_sem(m, k, j + b)
                peer = dict(fsdp=flip(f, b, F))
                c.start(remote(src, dst, e.row_send.at[i], e.row_recv.at[i], peer))

    def row_wait(m, k, j):
        i = row_sem(m, k, j)
        spot = row_place(m, k, j)
        peer = dict(seq=flip(z, 1, S))
        remote(spot, spot, e.row_send.at[i], e.row_recv.at[i], peer).wait_recv()

    def row_own(m):
        return pltpu.make_async_copy(row_source(m, z), row_place(m, 0, 0), e.own_sem.at[2 + m])

    def row_arrive(m, *peers):
        for k in peers or range(1, S):
            row_wait(m, k, 0)
            row_forward(m, k, 0)

    def row_relay(m):
        for j in arrivals(F):
            if low_bit(j, F) > 1:
                for k in range(S):
                    row_wait(m, k, j)
                    row_forward(m, k, j)

    def row_rest(m):
        row_own(m).wait()
        for j in arrivals(F):
            if low_bit(j, F) == 1:
                for k in range(S):
                    row_wait(m, k, j)

    def begin_own():
        for a in range(2):
            tok_own(a).start()
        for m in range(6):
            row_own(m).start()

    g.tok_seq, g.tok_tensor, g.tok_direct, g.tok_passed = tok_seq, tok_tensor, tok_direct, tok_passed
    g.tok_rest, g.row_seq, g.row_forward, g.row_arrive = tok_rest, row_seq, row_forward, row_arrive
    g.row_relay, g.row_rest, g.begin_own = row_relay, row_rest, begin_own
    return g


def attention_ops(c, e):
    S, T, F, z, y, f = c.S, c.T, c.F, c.z, c.y, c.f
    tok = e.hid_in.shape[0]
    ntok = e.hid.shape[0]
    keys = e.pair.shape[0]
    scale = HEAD_DIM ** (-0.5)
    chunk = 32
    qc = max(32, min(tok, tok * 1024 // keys))
    o = types.SimpleNamespace()

    def norm():
        def norm_chunk(i):
            part = at(i, chunk)
            x = f32(e.hid[part, :])
            mean = jnp.mean(x, axis=-1, keepdims=True)
            centered = x - mean
            inv_std = lax.rsqrt(jnp.mean(centered * centered, axis=-1, keepdims=True) + norm_eps)
            xhat = centered * inv_std
            e.attn_in[part, :] = bf(xhat * e.attn_gain[...] + e.attn_bias[...])
            e.mlp_in[part, :] = bf(xhat * e.mlp_gain[...] + e.mlp_bias[...])
            e.stat[0, part, :] = jnp.broadcast_to(mean, (chunk, LANES))
            e.stat[1, part, :] = jnp.broadcast_to(inv_std, (chunk, LANES))

        repeat(ntok // chunk, norm_chunk)

    def angles(zd, here=slice(None)):
        block = pl.ds(zd * F + f, 1)
        cos_in, sin_in = e.inner[0, here, :], e.inner[1, here, :]
        cos_out, sin_out = e.outer[0, block, :], e.outer[1, block, :]
        return (cos_in * cos_out - sin_in * sin_out, sin_in * cos_out + cos_in * sin_out)

    def qkv():
        bias = e.qkv_bias[:, at(z, 3 * HEAD_DIM)]
        for n in range(3):
            columns = slice(n * HEAD_DIM, (n + 1) * HEAD_DIM)
            part = mm(e.attn_in[...], e.wq[:, columns], 1, 0) + bias[:, columns]
            for zd in range(S):
                piece = part[zd * tok : (zd + 1) * tok]
                if n < 2:
                    piece = turn(piece, *angles(zd))
                if n == 0:
                    e.query[zd * tok : (zd + 1) * tok, :] = bf(piece)
                else:
                    spot = at(zd * F + f, tok)
                    e.pair[spot, (n - 1) * HEAD_DIM : n * HEAD_DIM] = bf(piece)

    def pair_place(zd, j):
        return e.pair.at[at(zd * F + flip(f, j, F), tok), :]

    def pair_forward(zd, j):
        spot = pair_place(zd, j)
        for b in reversed(c.fbits):
            if b < low_bit(j, F):
                i = zd * F + j + b
                peer = dict(fsdp=flip(f, b, F))
                c.start(remote(spot, spot, e.pair_send.at[i], e.pair_recv.at[i], peer), "pair")

    def pair_wait(zd, j):
        i = zd * F + j
        spot = pair_place(zd, j)
        peer = dict(fsdp=flip(f, 1, F))
        remote(spot, spot, e.pair_send.at[i], e.pair_recv.at[i], peer).wait_recv()

    def pair_own():
        for zd in range(S):
            pair_forward(zd, 0)

    def pair_relay():
        for j in arrivals(F):
            if low_bit(j, F) > 1:
                for zd in range(S):
                    pair_wait(zd, j)
                    pair_forward(zd, j)

    def pair_rest():
        for j in arrivals(F):
            if low_bit(j, F) == 1:
                for zd in range(S):
                    pair_wait(zd, j)

    def masked_scores(zd, i, n):
        start_row = zd * tok + i * qc
        q = e.query[pl.ds(pl.multiple_of(start_row, qc), qc), :]
        scores = mm(q, e.pair[:n, :HEAD_DIM], 1, 1) * scale
        last = (zd * F + f) * tok + i * qc
        ahead = lax.broadcasted_iota(jnp.int32, scores.shape, 1) - lax.broadcasted_iota(
            jnp.int32, scores.shape, 0
        )
        return (scores, ahead <= last)

    def forward():
        for zd in range(S):
            n = (zd + 1) * F * tok

            def forward_chunk(i, zd=zd, n=n):
                here = pl.ds(pl.multiple_of(zd * tok + i * qc, qc), qc)
                scores, allowed = masked_scores(zd, i, n)
                top = jnp.max(jnp.where(allowed, scores, -1e30), axis=-1, keepdims=True)
                terms = jnp.where(allowed, jnp.exp(scores - top), 0.0)
                total = jnp.sum(terms, axis=-1, keepdims=True)
                mixed = mm(bf(terms), e.pair[:n, HEAD_DIM:], 1, 0) / total
                e.attn[here, :] = bf(mixed)
                e.row_info[here, :] = jnp.broadcast_to(top + jnp.log(total), (qc, LANES))

            repeat(tok // qc, forward_chunk)

    def backward():
        e.attn_grad[...] = bf(mm(e.cot[...], e.wp[...], 1, 0))
        for zd in range(S):
            n = (zd + 1) * F * tok

            def backward_chunk(i, zd=zd, n=n):
                here = pl.ds(pl.multiple_of(zd * tok + i * qc, qc), qc)
                scores, allowed = masked_scores(zd, i, n)
                weights_here = jnp.where(allowed, jnp.exp(scores - e.row_info[here, :1]), 0.0)
                grad = e.attn_grad[here, :]
                delta = jnp.sum(f32(grad) * f32(e.attn[here, :]), axis=-1, keepdims=True)
                slopes = mm(grad, e.pair[:n, HEAD_DIM:], 1, 1)
                inner_grad = bf(weights_here * (slopes - delta))
                e.probs[here, :n] = bf(weights_here)
                e.score_grad[here, :n] = inner_grad
                if n < keys:
                    blank = jnp.zeros((qc, keys - n), jnp.bfloat16)
                    e.probs[here, n:] = blank
                    e.score_grad[here, n:] = blank
                cos_part, sin_part = angles(zd, pl.ds(pl.multiple_of(i * qc, qc), qc))
                grad_here = mm(inner_grad, e.pair[:n, :HEAD_DIM], 1, 0) * scale
                e.tg[here, :HEAD_DIM] = bf(turn(grad_here, cos_part, -sin_part))

            repeat(tok // qc, backward_chunk)

    def part_sum(j):
        def lanes(ref):
            return jnp.concatenate(
                [ref[:, at(zd * F + flip(f, j, F), tok)] for zd in range(S)], axis=1
            )

        total = jnp.concatenate(
            [
                mm(lanes(e.score_grad), e.query[...], 0, 0) * scale,
                mm(lanes(e.probs), e.attn_grad[...], 0, 0),
            ],
            axis=1,
        )
        for b in c.fbits:
            if b < low_bit(j, F):
                i = slot_of(j, b, F)
                spot = e.part_in.at[i]
                peer = dict(fsdp=flip(f, b, F))
                remote(spot, spot, e.part_send.at[i], e.part_recv.at[i], peer).wait_recv()
                total = total + f32(e.part_in[i])
        return total

    def part_stage(bit):
        c.free("pair")
        for j in range(1, F):
            if low_bit(j, F) == bit:
                spot = e.pair.at[(j - 1) * ntok : j * ntok, :]
                e.pair[(j - 1) * ntok : j * ntok, :] = bf(part_sum(j))
                i = slot_of(j - bit, bit, F)
                peer = dict(fsdp=flip(f, bit, F))
                here = e.part_in.at[i]
                c.start(remote(spot, here, e.part_send.at[j - 1], e.part_recv.at[i], peer))

    def part_later():
        for bit in c.fbits[1:]:
            part_stage(bit)

    def part_home():
        total = part_sum(0)
        for zd in range(S):
            here = slice(zd * tok, (zd + 1) * tok)
            cos_part, sin_part = angles(zd)
            key_part = turn(total[here, :HEAD_DIM], cos_part, -sin_part)
            e.tg[here, HEAD_DIM : 2 * HEAD_DIM] = bf(key_part)
            e.tg[here, 2 * HEAD_DIM :] = bf(total[here, HEAD_DIM:])

    def up(first, size):
        cols = e.wu.shape[1]
        for n in range(first // STRIP, (first + size) // STRIP):
            strip = slice(n * STRIP, (n + 1) * STRIP)
            bias = e.up_bias[:, pl.ds(pl.multiple_of(z * cols + n * STRIP, STRIP), STRIP)]
            mid = mm(e.mlp_in[...], e.wu[:, strip], 1, 0) + bias
            cdf = 0.5 * (1.0 + lax.erf(mid * 0.7071067811865476))
            e.active[:, strip] = bf(mid * cdf)
            e.slope[:, strip] = cdf + mid * jnp.exp(-0.5 * mid * mid) * 0.3989422804014327

    o.norm, o.qkv, o.pair_own, o.pair_relay, o.pair_rest = norm, qkv, pair_own, pair_relay, pair_rest
    o.forward, o.backward, o.part_stage, o.part_later = forward, backward, part_stage, part_later
    o.part_home, o.up = part_home, up
    return o


def grad_units(ff):
    half = ff // 2
    return (
        (0, 0, HEAD_DIM),
        (1, 0, half),
        (1, half, half),
        (2, 0, 3 * HEAD_DIM),
        (3, 0, half),
        (3, half, half),
    )


def spread_ops(c, e, turned):
    S, T, F, z, y, f = c.S, c.T, c.F, c.z, c.y, c.f
    tok, width = e.homes[0].shape
    ntok, D = e.wide.shape
    ff = e.active.shape[1]
    rows = e.grads[0].shape[0]
    rights, lefts = (e.attn, e.active, e.tg, e.pre), (e.cot, e.cot, e.attn_in, e.mlp_in)
    units = grad_units(ff)
    n_u = len(units)
    p = types.SimpleNamespace()

    def block_sum(u, j):
        g, first, size = units[u]
        right, left = rights[g].at[:, first : first + size], lefts[g]
        fd = flip(f, j, F)
        if turned:
            block = jnp.concatenate([left[at(zd * F + fd, rows), :] for zd in range(S)], axis=0)
            total = mm(block, right[...], 1, 0)
        else:
            block = jnp.concatenate([left[:, at(zd * F + fd, rows)] for zd in range(S)], axis=1)
            total = mm(block, right[...], 0, 0)
        for bit in c.fbits:
            if bit < low_bit(j, F):
                s = slot_of(j, bit, F)
                i = u * (F - 1) + s
                spot = e.in_b[u].at[s]
                peer = dict(fsdp=flip(f, bit, F))
                remote(spot, spot, e.out_sem.at[i], e.in_sem.at[i], peer).wait_recv()
                total = total + f32(e.in_b[u][s])
        return total

    def fsdp_stage(u, bit):
        for j in range(1, F):
            if low_bit(j, F) == bit:
                key, spot = e.out_spot(u, j)
                c.free(key)
                spot[...] = bf(block_sum(u, j))
                there = slot_of(j - bit, bit, F)
                send = e.out_sem.at[u * (F - 1) + j - 1]
                recv = e.in_sem.at[u * (F - 1) + there]
                peer = dict(fsdp=flip(f, bit, F))
                c.start(remote(spot, e.in_b[u].at[there], send, recv, peer), key)

    def first(u):
        fsdp_stage(u, c.fbits[0])

    def later(u):
        for bit in c.fbits[1:]:
            fsdp_stage(u, bit)

    def grad_place(u, zd):
        g, first_col, size = units[u]
        start_col = zd * rights[g].shape[1] + first_col
        return e.grads[g].at[:, pl.ds(pl.multiple_of(start_col, LANES), size)]

    def own_grad(u):
        src = e.seq_b[u].at[at(z, rows), :]
        return pltpu.make_async_copy(src, grad_place(u, z), e.home_sem.at[u])

    def seq(u):
        e.seq_b[u][...] = bf(block_sum(u, 0))
        own_grad(u).start()

    def seq_send(u, *peers):
        for k in peers or range(1, S):
            peer = flip(z, k, S)
            src, dst = e.seq_b[u].at[at(peer, rows), :], grad_place(u, z)
            i = u * S + k
            c.start(remote(src, dst, e.seq_send.at[i], e.seq_recv.at[i], dict(seq=peer)))

    def seq_wait():
        for u in range(n_u):
            for k in range(1, S):
                peer = flip(z, k, S)
                spot = grad_place(u, peer)
                i = u * S + k
                remote(spot, spot, e.seq_send.at[i], e.seq_recv.at[i], dict(seq=peer)).wait_recv()
            own_grad(u).wait()

    def half_strips(s, t, term):
        for n in range(width // STRIP):
            there = pl.ds(pl.multiple_of(flip(y, t, T) * width + n * STRIP, STRIP), STRIP)
            here = slice(n * STRIP, (n + 1) * STRIP)
            value = term(there)
            if t:
                for zd in range(S):
                    e.y_out[(t - 1) * S + zd, :, here] = bf(value[zd * tok : (zd + 1) * tok])
            elif s == 0:
                e.own_half[:, here] = value
            else:
                e.wide[:, there] = value

    def y_index(s, t, j):
        return (s * max(T - 1, 1) + t - 1) * S + j

    def tensor_send(s):
        for j in [*sorted(range(1, S), key=lambda j: (low_bit(j, S), j)), 0]:
            zd = flip(z, line_mask(j), S)
            for t in range(1, T):
                i = y_index(s, t, j)
                peer = dict(tensor=flip(y, t, T))
                here = e.y_out.at[(t - 1) * S + zd]
                c.start(remote(here, e.y_in.at[i], e.y_send.at[i], e.y_recv.at[i], peer), "y")

    def token_own(s, zd):
        if s == 0:
            return e.own_half.at[at(zd, tok), :]
        return e.wide.at[at(zd, tok), at(y, width)]

    def token_part(s, j):
        total = token_own(s, flip(z, line_mask(j), S))[...]
        for t in range(1, T):
            i = y_index(s, t, j)
            spot = e.y_in.at[i]
            peer = dict(tensor=flip(y, t, T))
            remote(spot, spot, e.y_send.at[i], e.y_recv.at[i], peer).wait_recv()
            total = total + f32(e.y_in[i])
        for bit in c.sbits:
            if bit < low_bit(j, S):
                i = s * (S - 1) + slot_of(j, bit, S)
                spot = e.z_in.at[i]
                peer = dict(seq=flip(z, line_mask(bit), S))
                remote(spot, spot, e.z_send.at[i], e.z_recv.at[i], peer).wait_recv()
                total = total + f32(e.z_in[i])
        return total

    def token_send(s, j):
        bit = low_bit(j, S)
        i = s * (S - 1) + j - 1
        there = s * (S - 1) + slot_of(j - bit, bit, S)
        c.free(("z", j))
        e.z_out[j - 1] = bf(token_part(s, j))
        peer = dict(seq=flip(z, line_mask(bit), S))
        here = e.z_out.at[j - 1]
        copy = remote(here, e.z_in.at[there], e.z_send.at[i], e.z_recv.at[there], peer)
        c.start(copy, ("z", j))

    def token_sends(s):
        for j in sorted(range(1, S), key=lambda j: (low_bit(j, S), j)):
            token_send(s, j)

    def home_copy(s):
        return pltpu.make_async_copy(token_own(s, z), e.homes[s], e.home_sem.at[n_u + s])

    def token_home(s):
        total = token_part(s, 0)
        token_own(s, z)[...] = total
        home_copy(s).start()

    def home_wait():
        for s in range(2):
            home_copy(s).wait()

    n_f = len(c.fbits)
    vec = e.vec

    def vec_copy(b):
        peer = dict(fsdp=flip(f, c.fbits[b], F))
        return remote(vec.at[b], e.vec_in.at[b], e.v_send.at[b], e.v_recv.at[b], peer)

    def vec_start(b):
        c.start(vec_copy(b))

    def vec_sum(b):
        vec_copy(b).wait_recv()
        vec[b + 1] = vec[b] + e.vec_in[b]

    def vec_fsdp():
        for b in range(n_f - 1):
            vec_sum(b)
            vec_start(b + 1)

    def vec_seq_copy(k):
        peer = dict(seq=flip(z, k, S))
        i = n_f + k - 1
        return remote(vec.at[n_f], e.vec_seq.at[k - 1], e.v_send.at[i], e.v_recv.at[i], peer)

    def vec_seq_start():
        vec_sum(n_f - 1)
        for k in range(1, S):
            c.start(vec_seq_copy(k))

    def tree(parts):
        while len(parts) > 1:
            parts = [a + b for a, b in zip(parts[::2], parts[1::2])]
        return parts[0]

    def vec_seq_sum():
        parts = []
        for k in range(S):
            if k:
                vec_seq_copy(k).wait_recv()
            value = vec[n_f] if k == 0 else e.vec_seq[k - 1]
            zd = flip(z, k, S)
            e.qkv_bias_o[:, at(zd, 3 * HEAD_DIM)] = value[4:5, : 3 * HEAD_DIM]
            e.up_bias_o[:, at(zd, ff)] = value[5:6, :ff]
            parts.append(value)
        total = tree(parts)
        e.out_bias_o[...] = total[6:7, :width]
        e.vec_ten[0] = total[:4]
        for t in range(1, T):
            c.start(vec_ten_copy(t))

    def vec_ten_copy(t):
        peer = dict(tensor=flip(y, t, T))
        i = n_f + S - 1 + t - 1
        return remote(e.vec_ten.at[0], e.vec_ten.at[t], e.v_send.at[i], e.v_recv.at[i], peer)

    def vec_ten_sum():
        parts = [e.vec_ten[0]]
        for t in range(1, T):
            vec_ten_copy(t).wait_recv()
            parts.append(e.vec_ten[t])
        e.gain_o[...] = tree(parts)

    def branch():
        def term(column):
            return mm(e.active[...], e.wd[column, :], 1, 1) + mm(e.attn[...], e.wp[column, :], 1, 1)

        for t in range(1, T):
            half_strips(0, t, term)
        tensor_send(0)
        return lambda: half_strips(0, 0, term)

    def hidden_grad():
        vec[0] = jnp.zeros(vec.shape[1:], jnp.float32)
        for n in range(ff // STRIP):
            here = slice(n * STRIP, (n + 1) * STRIP)
            value = mm(e.cot[...], e.wd[:, here], 0 if turned else 1, 0) * e.slope[:, here]
            vec[0, 5:6, here] = jnp.sum(value, axis=0, keepdims=True)
            e.pre[:, here] = bf(value)

    def unit_rows(column):
        mean, inv_std = e.stat[0, :, :1], e.stat[1, :, :1]
        return ((f32(e.hid[:, column]) - mean) * inv_std, inv_std)

    def norm_strips():
        lane_parts = range(0, STRIP, LANES)

        def norm_strip(n):
            here = at(n, STRIP)
            a = mm(e.tg[...], e.wq[here, :], 1, 1)
            m = mm(e.pre[...], e.wu[here, :], 1, 1)
            xhat, _ = unit_rows(here)
            vec[0, 0:1, here] = jnp.sum(a * xhat, axis=0, keepdims=True)
            vec[0, 1:2, here] = jnp.sum(a, axis=0, keepdims=True)
            vec[0, 2:3, here] = jnp.sum(m * xhat, axis=0, keepdims=True)
            vec[0, 3:4, here] = jnp.sum(m, axis=0, keepdims=True)
            both = a * e.attn_gain[:, here] + m * e.mlp_gain[:, here]
            e.wide[:, here] = both
            scaled = both * xhat
            e.sums[0] += sum(both[:, i : i + LANES] for i in lane_parts)
            e.sums[1] += sum(scaled[:, i : i + LANES] for i in lane_parts)

        e.sums[...] = jnp.zeros_like(e.sums)
        repeat(D // STRIP, norm_strip)
        vec[0, 4:5, : 3 * HEAD_DIM] = jnp.sum(f32(e.tg[...]), axis=0, keepdims=True)
        vec[0, 6:7, :width] = jnp.sum(f32(e.own_cot()), axis=0, keepdims=True)
        vec_start(0)
        for i in range(2):
            mean = jnp.sum(e.sums[i], axis=-1, keepdims=True) / D
            e.sums[i] = jnp.broadcast_to(mean, e.sums.shape[1:])

    def input_strips():
        def term(column):
            xhat, inv_std = unit_rows(column)
            return inv_std * (e.wide[:, column] - e.sums[0, :, :1] - xhat * e.sums[1, :, :1])

        c.free("y")
        for t in range(1, T):
            half_strips(1, t, term)
        tensor_send(1)
        return lambda: half_strips(1, 0, term)

    p.first, p.later, p.seq, p.seq_send, p.seq_wait = first, later, seq, seq_send, seq_wait
    p.token_send, p.token_sends, p.token_home = token_send, token_sends, token_home
    p.home_wait, p.vec_fsdp = home_wait, vec_fsdp
    p.vec_seq_start, p.vec_seq_sum, p.vec_ten_sum = vec_seq_start, vec_seq_sum, vec_ten_sum
    p.branch, p.hidden_grad, p.norm_strips, p.input_strips = (
        branch,
        hidden_grad,
        norm_strips,
        input_strips,
    )
    return p


def gather_buffers(S, T, F, tok, width, rows, ff):
    ntok, D, keys = S * tok, T * width, S * F * tok
    kept = dict(
        hid=((ntok, D), SMALL),
        cot=((ntok, D), SMALL),
        attn_in=((ntok, D), SMALL),
        mlp_in=((ntok, D), SMALL),
        stat=((2, ntok, LANES), WIDE),
        wq=((D, 3 * HEAD_DIM), SMALL),
        wp=((D, HEAD_DIM), SMALL),
        wu=((D, ff), SMALL),
        wd=((D, ff), SMALL),
        attn=((ntok, HEAD_DIM), SMALL),
        active=((ntok, ff), SMALL),
        tg=((ntok, 3 * HEAD_DIM), SMALL),
    )
    passing = dict(
        query=((ntok, HEAD_DIM), SMALL),
        pair=((keys, 2 * HEAD_DIM), SMALL),
        attn_grad=((ntok, HEAD_DIM), SMALL),
        probs=((ntok, keys), SMALL),
        score_grad=((ntok, keys), SMALL),
        row_info=((ntok, LANES), WIDE),
        part_in=((max(F - 1, 1), ntok, 2 * HEAD_DIM), SMALL),
    )
    sems = dict(
        own_sem=8,
        tok_send=2 * S * T,
        tok_recv=2 * S * T,
        row_send=6 * S * F,
        row_recv=6 * S * F,
        pair_send=S * F,
        pair_recv=S * F,
        part_send=max(F - 1, 1),
        part_recv=max(F - 1, 1),
    )
    return kept, passing, sems


def spread_buffers(S, T, F, tok, width, rows, ff):
    ntok, D = S * tok, T * width
    n_f, n_y, parts = len(bits_of(F)), max(T - 1, 1) * S, max(F - 1, 1)
    held = dict(
        pre=((ntok, ff), SMALL),
        wide=((ntok, D), WIDE),
        own_half=((ntok, width), WIDE),
        sums=((2, ntok, LANES), WIDE),
        vec=((n_f + 1, 8, D), WIDE),
        vec_in=((n_f, 8, D), WIDE),
        vec_seq=((max(S - 1, 1), 8, D), WIDE),
        vec_ten=((T, 4, D), WIDE),
        y_out=((n_y, tok, width), SMALL),
        y_in=((2 * n_y, tok, width), SMALL),
        z_out=((max(S - 1, 1), tok, width), SMALL),
        z_in=((2 * max(S - 1, 1), tok, width), SMALL),
    )
    for u, (_, _, size) in enumerate(grad_units(ff)):
        held[f"in_b{u}"] = ((parts, S * rows, size), SMALL)
        held[f"seq_b{u}"] = ((S * rows, size), SMALL)
    sems = dict(
        home_sem=8,
        out_sem=6 * parts,
        in_sem=6 * parts,
        seq_send=6 * S,
        seq_recv=6 * S,
        y_send=2 * n_y,
        y_recv=2 * n_y,
        z_send=2 * max(S - 1, 1),
        z_recv=2 * max(S - 1, 1),
        v_send=n_f + S + T,
        v_recv=n_f + S + T,
    )
    outs = {f"grad{g}": ((rows, S * n), SMALL) for g, n in enumerate((HEAD_DIM, ff, 3 * HEAD_DIM, ff))}
    outs |= {f"home{s}": ((tok, width), WIDE) for s in range(2)}
    vectors = dict(
        gain_o=((4, D), WIDE),
        qkv_bias_o=((1, 3 * width), WIDE),
        up_bias_o=((1, S * ff), WIDE),
        out_bias_o=((1, width), WIDE),
    )
    return held, sems, outs, vectors


def send_buffers(S, F, rows, ff, units):
    sizes = [size for _, _, size in grad_units(ff)]
    return {f"out_b{u}": ((max(F - 1, 1), S * rows, sizes[u]), SMALL) for u in units}


def gather_lists(e):
    e.in_b = [getattr(e, f"in_b{u}") for u in range(6)]
    e.seq_b = [getattr(e, f"seq_b{u}") for u in range(6)]
    e.grads = [getattr(e, f"grad{g}") for g in range(4)]
    e.homes = [e.home0, e.home1]


def launch(body, sizes, collective, far, near, outs, near_outs, scratch, sems, **lists):
    names = [*far, *near, *outs, *near_outs, *scratch, *sems]

    def kernel(*refs):
        body(types.SimpleNamespace(**dict(zip(names, refs)), **lists), *sizes)

    kernel.__name__ = body.__name__
    any_spec = pl.BlockSpec(memory_space=pl.ANY)
    vmem = pl.BlockSpec(memory_space=pltpu.VMEM)
    results = pl.pallas_call(
        kernel,
        out_shape=[jax.ShapeDtypeStruct(*o) for o in [*outs.values(), *near_outs.values()]],
        in_specs=[any_spec] * len(far) + [vmem] * len(near),
        out_specs=[any_spec] * len(outs) + [vmem] * len(near_outs),
        scratch_shapes=[pltpu.VMEM(*s) for s in scratch.values()]
        + [pltpu.SemaphoreType.DMA((n,)) for n in sems.values()],
        compiler_params=pltpu.CompilerParams(
            collective_id=collective, has_side_effects=True, vmem_limit_bytes=VMEM_BYTES
        ),
    )(*far.values(), *near.values())
    return dict(zip([*outs, *near_outs], results))


def whole_kernel(e, S, T, F):
    c = make_core(S, T, F)
    width = e.hid_in.shape[1]
    tok = e.hid_in.shape[0]
    ff = e.active.shape[1]
    half = ff // 2
    gather_lists(e)
    e.slope = e.wide.at[:, :ff]
    e.row_info = e.sums.at[0]
    e.own_cot = lambda: e.cot[at(c.z, tok), at(c.y, width)]
    wide_q = 3 * HEAD_DIM
    lent = [e.probs.at[:, :wide_q], e.probs.at[:, wide_q : 2 * wide_q], e.score_grad.at[:, :wide_q]]

    def out_spot(u, j):
        if u == Q1:
            return (("out", u, j), lent[j - 1])
        shared = {U1: D1, U2: D2}.get(u, u)
        return (("out", shared, j), getattr(e, f"out_b{shared}").at[j - 1])

    e.out_spot = out_spot
    g, o, p = gather_ops(c, e), attention_ops(c, e), spread_ops(c, e, False)
    near, vectors = e.near_names, e.vector_names

    def near_copy(i):
        return pltpu.make_async_copy(getattr(e, near[i] + "_i"), getattr(e, near[i]), e.near_sem.at[i])

    def vec_copy(i):
        return pltpu.make_async_copy(getattr(e, vectors[i]), getattr(e, vectors[i] + "_h"), e.vec_sem.at[i])

    def begin():
        g.begin_own()
        for i in range(len(near)):
            near_copy(i).start()

    def norm():
        for i in range(len(near)):
            near_copy(i).wait()
        o.norm()

    def vec_home():
        p.vec_ten_sum()
        for i in range(len(vectors)):
            vec_copy(i).start()

    c.greet()
    g.row_seq(WU1, 3)
    g.row_seq(WU2, 1)
    g.row_forward(WD2, 0, 0)
    g.row_forward(WQ, 0, 0)
    g.row_forward(WP, 0, 0)
    g.tok_tensor(0, 0)
    g.row_seq(WP, 1)
    g.row_seq(WU2, 3)
    g.row_arrive(WU1, 3)
    g.row_seq(WQ, 1)
    g.row_arrive(WU2, 3)
    g.row_arrive(WU2, 1)
    g.row_forward(WU2, 0, 0)
    g.row_seq(WQ, 3)
    g.row_arrive(WQ, 1)
    g.tok_seq(0, 0)
    begin()
    g.tok_direct(0, 1)
    g.row_seq(WU1, 2)
    g.row_seq(WU1, 1)
    g.row_forward(WU1, 0, 0)
    g.tok_tensor(1, 0)
    g.row_arrive(WP, 1)
    g.row_forward(WD1, 0, 0)
    g.tok_direct(0, 2)
    g.row_arrive(WQ, 3)
    g.row_seq(WP, 2)
    g.row_seq(WQ, 2)
    g.row_arrive(WU1, 1)
    g.tok_passed(0)
    g.row_seq(WD2, 1)
    g.row_arrive(WU1, 2)
    g.tok_seq(1, 0)
    g.tok_rest(0)
    g.row_arrive(WQ, 2)
    g.row_arrive(WP, 2)
    g.row_arrive(WD2, 1)
    g.row_seq(WP, 3)
    norm()
    g.row_relay(WQ)
    g.row_rest(WQ)
    g.row_relay(WU1)
    g.row_seq(WU2, 2)
    g.row_seq(WD1, 1)
    g.row_rest(WU1)
    g.row_arrive(WP, 3)
    g.tok_direct(1, 1)
    o.qkv()
    o.pair_own()
    g.row_seq(WD1, 3)
    g.tok_direct(1, 2)
    g.row_arrive(WD1, 1)
    o.up(0, half)
    g.row_seq(WD2, 2)
    g.row_seq(WD2, 3)
    g.row_arrive(WD1, 3)
    g.row_arrive(WU2, 2)
    o.pair_relay()
    o.pair_rest()
    g.tok_passed(1)
    g.row_arrive(WD2, 2)
    g.row_seq(WD1, 2)
    o.forward()
    g.row_arrive(WD2, 3)
    g.tok_rest(1)
    p.first(D1)
    g.row_arrive(WD1, 2)
    g.row_relay(WU2)
    g.row_relay(WD2)
    p.later(D1)
    g.row_rest(WU2)
    p.first(P1)
    g.row_relay(WD1)
    g.row_rest(WD2)
    o.up(half, half)
    g.row_relay(WP)
    p.first(D2)
    g.row_rest(WP)
    p.later(D2)
    g.row_rest(WD1)
    own_strips = p.branch()
    p.later(P1)
    p.seq(D1)
    p.seq_send(D1, 3)
    own_strips()
    p.seq_send(D1, 2)
    p.seq_send(D1, 1)
    o.backward()
    o.part_stage(c.fbits[0])
    p.seq(D2)
    p.seq_send(D2, 3)
    p.token_send(0, 3)
    o.part_later()
    p.seq(P1)
    p.seq_send(D2, 2)
    p.hidden_grad()
    p.first(U1)
    p.seq_send(P1, 2)
    p.first(U2)
    p.token_send(0, 1)
    p.later(U1)
    p.seq_send(D2, 1)
    p.seq_send(P1, 3)
    p.token_send(0, 2)
    o.part_home()
    p.norm_strips()
    own_terms = p.input_strips()
    p.first(Q1)
    p.seq(U1)
    p.seq_send(U1, 2)
    p.seq_send(P1, 1)
    p.vec_fsdp()
    own_terms()
    p.vec_seq_start()
    p.later(U2)
    p.token_send(1, 3)
    p.later(Q1)
    p.seq_send(U1, 3)
    p.seq(U2)
    p.seq_send(U2, 2)
    p.token_send(1, 2)
    p.token_send(1, 1)
    p.seq(Q1)
    p.seq_send(Q1, 2)
    p.vec_seq_sum()
    p.token_home(0)
    p.seq_send(U1, 1)
    p.seq_send(U2, 1)
    p.seq_send(Q1, 1)
    p.seq_send(U2, 3)
    p.seq_send(Q1, 3)
    vec_home()
    p.token_home(1)
    p.seq_wait()
    p.home_wait()
    for i in range(len(vectors)):
        vec_copy(i).wait()
    c.finish()


def first_kernel(e, S, T, F):
    c = make_core(S, T, F)
    half = e.active.shape[1] // 2
    g, o = gather_ops(c, e), attention_ops(c, e)
    names = e.kept_names

    def out_copy(name):
        i = names.index(name)
        return pltpu.make_async_copy(getattr(e, name), getattr(e, name + "_o"), e.put_sem.at[i])

    c.greet()
    g.tok_seq(0, 0)
    g.tok_tensor(0, 0)
    for m in range(6):
        g.row_forward(m, 0, 0)
    g.begin_own()
    for j in c.sbits:
        g.tok_direct(0, j)
    g.row_seq(WQ)
    g.tok_passed(0)
    g.row_seq(WU1)
    g.tok_tensor(1, 0)
    g.tok_rest(0)
    o.norm()
    g.row_arrive(WQ)
    g.tok_seq(1, 0)
    g.row_relay(WQ)
    g.row_rest(WQ)
    o.qkv()
    o.pair_own()
    g.row_arrive(WU1)
    for m in (WP, WU2, WD1, WD2):
        g.row_seq(m)
    for j in c.sbits:
        g.tok_direct(1, j)
    g.row_relay(WU1)
    o.pair_relay()
    g.tok_passed(1)
    g.row_rest(WU1)
    o.up(0, half)
    g.row_arrive(WP)
    o.pair_rest()
    o.forward()
    g.row_arrive(WU2)
    g.tok_rest(1)
    g.row_relay(WP)
    g.row_rest(WP)
    o.backward()
    o.part_stage(c.fbits[0])
    g.row_relay(WU2)
    g.row_rest(WU2)
    o.up(half, half)
    o.part_later()
    g.row_arrive(WD1)
    g.row_arrive(WD2)
    o.part_home()
    for m in (WD1, WD2):
        g.row_relay(m)
        g.row_rest(m)
    for name in names:
        out_copy(name).start()
    for name in names:
        out_copy(name).wait()
    c.finish()


def second_kernel(e, S, T, F, turned):
    c = make_core(S, T, F)
    gather_lists(e)
    ff = e.active.shape[1]
    e.slope = e.wide.at[:, :ff]
    e.own_cot = lambda: e.own_cot_in[...]
    e.out_spot = lambda u, j: (("out", u, j), getattr(e, f"out_b{u}").at[j - 1])
    e.wd = e.wu = e.wud
    p = spread_ops(c, e, turned)
    names = e.kept_names

    def load(name):
        i = names.index(name)
        return pltpu.make_async_copy(getattr(e, name + "_i"), getattr(e, name), e.load_sem.at[i])

    for name in names:
        if name != "wu":
            load(name).start()
    c.greet()
    for name in names:
        if name != "wu":
            load(name).wait()
    p.first(P1)
    p.first(D1)
    p.first(D2)
    own_strips = p.branch()
    p.later(P1)
    own_strips()
    p.later(D1)
    p.hidden_grad()
    load("wu").start()
    p.seq(P1)
    p.seq_send(P1)
    p.later(D2)
    p.token_sends(0)
    p.first(Q1)
    p.first(U1)
    p.first(U2)
    load("wu").wait()
    p.norm_strips()
    p.seq(D1)
    p.seq_send(D1)
    p.later(Q1)
    own_terms = p.input_strips()
    own_terms()
    p.token_home(0)
    p.seq(D2)
    p.seq_send(D2)
    p.later(U1)
    p.vec_fsdp()
    p.seq(Q1)
    p.seq_send(Q1)
    p.later(U2)
    p.vec_seq_start()
    p.token_sends(1)
    p.seq(U1)
    p.seq_send(U1)
    p.seq(U2)
    p.seq_send(U2)
    p.vec_seq_sum()
    p.vec_ten_sum()
    p.token_home(1)
    p.seq_wait()
    p.home_wait()
    c.finish()


def per_device(
    hidden_in,
    out_cotangent,
    attn_norm_gain,
    attn_norm_bias,
    mlp_norm_gain,
    mlp_norm_bias,
    qkv_weight,
    qkv_bias,
    proj_weight,
    proj_bias,
    up_weight,
    up_bias,
    down_weight,
    down_bias,
):
    S, T, F = [lax.axis_size(a) for a in ("seq", "tensor", "fsdp")]
    tok, width = hidden_in.shape
    rows, ff = qkv_weight.shape[0], up_weight.shape[1] // S
    if width != S * HEAD_DIM or S * F * rows != T * width:
        raise ValueError
    shape = (S, T, F, tok, width, rows, ff)
    inner, outer = rotary_tables(tok, S * F)
    far = dict(
        hid_in=hidden_in,
        cot_in=out_cotangent,
        wq_in=qkv_weight,
        wp_in=proj_weight,
        wu_in=up_weight,
        wd_in=down_weight,
    )
    row = lambda v: v.reshape(1, -1)
    gains = dict(attn_gain=row(attn_norm_gain), mlp_gain=row(mlp_norm_gain))
    near = gains | dict(
        attn_bias=row(attn_norm_bias),
        mlp_bias=row(mlp_norm_bias),
        qkv_bias=row(qkv_bias),
        up_bias=row(up_bias),
        inner=inner,
        outer=outer,
    )
    kept, passing, gather_sems = gather_buffers(*shape)
    held, spread_sems, outs, vectors = spread_buffers(*shape)
    if rows % LANES == 0 and (S, T, F) == (4, 2, 4):
        scratch = kept | passing | held | send_buffers(S, F, rows, ff, (P1, D1, D2)) | vectors
        scratch |= {k: (v.shape, v.dtype) for k, v in near.items()}
        del scratch["row_info"]
        sems = gather_sems | spread_sems | dict(near_sem=len(near), vec_sem=len(vectors))
        far |= {k + "_i": v for k, v in near.items()}
        outs |= {k + "_h": v for k, v in vectors.items()}
        lists = dict(near_names=list(near), vector_names=list(vectors))
        res = launch(whole_kernel, (S, T, F), 0, far, {}, outs, {}, scratch, sems, **lists)
        res |= {k: res[k + "_h"] for k in vectors}
    else:
        slope = dict(slope=((S * tok, ff), WIDE))
        saved = {k + "_o": v for k, v in (kept | slope).items()}
        sems = gather_sems | dict(put_sem=len(saved))
        scratch = kept | slope | passing
        lists = dict(kept_names=[*kept, *slope])
        mid = launch(first_kernel, (S, T, F), 0, far, near, saved, {}, scratch, sems, **lists)
        turned = rows % LANES != 0
        if turned:
            for k in ("cot_o", "attn_in_o", "mlp_in_o"):
                mid[k] = mid[k].T
        ins = {k[:-2] + "_i": v for k, v in mid.items()}
        scratch = {k: (ins[k + "_i"].shape, t) for k, (_, t) in kept.items() if k not in ("wu", "wd")}
        scratch |= dict(wud=kept["wu"]) | held | send_buffers(S, F, rows, ff, range(6))
        near = gains | dict(own_cot_in=out_cotangent)
        sems = spread_sems | dict(load_sem=len(ins))
        res = launch(
            second_kernel, (S, T, F, turned), 1, ins, near, outs, vectors, scratch, sems, **lists
        )
    return finish(res, hidden_in, out_cotangent, row(proj_bias), row(down_bias))


def last_kernel(*refs):
    sources, (gain, qkv_b, up_b, out_b, proj_bias, down_bias), refs = refs[:8], refs[8:14], refs[14:]
    outs, refs = refs[:14], refs[14:]
    held, wide, (hidden, norm, load_sem, out_sem) = refs[:8], refs[8:12], refs[12:]
    loads = [pltpu.make_async_copy(a, b, load_sem.at[i]) for i, (a, b) in enumerate(zip(sources, held))]
    for copy in loads:
        copy.start()
    stores = []

    def store(src, dst):
        copy = pltpu.make_async_copy(src, dst, out_sem.at[len(stores)])
        copy.start()
        stores.append(copy)

    for i in range(4):
        store(gain.at[i : i + 1, :], outs[2 + i])
    for i, ref in enumerate((qkv_b, out_b, up_b, out_b)):
        store(ref, outs[7 + 2 * i])
    for i in range(4):
        loads[i].wait()
        rows = held[i].shape[0]
        step = max(16, rows // 4)
        for r in range(0, rows, step):
            part = slice(r, r + step)
            wide[i][part, :] = f32(held[i][part, :])
            store(wide[i].at[part, :], outs[6 + 2 * i].at[part, :])
    for copy in loads[4:]:
        copy.wait()
    hidden[...] = bf(f32(held[6][...]) + held[4][...] + proj_bias[...] + down_bias[...])
    norm[...] = bf(f32(held[7][...]) + held[5][...])
    store(hidden, outs[0])
    store(norm, outs[1])
    for copy in stores:
        copy.wait()


def finish(res, hidden_in, out_cotangent, proj_bias, down_bias):
    r = types.SimpleNamespace(**res)
    far = [r.grad2, r.grad0, r.grad3, r.grad1, r.home0, r.home1, hidden_in, out_cotangent]
    near = [r.gain_o, r.qkv_bias_o, r.up_bias_o, r.out_bias_o, proj_bias, down_bias]
    shape = jax.ShapeDtypeStruct
    D = r.gain_o.shape[1]
    qkv_b, up_b, out_b = [shape(v.shape, WIDE) for v in near[1:4]]
    big = [shape(a.shape, WIDE) for a in far[:4]]
    outs = [shape(hidden_in.shape, SMALL)] * 2 + [shape((1, D), WIDE)] * 4
    outs += [big[0], qkv_b, big[1], out_b, big[2], up_b, big[3], out_b]
    any_spec = pl.BlockSpec(memory_space=pl.ANY)
    vmem = pl.BlockSpec(memory_space=pltpu.VMEM)
    results = pl.pallas_call(
        last_kernel,
        out_shape=outs,
        in_specs=[any_spec] * len(far) + [vmem] * len(near),
        out_specs=[any_spec] * len(outs),
        scratch_shapes=[pltpu.VMEM(a.shape, a.dtype) for a in far]
        + [pltpu.VMEM(a.shape, WIDE) for a in far[:4]]
        + [pltpu.VMEM(hidden_in.shape, SMALL)] * 2
        + [pltpu.SemaphoreType.DMA((len(far),)), pltpu.SemaphoreType.DMA((32,))],
        compiler_params=pltpu.CompilerParams(vmem_limit_bytes=VMEM_BYTES),
    )(*far, *near)
    flat = {2, 3, 4, 5, 7, 9, 11, 13}
    return tuple(v.reshape(-1) if i in flat else v for i, v in enumerate(results))


def solution(mesh):
    matrix = P(("seq", "fsdp"), "tensor")
    vector = P("tensor")
    return jax.shard_map(
        per_device,
        mesh=mesh,
        in_specs=(
            matrix, matrix, P(), P(), P(), P(),
            matrix, vector, matrix, vector, matrix, vector, matrix, vector,
        ),
        out_specs=(
            matrix, matrix, P(), P(), P(), P(),
            matrix, vector, matrix, vector, matrix, vector, matrix, vector,
        ),
        check_vma=False,
    )
```

```python
import functools
import types

import jax
import jax.numpy as jnp
import numpy as np
from jax import lax
from jax.experimental import pallas as pl
from jax.experimental.pallas import tpu as pltpu
from jax.sharding import PartitionSpec as P

HEAD_DIM = 256
ROT = 64
LANES = 128
STRIP = 256
MESH = pl.DeviceIdType.MESH
VMEM_BYTES = 67_043_328
SMALL, WIDE = jnp.bfloat16, jnp.float32

norm_eps = 1e-05
rope_base = 10000.0

WQ, WP, WU1, WU2, WD1, WD2 = range(6)
P1, D1, D2, Q1, U1, U2 = range(6)


def bits_of(size):
    return [1 << b for b in range(size.bit_length() - 1)]


def bf(value):
    return value.astype(jnp.bfloat16)


def f32(value):
    return value.astype(jnp.float32)


def mm(left, right, left_dim, right_dim):
    return lax.dot_general(
        left, right, (((left_dim,), (right_dim,)), ((), ())), preferred_element_type=jnp.float32
    )


def rotary_tables(tok, blocks):
    half = ROT // 2
    frequency = rope_base ** (-np.arange(half, dtype=np.float64) * 2.0 / ROT)
    lanes = np.zeros(LANES)
    lanes[:half] = frequency
    lanes[half:ROT] = frequency
    inner = np.arange(tok, dtype=np.float64)[:, None] * lanes
    outer = np.arange(blocks, dtype=np.float64)[:, None] * tok * lanes
    pack = lambda a: np.stack([np.cos(a), np.sin(a)]).astype(np.float32)
    return (jnp.asarray(pack(inner)), jnp.asarray(pack(outer)))


def flip(rank, mask, size):
    out = jnp.int32(0)
    for b in range(size.bit_length() - 1):
        digit = lax.rem(lax.div(rank, jnp.int32(1 << b)), jnp.int32(2))
        out = out + ((1 - digit) if mask >> b & 1 else digit) * (1 << b)
    return out


def low_bit(j, size):
    return j & -j if j else size


def line_mask(j):
    mask = 0
    b = 0
    while j >> b:
        if j >> b & 1:
            mask ^= (2 << b) - 1
        b += 1
    return mask


def arrivals(size):
    return sorted(range(1, size), key=lambda j: (-low_bit(j, size), j))


def slot_of(j, bit, size):
    index = 0
    for jj in range(size):
        for bb in bits_of(size):
            if bb < low_bit(jj, size):
                if (jj, bb) == (j, bit):
                    return index
                index += 1
    raise ValueError


def at(index, size):
    return pl.ds(pl.multiple_of(index * size, size), size)


def remote(src, dst, send, recv, peer):
    return pltpu.make_async_remote_copy(
        src_ref=src, dst_ref=dst, send_sem=send, recv_sem=recv, device_id=peer, device_id_type=MESH
    )


def repeat(count, body):
    def step(i, carry):
        body(i)
        return carry

    lax.fori_loop(0, count, step, 0)


def turn(value, cos_part, sin_part):
    half = ROT // 2
    head = value[:, :LANES]
    lane = lax.broadcasted_iota(jnp.int32, head.shape, 1)
    other = jnp.where(
        lane < half, -pltpu.roll(head, LANES - half, 1), pltpu.roll(head, half, 1)
    )
    return jnp.concatenate([head * cos_part + other * sin_part, value[:, LANES:]], axis=1)


def make_core(S, T, F):
    c = types.SimpleNamespace(S=S, T=T, F=F)
    c.z, c.y, c.f = lax.axis_index("seq"), lax.axis_index("tensor"), lax.axis_index("fsdp")
    c.fbits, c.sbits = bits_of(F), bits_of(S)
    sends, busy = [], {}

    def start(copy, key=None):
        copy.start()
        sends.append(copy)
        if key is not None:
            busy.setdefault(key, []).append(copy)

    def free(key):
        done = busy.pop(key, [])
        for copy in done:
            copy.wait_send()
        sends[:] = [s for s in sends if not any(s is copy for copy in done)]

    def finish():
        for copy in sends:
            copy.wait_send()

    def greet():
        barrier = pltpu.get_barrier_semaphore()
        peers = [dict(seq=flip(c.z, k, S)) for k in range(1, S)]
        peers += [dict(tensor=flip(c.y, t, T)) for t in range(1, T)]
        peers += [dict(fsdp=flip(c.f, b, F)) for b in c.fbits]
        for peer in peers:
            pl.semaphore_signal(barrier, inc=1, device_id=peer, device_id_type=MESH)
        pl.semaphore_wait(barrier, len(peers))

    c.start, c.free, c.finish, c.greet = start, free, finish, greet
    return c


def gather_ops(c, e):
    S, T, F, z, y, f = c.S, c.T, c.F, c.z, c.y, c.f
    tok, width = e.hid_in.shape
    rows = e.wq_in.shape[0]
    half = e.wu.shape[1] // 2
    tokens = ((e.hid_in, e.hid), (e.cot_in, e.cot))
    weights = (
        (e.wq_in, e.wq, 0, e.wq.shape[1]),
        (e.wp_in, e.wp, 0, e.wp.shape[1]),
        (e.wu_in, e.wu, 0, half),
        (e.wu_in, e.wu, half, half),
        (e.wd_in, e.wd, 0, half),
        (e.wd_in, e.wd, half, half),
    )
    g = types.SimpleNamespace()

    def tok_sem(a, j, t):
        return (a * S + j) * T + t

    def tok_place(a, j, t):
        return tokens[a][1].at[at(flip(z, line_mask(j), S), tok), at(flip(y, t, T), width)]

    def tok_seq(a, j):
        src = tokens[a][0] if j == 0 else tok_place(a, j, 0)
        dst = tok_place(a, j, 0)
        for b in reversed(c.sbits):
            if b < low_bit(j, S):
                i = tok_sem(a, j + b, 0)
                peer = dict(seq=flip(z, line_mask(b), S))
                c.start(remote(src, dst, e.tok_send.at[i], e.tok_recv.at[i], peer))

    def tok_tensor(a, j):
        src = tokens[a][0] if j == 0 else tok_place(a, j, 0)
        dst = tok_place(a, j, 0)
        for t in range(1, T):
            i = tok_sem(a, j, t)
            peer = dict(tensor=flip(y, t, T))
            c.start(remote(src, dst, e.tok_send.at[i], e.tok_recv.at[i], peer))

    def tok_wait(a, j, t):
        i = tok_sem(a, j, t)
        spot = tok_place(a, j, t)
        peer = dict(tensor=flip(y, 1, T))
        remote(spot, spot, e.tok_send.at[i], e.tok_recv.at[i], peer).wait_recv()

    def tok_own(a):
        return pltpu.make_async_copy(tokens[a][0], tok_place(a, 0, 0), e.own_sem.at[a])

    def tok_direct(a, j):
        tok_wait(a, j, 0)
        tok_seq(a, j)
        tok_tensor(a, j)

    def tok_passed(a):
        for j in arrivals(S):
            if j not in c.sbits:
                tok_wait(a, j, 0)
                tok_seq(a, j)
                tok_tensor(a, j)

    def tok_rest(a):
        tok_own(a).wait()
        for j in range(S):
            for t in range(1, T):
                tok_wait(a, j, t)

    def row_sem(m, k, j):
        return (m * S + k) * F + j

    def row_place(m, k, j):
        _, dst, first, size = weights[m]
        return dst.at[at(flip(z, k, S) * F + flip(f, j, F), rows), first : first + size]

    def row_source(m, zd):
        src, dst, first, size = weights[m]
        return src.at[:, pl.ds(pl.multiple_of(zd * dst.shape[1] + first, LANES), size)]

    def row_seq(m, *peers):
        for k in peers or range(1, S):
            i = row_sem(m, k, 0)
            zd = flip(z, k, S)
            src = row_source(m, zd)
            dst = row_place(m, 0, 0)
            c.start(remote(src, dst, e.row_send.at[i], e.row_recv.at[i], dict(seq=zd)))

    def row_forward(m, k, j):
        dst = row_place(m, k, j)
        src = row_source(m, z) if k == 0 and j == 0 else dst
        for b in reversed(c.fbits):
            if b < low_bit(j, F):
                i = row_sem(m, k, j + b)
                peer = dict(fsdp=flip(f, b, F))
                c.start(remote(src, dst, e.row_send.at[i], e.row_recv.at[i], peer))

    def row_wait(m, k, j):
        i = row_sem(m, k, j)
        spot = row_place(m, k, j)
        peer = dict(seq=flip(z, 1, S))
        remote(spot, spot, e.row_send.at[i], e.row_recv.at[i], peer).wait_recv()

    def row_own(m):
        return pltpu.make_async_copy(row_source(m, z), row_place(m, 0, 0), e.own_sem.at[2 + m])

    def row_arrive(m, *peers):
        for k in peers or range(1, S):
            row_wait(m, k, 0)
            row_forward(m, k, 0)

    def row_relay(m):
        for j in arrivals(F):
            if low_bit(j, F) > 1:
                for k in range(S):
                    row_wait(m, k, j)
                    row_forward(m, k, j)

    def row_rest(m):
        row_own(m).wait()
        for j in arrivals(F):
            if low_bit(j, F) == 1:
                for k in range(S):
                    row_wait(m, k, j)

    def begin_own():
        for a in range(2):
            tok_own(a).start()
        for m in range(6):
            row_own(m).start()

    g.tok_seq, g.tok_tensor, g.tok_direct, g.tok_passed = tok_seq, tok_tensor, tok_direct, tok_passed
    g.tok_rest, g.row_seq, g.row_forward, g.row_arrive = tok_rest, row_seq, row_forward, row_arrive
    g.row_relay, g.row_rest, g.begin_own = row_relay, row_rest, begin_own
    return g


def attention_ops(c, e):
    S, T, F, z, y, f = c.S, c.T, c.F, c.z, c.y, c.f
    tok = e.hid_in.shape[0]
    ntok = e.hid.shape[0]
    scale = HEAD_DIM ** (-0.5)
    chunk = 32
    o = types.SimpleNamespace()

    def norm():
        def norm_chunk(i):
            part = at(i, chunk)
            x = f32(e.hid[part, :])
            mean = jnp.mean(x, axis=-1, keepdims=True)
            centered = x - mean
            inv_std = lax.rsqrt(jnp.mean(centered * centered, axis=-1, keepdims=True) + norm_eps)
            xhat = centered * inv_std
            e.attn_in[part, :] = bf(xhat * e.attn_gain[...] + e.attn_bias[...])
            e.mlp_in[part, :] = bf(xhat * e.mlp_gain[...] + e.mlp_bias[...])
            e.stat[0, part, :] = jnp.broadcast_to(mean, (chunk, LANES))
            e.stat[1, part, :] = jnp.broadcast_to(inv_std, (chunk, LANES))

        repeat(ntok // chunk, norm_chunk)

    def angles(zd):
        block = pl.ds(zd * F + f, 1)
        cos_in, sin_in = e.inner[0], e.inner[1]
        cos_out, sin_out = e.outer[0, block, :], e.outer[1, block, :]
        return (cos_in * cos_out - sin_in * sin_out, sin_in * cos_out + cos_in * sin_out)

    def qkv():
        bias = e.qkv_bias[:, at(z, 3 * HEAD_DIM)]
        for n in range(3):
            columns = slice(n * HEAD_DIM, (n + 1) * HEAD_DIM)
            part = mm(e.attn_in[...], e.wq[:, columns], 1, 0) + bias[:, columns]
            for zd in range(S):
                piece = part[zd * tok : (zd + 1) * tok]
                if n < 2:
                    piece = turn(piece, *angles(zd))
                if n == 0:
                    e.query[zd * tok : (zd + 1) * tok, :] = bf(piece)
                else:
                    spot = at(zd * F + f, tok)
                    e.pair[spot, (n - 1) * HEAD_DIM : n * HEAD_DIM] = bf(piece)

    def pair_place(zd, j):
        return e.pair.at[at(zd * F + flip(f, j, F), tok), :]

    def pair_forward(zd, j):
        spot = pair_place(zd, j)
        for b in reversed(c.fbits):
            if b < low_bit(j, F):
                i = zd * F + j + b
                peer = dict(fsdp=flip(f, b, F))
                c.start(remote(spot, spot, e.pair_send.at[i], e.pair_recv.at[i], peer), "pair")

    def pair_wait(zd, j):
        i = zd * F + j
        spot = pair_place(zd, j)
        peer = dict(fsdp=flip(f, 1, F))
        remote(spot, spot, e.pair_send.at[i], e.pair_recv.at[i], peer).wait_recv()

    def pair_own():
        for zd in range(S):
            pair_forward(zd, 0)

    def pair_relay():
        for j in arrivals(F):
            if low_bit(j, F) > 1:
                for zd in range(S):
                    pair_wait(zd, j)
                    pair_forward(zd, j)

    def pair_rest():
        for j in arrivals(F):
            if low_bit(j, F) == 1:
                for zd in range(S):
                    pair_wait(zd, j)

    n = F * tok

    def row_chunks(b, body):
        count = ntok - b * tok
        size = count // 2 if count > 2 * tok else count
        while size * n > 2 * tok * 512 and size > 32:
            size //= 2

        def step(i):
            first = pl.multiple_of(b * tok + i * size, 32)
            here = pl.ds(first, size)
            scores = mm(e.query[here, :], e.pair[b * n : (b + 1) * n, :HEAD_DIM], 1, 1) * scale
            row = i * size + lax.broadcasted_iota(jnp.int32, scores.shape, 0)
            column = lax.broadcasted_iota(jnp.int32, scores.shape, 1)
            body(here, scores, (column - row <= f * tok) | (row >= tok))

        repeat(count // size, step)

    def wide_rows(value):
        return jnp.broadcast_to(value, (value.shape[0], LANES))

    def forward():
        for b in range(S):
            values = e.pair.at[b * n : (b + 1) * n, HEAD_DIM:]

            def block(here, scores, allowed, b=b, values=values):
                top = jnp.max(jnp.where(allowed, scores, -1e30), axis=-1, keepdims=True)
                if b:
                    old = e.row_info[here, :1]
                    top = jnp.maximum(top, old)
                terms = jnp.where(allowed, jnp.exp(scores - top), 0.0)
                total = jnp.sum(terms, axis=-1, keepdims=True)
                mixed = mm(bf(terms), values[...], 1, 0)
                if b:
                    rescale = jnp.exp(old - top)
                    total = total + e.row_sum[here, :1] * rescale
                    mixed = mixed + e.acc[here, :] * rescale
                e.row_info[here, :] = wide_rows(top)
                e.row_sum[here, :] = wide_rows(total)
                e.acc[here, :] = mixed

            row_chunks(b, block)
            done = slice(b * tok, (b + 1) * tok)
            total = e.row_sum[done, :]
            e.attn[done, :] = bf(e.acc[done, :] / total[:, :1])
            e.row_info[done, :] = e.row_info[done, :] + jnp.log(total)

    def backward():
        e.attn_grad[...] = bf(mm(e.cot[...], e.wp[...], 1, 0))
        delta = jnp.sum(f32(e.attn_grad[...]) * f32(e.attn[...]), axis=-1, keepdims=True)
        e.row_sum[...] = wide_rows(delta)
        for b in range(S):
            keys_here = slice(b * n, (b + 1) * n)

            def block(here, scores, allowed, b=b, keys_here=keys_here):
                weights_here = jnp.where(allowed, jnp.exp(scores - e.row_info[here, :1]), 0.0)
                slopes = mm(e.attn_grad[here, :], e.pair[keys_here, HEAD_DIM:], 1, 1)
                inner_grad = bf(weights_here * (slopes - e.row_sum[here, :1]))
                e.probs[here, keys_here] = bf(weights_here)
                e.score_grad[here, keys_here] = inner_grad
                term = mm(inner_grad, e.pair[keys_here, :HEAD_DIM], 1, 0)
                e.acc[here, :] = e.acc[here, :] + term if b else term

            row_chunks(b, block)
            if b:
                blank = jnp.zeros((b * tok, n), jnp.bfloat16)
                e.probs[: b * tok, keys_here] = blank
                e.score_grad[: b * tok, keys_here] = blank
            done = slice(b * tok, (b + 1) * tok)
            cos_part, sin_part = angles(b)
            e.tg[done, :HEAD_DIM] = bf(turn(e.acc[done, :] * scale, cos_part, -sin_part))

    def part_sum(j):
        def lanes(ref):
            return jnp.concatenate(
                [ref[:, at(zd * F + flip(f, j, F), tok)] for zd in range(S)], axis=1
            )

        total = jnp.concatenate(
            [
                mm(lanes(e.score_grad), e.query[...], 0, 0) * scale,
                mm(lanes(e.probs), e.attn_grad[...], 0, 0),
            ],
            axis=1,
        )
        for b in c.fbits:
            if b < low_bit(j, F):
                i = slot_of(j, b, F)
                spot = e.part_in.at[i]
                peer = dict(fsdp=flip(f, b, F))
                remote(spot, spot, e.part_send.at[i], e.part_recv.at[i], peer).wait_recv()
                total = total + f32(e.part_in[i])
        return total

    def part_stage(bit):
        c.free("pair")
        for j in range(1, F):
            if low_bit(j, F) == bit:
                spot = e.pair.at[(j - 1) * ntok : j * ntok, :]
                e.pair[(j - 1) * ntok : j * ntok, :] = bf(part_sum(j))
                i = slot_of(j - bit, bit, F)
                peer = dict(fsdp=flip(f, bit, F))
                here = e.part_in.at[i]
                c.start(remote(spot, here, e.part_send.at[j - 1], e.part_recv.at[i], peer))

    def part_later():
        for bit in c.fbits[1:]:
            part_stage(bit)

    def part_home():
        total = part_sum(0)
        for zd in range(S):
            here = slice(zd * tok, (zd + 1) * tok)
            cos_part, sin_part = angles(zd)
            key_part = turn(total[here, :HEAD_DIM], cos_part, -sin_part)
            e.tg[here, HEAD_DIM : 2 * HEAD_DIM] = bf(key_part)
            e.tg[here, 2 * HEAD_DIM :] = bf(total[here, HEAD_DIM:])

    def up(first, size):
        cols = e.wu.shape[1]
        for n in range(first // STRIP, (first + size) // STRIP):
            strip = slice(n * STRIP, (n + 1) * STRIP)
            bias = e.up_bias[:, pl.ds(pl.multiple_of(z * cols + n * STRIP, STRIP), STRIP)]
            mid = mm(e.mlp_in[...], e.wu[:, strip], 1, 0) + bias
            cdf = 0.5 * (1.0 + lax.erf(mid * 0.7071067811865476))
            e.active[:, strip] = bf(mid * cdf)
            e.slope[:, strip] = cdf + mid * jnp.exp(-0.5 * mid * mid) * 0.3989422804014327

    o.norm, o.qkv, o.pair_own, o.pair_relay, o.pair_rest = norm, qkv, pair_own, pair_relay, pair_rest
    o.forward, o.backward, o.part_stage, o.part_later = forward, backward, part_stage, part_later
    o.part_home, o.up = part_home, up
    return o


def grad_units(ff):
    half = ff // 2
    return (
        (0, 0, HEAD_DIM),
        (1, 0, half),
        (1, half, half),
        (2, 0, 3 * HEAD_DIM),
        (3, 0, half),
        (3, half, half),
    )


def spread_ops(c, e, turned):
    S, T, F, z, y, f = c.S, c.T, c.F, c.z, c.y, c.f
    tok, width = e.homes[0].shape
    ntok, D = e.wide.shape
    ff = e.active.shape[1]
    rows = e.grads[0].shape[0]
    rights, lefts = (e.attn, e.active, e.tg, e.pre), (e.cot, e.cot, e.attn_in, e.mlp_in)
    units = grad_units(ff)
    n_u = len(units)
    p = types.SimpleNamespace()

    def block_sum(u, j):
        g, first, size = units[u]
        right, left = rights[g].at[:, first : first + size], lefts[g]
        fd = flip(f, j, F)
        if turned:
            block = jnp.concatenate([left[at(zd * F + fd, rows), :] for zd in range(S)], axis=0)
            total = mm(block, right[...], 1, 0)
        else:
            block = jnp.concatenate([left[:, at(zd * F + fd, rows)] for zd in range(S)], axis=1)
            total = mm(block, right[...], 0, 0)
        for bit in c.fbits:
            if bit < low_bit(j, F):
                s = slot_of(j, bit, F)
                i = u * (F - 1) + s
                spot = e.in_b[u].at[s]
                peer = dict(fsdp=flip(f, bit, F))
                remote(spot, spot, e.out_sem.at[i], e.in_sem.at[i], peer).wait_recv()
                total = total + f32(e.in_b[u][s])
        return total

    def fsdp_stage(u, bit):
        for j in range(1, F):
            if low_bit(j, F) == bit:
                key, spot = e.out_spot(u, j)
                c.free(key)
                spot[...] = bf(block_sum(u, j))
                there = slot_of(j - bit, bit, F)
                send = e.out_sem.at[u * (F - 1) + j - 1]
                recv = e.in_sem.at[u * (F - 1) + there]
                peer = dict(fsdp=flip(f, bit, F))
                c.start(remote(spot, e.in_b[u].at[there], send, recv, peer), key)

    def first(u):
        fsdp_stage(u, c.fbits[0])

    def later(u):
        for bit in c.fbits[1:]:
            fsdp_stage(u, bit)

    def grad_place(u, zd):
        g, first_col, size = units[u]
        start_col = zd * rights[g].shape[1] + first_col
        return e.grads[g].at[:, pl.ds(pl.multiple_of(start_col, LANES), size)]

    def own_grad(u):
        src = e.seq_b[u].at[at(z, rows), :]
        return pltpu.make_async_copy(src, grad_place(u, z), e.home_sem.at[u])

    def seq(u):
        e.seq_b[u][...] = bf(block_sum(u, 0))
        own_grad(u).start()

    def seq_send(u, *peers):
        for k in peers or range(1, S):
            peer = flip(z, k, S)
            src, dst = e.seq_b[u].at[at(peer, rows), :], grad_place(u, z)
            i = u * S + k
            c.start(remote(src, dst, e.seq_send.at[i], e.seq_recv.at[i], dict(seq=peer)))

    def seq_wait():
        for u in range(n_u):
            for k in range(1, S):
                peer = flip(z, k, S)
                spot = grad_place(u, peer)
                i = u * S + k
                remote(spot, spot, e.seq_send.at[i], e.seq_recv.at[i], dict(seq=peer)).wait_recv()
            own_grad(u).wait()

    def half_strips(s, t, term):
        for n in range(width // STRIP):
            there = pl.ds(pl.multiple_of(flip(y, t, T) * width + n * STRIP, STRIP), STRIP)
            here = slice(n * STRIP, (n + 1) * STRIP)
            value = term(there)
            if t:
                for zd in range(S):
                    e.y_out[(t - 1) * S + zd, :, here] = bf(value[zd * tok : (zd + 1) * tok])
            elif s == 0:
                e.own_half[:, here] = value
            else:
                e.wide[:, there] = value

    def y_index(s, t, j):
        return (s * max(T - 1, 1) + t - 1) * S + j

    def tensor_send(s):
        for j in [*sorted(range(1, S), key=lambda j: (low_bit(j, S), j)), 0]:
            zd = flip(z, line_mask(j), S)
            for t in range(1, T):
                i = y_index(s, t, j)
                peer = dict(tensor=flip(y, t, T))
                here = e.y_out.at[(t - 1) * S + zd]
                c.start(remote(here, e.y_in.at[i], e.y_send.at[i], e.y_recv.at[i], peer), "y")

    def token_own(s, zd):
        if s == 0:
            return e.own_half.at[at(zd, tok), :]
        return e.wide.at[at(zd, tok), at(y, width)]

    def token_part(s, j):
        total = token_own(s, flip(z, line_mask(j), S))[...]
        for t in range(1, T):
            i = y_index(s, t, j)
            spot = e.y_in.at[i]
            peer = dict(tensor=flip(y, t, T))
            remote(spot, spot, e.y_send.at[i], e.y_recv.at[i], peer).wait_recv()
            total = total + f32(e.y_in[i])
        for bit in c.sbits:
            if bit < low_bit(j, S):
                i = s * (S - 1) + slot_of(j, bit, S)
                spot = e.z_in.at[i]
                peer = dict(seq=flip(z, line_mask(bit), S))
                remote(spot, spot, e.z_send.at[i], e.z_recv.at[i], peer).wait_recv()
                total = total + f32(e.z_in[i])
        return total

    def token_send(s, j):
        bit = low_bit(j, S)
        i = s * (S - 1) + j - 1
        there = s * (S - 1) + slot_of(j - bit, bit, S)
        c.free(("z", j))
        e.z_out[j - 1] = bf(token_part(s, j))
        peer = dict(seq=flip(z, line_mask(bit), S))
        here = e.z_out.at[j - 1]
        copy = remote(here, e.z_in.at[there], e.z_send.at[i], e.z_recv.at[there], peer)
        c.start(copy, ("z", j))

    def token_sends(s):
        for j in sorted(range(1, S), key=lambda j: (low_bit(j, S), j)):
            token_send(s, j)

    def home_copy(s):
        return pltpu.make_async_copy(token_own(s, z), e.homes[s], e.home_sem.at[n_u + s])

    def token_home(s):
        total = token_part(s, 0)
        token_own(s, z)[...] = total
        home_copy(s).start()

    def home_wait():
        for s in range(2):
            home_copy(s).wait()

    n_f = len(c.fbits)
    vec = e.vec

    def vec_copy(b):
        peer = dict(fsdp=flip(f, c.fbits[b], F))
        return remote(vec.at[b], e.vec_in.at[b], e.v_send.at[b], e.v_recv.at[b], peer)

    def vec_start(b):
        c.start(vec_copy(b))

    def vec_sum(b):
        vec_copy(b).wait_recv()
        vec[b + 1] = vec[b] + e.vec_in[b]

    def vec_fsdp():
        for b in range(n_f - 1):
            vec_sum(b)
            vec_start(b + 1)

    def vec_seq_copy(k):
        peer = dict(seq=flip(z, k, S))
        i = n_f + k - 1
        return remote(vec.at[n_f], e.vec_seq.at[k - 1], e.v_send.at[i], e.v_recv.at[i], peer)

    def vec_seq_start():
        vec_sum(n_f - 1)
        for k in range(1, S):
            c.start(vec_seq_copy(k))

    def tree(parts):
        while len(parts) > 1:
            parts = [a + b for a, b in zip(parts[::2], parts[1::2])]
        return parts[0]

    def vec_seq_sum():
        parts = []
        for k in range(S):
            if k:
                vec_seq_copy(k).wait_recv()
            value = vec[n_f] if k == 0 else e.vec_seq[k - 1]
            zd = flip(z, k, S)
            e.qkv_bias_o[:, at(zd, 3 * HEAD_DIM)] = value[4:5, : 3 * HEAD_DIM]
            e.up_bias_o[:, at(zd, ff)] = value[5:6, :ff]
            parts.append(value)
        total = tree(parts)
        e.out_bias_o[...] = total[6:7, :width]
        e.vec_ten[0] = total[:4]
        for t in range(1, T):
            c.start(vec_ten_copy(t))

    def vec_ten_copy(t):
        peer = dict(tensor=flip(y, t, T))
        i = n_f + S - 1 + t - 1
        return remote(e.vec_ten.at[0], e.vec_ten.at[t], e.v_send.at[i], e.v_recv.at[i], peer)

    def vec_ten_sum():
        parts = [e.vec_ten[0]]
        for t in range(1, T):
            vec_ten_copy(t).wait_recv()
            parts.append(e.vec_ten[t])
        e.gain_o[...] = tree(parts)

    def branch():
        def term(column):
            return mm(e.active[...], e.wd[column, :], 1, 1) + mm(e.attn[...], e.wp[column, :], 1, 1)

        for t in range(1, T):
            half_strips(0, t, term)
        tensor_send(0)
        return lambda: half_strips(0, 0, term)

    def hidden_grad():
        vec[0] = jnp.zeros(vec.shape[1:], jnp.float32)
        for n in range(ff // STRIP):
            here = slice(n * STRIP, (n + 1) * STRIP)
            value = mm(e.cot[...], e.wd[:, here], 0 if turned else 1, 0) * e.slope[:, here]
            vec[0, 5:6, here] = jnp.sum(value, axis=0, keepdims=True)
            e.pre[:, here] = bf(value)

    def unit_rows(column):
        mean, inv_std = e.stat[0, :, :1], e.stat[1, :, :1]
        return ((f32(e.hid[:, column]) - mean) * inv_std, inv_std)

    def add_strip(here, value, gain, row):
        xhat, _ = unit_rows(here)
        scaled = value * xhat
        vec[0, row : row + 1, here] = jnp.sum(scaled, axis=0, keepdims=True)
        vec[0, row + 1 : row + 2, here] = jnp.sum(value, axis=0, keepdims=True)
        gain_here = gain[:, here]
        both, scaled = value * gain_here, scaled * gain_here
        lane_parts = range(0, STRIP, LANES)
        e.sums[0] += sum(both[:, i : i + LANES] for i in lane_parts)
        e.sums[1] += sum(scaled[:, i : i + LANES] for i in lane_parts)
        return both

    def mlp_strips():
        def strip(n):
            here = at(n, STRIP)
            e.wide[:, here] = add_strip(here, mm(e.pre[...], e.wu[here, :], 1, 1), e.mlp_gain, 2)

        e.sums[...] = jnp.zeros_like(e.sums)
        repeat(D // STRIP, strip)

    def norm_strips():
        def strip(n):
            here = at(n, STRIP)
            e.wide[:, here] += add_strip(here, mm(e.tg[...], e.wq[here, :], 1, 1), e.attn_gain, 0)

        repeat(D // STRIP, strip)
        for i in range(2):
            mean = jnp.sum(e.sums[i], axis=-1, keepdims=True) / D
            e.sums[i] = jnp.broadcast_to(mean, e.sums.shape[1:])

    def vec_begin():
        vec[0, 4:5, : 3 * HEAD_DIM] = jnp.sum(f32(e.tg[...]), axis=0, keepdims=True)
        vec[0, 6:7, :width] = jnp.sum(f32(e.own_cot()), axis=0, keepdims=True)
        vec_start(0)

    def input_strips():
        def term(column):
            xhat, inv_std = unit_rows(column)
            return inv_std * (e.wide[:, column] - e.sums[0, :, :1] - xhat * e.sums[1, :, :1])

        c.free("y")
        for t in range(1, T):
            half_strips(1, t, term)
        tensor_send(1)
        return lambda: half_strips(1, 0, term)

    p.first, p.later, p.seq, p.seq_send, p.seq_wait = first, later, seq, seq_send, seq_wait
    p.token_send, p.token_sends, p.token_home = token_send, token_sends, token_home
    p.home_wait, p.vec_fsdp = home_wait, vec_fsdp
    p.vec_seq_start, p.vec_seq_sum, p.vec_ten_sum = vec_seq_start, vec_seq_sum, vec_ten_sum
    p.branch, p.hidden_grad, p.mlp_strips = branch, hidden_grad, mlp_strips
    p.norm_strips, p.input_strips, p.vec_begin = norm_strips, input_strips, vec_begin
    return p


def gather_buffers(S, T, F, tok, width, rows, ff):
    ntok, D, keys = S * tok, T * width, S * F * tok
    kept = dict(
        hid=((ntok, D), SMALL),
        cot=((ntok, D), SMALL),
        attn_in=((ntok, D), SMALL),
        mlp_in=((ntok, D), SMALL),
        stat=((2, ntok, LANES), WIDE),
        wq=((D, 3 * HEAD_DIM), SMALL),
        wp=((D, HEAD_DIM), SMALL),
        wu=((D, ff), SMALL),
        wd=((D, ff), SMALL),
        attn=((ntok, HEAD_DIM), SMALL),
        active=((ntok, ff), SMALL),
        tg=((ntok, 3 * HEAD_DIM), SMALL),
    )
    passing = dict(
        query=((ntok, HEAD_DIM), SMALL),
        pair=((keys, 2 * HEAD_DIM), SMALL),
        attn_grad=((ntok, HEAD_DIM), SMALL),
        probs=((ntok, keys), SMALL),
        score_grad=((ntok, keys), SMALL),
        row_info=((ntok, LANES), WIDE),
        row_sum=((ntok, LANES), WIDE),
        acc=((ntok, HEAD_DIM), WIDE),
        part_in=((max(F - 1, 1), ntok, 2 * HEAD_DIM), SMALL),
    )
    sems = dict(
        own_sem=8,
        tok_send=2 * S * T,
        tok_recv=2 * S * T,
        row_send=6 * S * F,
        row_recv=6 * S * F,
        pair_send=S * F,
        pair_recv=S * F,
        part_send=max(F - 1, 1),
        part_recv=max(F - 1, 1),
    )
    return kept, passing, sems


def spread_buffers(S, T, F, tok, width, rows, ff):
    ntok, D = S * tok, T * width
    n_f, n_y, parts = len(bits_of(F)), max(T - 1, 1) * S, max(F - 1, 1)
    held = dict(
        pre=((ntok, ff), SMALL),
        wide=((ntok, D), WIDE),
        own_half=((ntok, width), WIDE),
        sums=((2, ntok, LANES), WIDE),
        vec=((n_f + 1, 8, D), WIDE),
        vec_in=((n_f, 8, D), WIDE),
        vec_seq=((max(S - 1, 1), 8, D), WIDE),
        vec_ten=((T, 4, D), WIDE),
        y_out=((n_y, tok, width), SMALL),
        y_in=((2 * n_y, tok, width), SMALL),
        z_out=((max(S - 1, 1), tok, width), SMALL),
        z_in=((2 * max(S - 1, 1), tok, width), SMALL),
    )
    for u, (_, _, size) in enumerate(grad_units(ff)):
        held[f"in_b{u}"] = ((parts, S * rows, size), SMALL)
        held[f"seq_b{u}"] = ((S * rows, size), SMALL)
    sems = dict(
        home_sem=8,
        out_sem=6 * parts,
        in_sem=6 * parts,
        seq_send=6 * S,
        seq_recv=6 * S,
        y_send=2 * n_y,
        y_recv=2 * n_y,
        z_send=2 * max(S - 1, 1),
        z_recv=2 * max(S - 1, 1),
        v_send=n_f + S + T,
        v_recv=n_f + S + T,
    )
    outs = {f"grad{g}": ((rows, S * n), SMALL) for g, n in enumerate((HEAD_DIM, ff, 3 * HEAD_DIM, ff))}
    outs |= {f"home{s}": ((tok, width), WIDE) for s in range(2)}
    vectors = dict(
        gain_o=((4, D), WIDE),
        qkv_bias_o=((1, 3 * width), WIDE),
        up_bias_o=((1, S * ff), WIDE),
        out_bias_o=((1, width), WIDE),
    )
    return held, sems, outs, vectors


def send_buffers(S, F, rows, ff, units):
    sizes = [size for _, _, size in grad_units(ff)]
    return {f"out_b{u}": ((max(F - 1, 1), S * rows, sizes[u]), SMALL) for u in units}


def gather_lists(e):
    e.in_b = [getattr(e, f"in_b{u}") for u in range(6)]
    e.seq_b = [getattr(e, f"seq_b{u}") for u in range(6)]
    e.grads = [getattr(e, f"grad{g}") for g in range(4)]
    e.homes = [e.home0, e.home1]


def launch(body, sizes, collective, far, near, outs, near_outs, scratch, sems, **lists):
    names = [*far, *near, *outs, *near_outs, *scratch, *sems]

    def kernel(*refs):
        body(types.SimpleNamespace(**dict(zip(names, refs)), **lists), *sizes)

    kernel.__name__ = body.__name__
    any_spec = pl.BlockSpec(memory_space=pl.ANY)
    vmem = pl.BlockSpec(memory_space=pltpu.VMEM)
    results = pl.pallas_call(
        kernel,
        out_shape=[jax.ShapeDtypeStruct(*o) for o in [*outs.values(), *near_outs.values()]],
        in_specs=[any_spec] * len(far) + [vmem] * len(near),
        out_specs=[any_spec] * len(outs) + [vmem] * len(near_outs),
        scratch_shapes=[pltpu.VMEM(*s) for s in scratch.values()]
        + [pltpu.SemaphoreType.DMA((n,)) for n in sems.values()],
        compiler_params=pltpu.CompilerParams(
            collective_id=collective, has_side_effects=True, vmem_limit_bytes=VMEM_BYTES
        ),
    )(*far.values(), *near.values())
    return dict(zip([*outs, *near_outs], results))


def whole_kernel(e, S, T, F):
    c = make_core(S, T, F)
    width = e.hid_in.shape[1]
    tok = e.hid_in.shape[0]
    ff = e.active.shape[1]
    half = ff // 2
    gather_lists(e)
    e.slope = e.wide.at[:, :ff]
    e.row_info, e.row_sum = e.sums.at[0], e.sums.at[1]
    e.acc = e.wide.at[:, ff : ff + HEAD_DIM]
    e.own_cot = lambda: e.cot[at(c.z, tok), at(c.y, width)]
    wide_q = 3 * HEAD_DIM
    lent = [e.probs.at[:, :wide_q], e.probs.at[:, wide_q : 2 * wide_q], e.score_grad.at[:, :wide_q]]

    def out_spot(u, j):
        if u == Q1:
            return (("out", u, j), lent[j - 1])
        shared = {U1: D1, U2: D2}.get(u, u)
        return (("out", shared, j), getattr(e, f"out_b{shared}").at[j - 1])

    e.out_spot = out_spot
    g, o, p = gather_ops(c, e), attention_ops(c, e), spread_ops(c, e, False)
    near, vectors = e.near_names, e.vector_names

    def near_copy(i):
        return pltpu.make_async_copy(getattr(e, near[i] + "_i"), getattr(e, near[i]), e.near_sem.at[i])

    def vec_copy(i):
        return pltpu.make_async_copy(getattr(e, vectors[i]), getattr(e, vectors[i] + "_h"), e.vec_sem.at[i])

    def begin():
        g.begin_own()
        for i in range(len(near)):
            near_copy(i).start()

    def norm():
        for i in range(len(near)):
            near_copy(i).wait()
        o.norm()

    def vec_home():
        p.vec_ten_sum()
        for i in range(len(vectors)):
            vec_copy(i).start()

    c.greet()
    g.row_seq(WU2, 1)
    g.row_forward(WU1, 0, 0)
    g.tok_tensor(1, 0)
    g.row_seq(WQ, 2)
    g.tok_seq(0, 0)
    begin()
    g.tok_tensor(0, 0)
    g.row_forward(WQ, 0, 0)
    g.row_seq(WQ, 1)
    g.row_seq(WQ, 3)
    g.row_seq(WD2, 1)
    g.row_forward(WD1, 0, 0)
    g.row_seq(WP, 3)
    g.row_arrive(WQ, 1)
    g.row_seq(WU2, 2)
    g.row_arrive(WQ, 2)
    g.row_arrive(WD2, 1)
    g.tok_direct(0, 2)
    g.row_forward(WP, 0, 0)
    g.row_arrive(WQ, 3)
    g.row_forward(WU2, 0, 0)
    g.row_seq(WU2, 3)
    g.row_arrive(WU2, 2)
    g.tok_direct(0, 1)
    g.row_seq(WP, 2)
    g.row_relay(WQ)
    g.row_seq(WU1, 1)
    g.row_seq(WU1, 3)
    g.row_seq(WP, 1)
    g.tok_passed(0)
    g.row_arrive(WP, 2)
    g.row_arrive(WU2, 3)
    g.row_rest(WQ)
    g.row_arrive(WU2, 1)
    g.row_forward(WD2, 0, 0)
    g.tok_seq(1, 0)
    g.row_arrive(WU1, 1)
    g.tok_rest(0)
    norm()
    g.row_seq(WU1, 2)
    o.qkv()
    o.pair_own()
    g.row_arrive(WP, 3)
    g.tok_direct(1, 1)
    g.row_relay(WU2)
    g.tok_direct(1, 2)
    g.row_rest(WU2)
    g.row_seq(WD2, 2)
    o.pair_relay()
    g.row_seq(WD1, 3)
    g.row_arrive(WU1, 3)
    g.row_arrive(WU1, 2)
    o.up(half, half)
    g.row_seq(WD1, 1)
    o.pair_rest()
    o.forward()
    g.row_arrive(WP, 1)
    g.row_arrive(WD2, 2)
    g.row_seq(WD1, 2)
    g.row_relay(WU1)
    g.tok_passed(1)
    g.row_arrive(WD1, 3)
    g.row_rest(WU1)
    g.row_arrive(WD1, 1)
    o.up(0, half)
    g.row_relay(WP)
    g.row_seq(WD2, 3)
    g.tok_rest(1)
    p.first(D1)
    g.row_arrive(WD1, 2)
    g.row_rest(WP)
    p.first(D2)
    g.row_arrive(WD2, 3)
    p.later(D1)
    g.row_relay(WD1)
    g.row_rest(WD1)
    g.row_relay(WD2)
    g.row_rest(WD2)
    p.later(D2)
    own_strips = p.branch()
    o.backward()
    p.seq(D1)
    p.seq_send(D1, 2)
    o.part_stage(c.fbits[0])
    p.seq_send(D1, 3)
    p.seq_send(D1, 1)
    p.first(P1)
    p.hidden_grad()
    p.mlp_strips()
    p.later(P1)
    own_strips()
    p.token_send(0, 3)
    o.part_later()
    p.seq(D2)
    p.seq_send(D2, 3)
    p.first(U1)
    p.seq(P1)
    p.seq_send(D2, 2)
    p.seq_send(D2, 1)
    p.first(U2)
    p.later(U2)
    p.seq_send(P1, 2)
    p.token_send(0, 2)
    p.token_send(0, 1)
    o.part_home()
    p.norm_strips()
    p.vec_begin()
    own_terms = p.input_strips()
    p.vec_fsdp()
    p.seq_send(P1, 3)
    p.seq(U2)
    p.seq_send(U2, 2)
    p.vec_seq_start()
    p.later(U1)
    p.seq_send(U2, 1)
    own_terms()
    p.first(Q1)
    p.token_send(1, 3)
    p.seq_send(U2, 3)
    p.vec_seq_sum()
    p.token_home(0)
    p.later(Q1)
    p.seq(U1)
    p.seq_send(U1, 3)
    p.token_send(1, 2)
    p.token_send(1, 1)
    p.seq(Q1)
    vec_home()
    p.seq_send(Q1, 2)
    p.seq_send(U1, 1)
    p.token_home(1)
    p.seq_send(Q1, 1)
    p.seq_send(P1, 1)
    p.seq_send(Q1, 3)
    p.seq_send(U1, 2)
    p.seq_wait()
    p.home_wait()
    for i in range(len(vectors)):
        vec_copy(i).wait()
    c.finish()


def first_kernel(e, S, T, F):
    c = make_core(S, T, F)
    half = e.active.shape[1] // 2
    g, o = gather_ops(c, e), attention_ops(c, e)
    names = e.kept_names

    def out_copy(name):
        i = names.index(name)
        return pltpu.make_async_copy(getattr(e, name), getattr(e, name + "_o"), e.put_sem.at[i])

    c.greet()
    g.tok_seq(0, 0)
    g.tok_tensor(0, 0)
    for m in range(6):
        g.row_forward(m, 0, 0)
    g.begin_own()
    for j in c.sbits:
        g.tok_direct(0, j)
    g.row_seq(WQ)
    g.tok_passed(0)
    g.row_seq(WU1)
    g.tok_tensor(1, 0)
    g.tok_rest(0)
    o.norm()
    g.row_arrive(WQ)
    g.tok_seq(1, 0)
    g.row_relay(WQ)
    g.row_rest(WQ)
    o.qkv()
    o.pair_own()
    g.row_arrive(WU1)
    for m in (WP, WU2, WD1, WD2):
        g.row_seq(m)
    for j in c.sbits:
        g.tok_direct(1, j)
    g.row_relay(WU1)
    o.pair_relay()
    g.tok_passed(1)
    g.row_rest(WU1)
    o.up(0, half)
    g.row_arrive(WP)
    o.pair_rest()
    o.forward()
    g.row_arrive(WU2)
    g.tok_rest(1)
    g.row_relay(WP)
    g.row_rest(WP)
    o.backward()
    o.part_stage(c.fbits[0])
    g.row_relay(WU2)
    g.row_rest(WU2)
    o.up(half, half)
    o.part_later()
    g.row_arrive(WD1)
    g.row_arrive(WD2)
    o.part_home()
    for m in (WD1, WD2):
        g.row_relay(m)
        g.row_rest(m)
    for name in names:
        out_copy(name).start()
    for name in names:
        out_copy(name).wait()
    c.finish()


def second_kernel(e, S, T, F, turned):
    c = make_core(S, T, F)
    gather_lists(e)
    ff = e.active.shape[1]
    e.slope = e.wide.at[:, :ff]
    e.own_cot = lambda: e.own_cot_in[...]
    e.out_spot = lambda u, j: (("out", u, j), getattr(e, f"out_b{u}").at[j - 1])
    e.wd = e.wu = e.wud
    p = spread_ops(c, e, turned)
    names = e.kept_names

    def load(name):
        i = names.index(name)
        return pltpu.make_async_copy(getattr(e, name + "_i"), getattr(e, name), e.load_sem.at[i])

    for name in names:
        if name != "wu":
            load(name).start()
    c.greet()
    for name in names:
        if name != "wu":
            load(name).wait()
    p.first(P1)
    p.first(D1)
    p.first(D2)
    own_strips = p.branch()
    p.later(P1)
    own_strips()
    p.later(D1)
    p.hidden_grad()
    load("wu").start()
    p.seq(P1)
    p.seq_send(P1)
    p.later(D2)
    p.token_sends(0)
    p.first(Q1)
    p.first(U1)
    p.first(U2)
    load("wu").wait()
    p.mlp_strips()
    p.norm_strips()
    p.vec_begin()
    p.seq(D1)
    p.seq_send(D1)
    p.later(Q1)
    own_terms = p.input_strips()
    own_terms()
    p.token_home(0)
    p.seq(D2)
    p.seq_send(D2)
    p.later(U1)
    p.vec_fsdp()
    p.seq(Q1)
    p.seq_send(Q1)
    p.later(U2)
    p.vec_seq_start()
    p.token_sends(1)
    p.seq(U1)
    p.seq_send(U1)
    p.seq(U2)
    p.seq_send(U2)
    p.vec_seq_sum()
    p.vec_ten_sum()
    p.token_home(1)
    p.seq_wait()
    p.home_wait()
    c.finish()


def per_device(
    hidden_in,
    out_cotangent,
    attn_norm_gain,
    attn_norm_bias,
    mlp_norm_gain,
    mlp_norm_bias,
    qkv_weight,
    qkv_bias,
    proj_weight,
    proj_bias,
    up_weight,
    up_bias,
    down_weight,
    down_bias,
):
    S, T, F = [lax.axis_size(a) for a in ("seq", "tensor", "fsdp")]
    tok, width = hidden_in.shape
    rows, ff = qkv_weight.shape[0], up_weight.shape[1] // S
    if width != S * HEAD_DIM or S * F * rows != T * width:
        raise ValueError
    shape = (S, T, F, tok, width, rows, ff)
    inner, outer = rotary_tables(tok, S * F)
    far = dict(
        hid_in=hidden_in,
        cot_in=out_cotangent,
        wq_in=qkv_weight,
        wp_in=proj_weight,
        wu_in=up_weight,
        wd_in=down_weight,
    )
    row = lambda v: v.reshape(1, -1)
    gains = dict(attn_gain=row(attn_norm_gain), mlp_gain=row(mlp_norm_gain))
    near = gains | dict(
        attn_bias=row(attn_norm_bias),
        mlp_bias=row(mlp_norm_bias),
        qkv_bias=row(qkv_bias),
        up_bias=row(up_bias),
        inner=inner,
        outer=outer,
    )
    kept, passing, gather_sems = gather_buffers(*shape)
    held, spread_sems, outs, vectors = spread_buffers(*shape)
    if rows % LANES == 0 and (S, T, F) == (4, 2, 4):
        scratch = kept | passing | held | send_buffers(S, F, rows, ff, (P1, D1, D2)) | vectors
        scratch |= {k: (v.shape, v.dtype) for k, v in near.items()}
        del scratch["row_info"], scratch["row_sum"], scratch["acc"]
        sems = gather_sems | spread_sems | dict(near_sem=len(near), vec_sem=len(vectors))
        far |= {k + "_i": v for k, v in near.items()}
        outs |= {k + "_h": v for k, v in vectors.items()}
        lists = dict(near_names=list(near), vector_names=list(vectors))
        res = launch(whole_kernel, (S, T, F), 0, far, {}, outs, {}, scratch, sems, **lists)
        res |= {k: res[k + "_h"] for k in vectors}
    else:
        slope = dict(slope=((S * tok, ff), WIDE))
        saved = {k + "_o": v for k, v in (kept | slope).items()}
        sems = gather_sems | dict(put_sem=len(saved))
        scratch = kept | slope | passing
        lists = dict(kept_names=[*kept, *slope])
        mid = launch(first_kernel, (S, T, F), 0, far, near, saved, {}, scratch, sems, **lists)
        turned = rows % LANES != 0
        if turned:
            for k in ("cot_o", "attn_in_o", "mlp_in_o"):
                mid[k] = mid[k].T
        ins = {k[:-2] + "_i": v for k, v in mid.items()}
        scratch = {k: (ins[k + "_i"].shape, t) for k, (_, t) in kept.items() if k not in ("wu", "wd")}
        scratch |= dict(wud=kept["wu"]) | held | send_buffers(S, F, rows, ff, range(6))
        near = gains | dict(own_cot_in=out_cotangent)
        sems = spread_sems | dict(load_sem=len(ins))
        res = launch(
            second_kernel, (S, T, F, turned), 1, ins, near, outs, vectors, scratch, sems, **lists
        )
    return finish(res, hidden_in, out_cotangent, row(proj_bias), row(down_bias))


def last_kernel(*refs):
    sources, (gain, qkv_b, up_b, out_b, proj_bias, down_bias), refs = refs[:8], refs[8:14], refs[14:]
    outs, refs = refs[:14], refs[14:]
    held, wide, (hidden, norm, load_sem, out_sem) = refs[:8], refs[8:12], refs[12:]
    loads = [pltpu.make_async_copy(a, b, load_sem.at[i]) for i, (a, b) in enumerate(zip(sources, held))]
    for copy in loads:
        copy.start()
    stores = []

    def store(src, dst):
        copy = pltpu.make_async_copy(src, dst, out_sem.at[len(stores)])
        copy.start()
        stores.append(copy)

    for i in range(4):
        store(gain.at[i : i + 1, :], outs[2 + i])
    for i, ref in enumerate((qkv_b, out_b, up_b, out_b)):
        store(ref, outs[7 + 2 * i])
    for i in range(4):
        loads[i].wait()
        rows = held[i].shape[0]
        step = max(16, rows // 4)
        for r in range(0, rows, step):
            part = slice(r, r + step)
            wide[i][part, :] = f32(held[i][part, :])
            store(wide[i].at[part, :], outs[6 + 2 * i].at[part, :])
    for copy in loads[4:]:
        copy.wait()
    hidden[...] = bf(f32(held[6][...]) + held[4][...] + proj_bias[...] + down_bias[...])
    norm[...] = bf(f32(held[7][...]) + held[5][...])
    store(hidden, outs[0])
    store(norm, outs[1])
    for copy in stores:
        copy.wait()


def finish(res, hidden_in, out_cotangent, proj_bias, down_bias):
    r = types.SimpleNamespace(**res)
    far = [r.grad2, r.grad0, r.grad3, r.grad1, r.home0, r.home1, hidden_in, out_cotangent]
    near = [r.gain_o, r.qkv_bias_o, r.up_bias_o, r.out_bias_o, proj_bias, down_bias]
    shape = jax.ShapeDtypeStruct
    D = r.gain_o.shape[1]
    qkv_b, up_b, out_b = [shape(v.shape, WIDE) for v in near[1:4]]
    big = [shape(a.shape, WIDE) for a in far[:4]]
    outs = [shape(hidden_in.shape, SMALL)] * 2 + [shape((1, D), WIDE)] * 4
    outs += [big[0], qkv_b, big[1], out_b, big[2], up_b, big[3], out_b]
    any_spec = pl.BlockSpec(memory_space=pl.ANY)
    vmem = pl.BlockSpec(memory_space=pltpu.VMEM)
    results = pl.pallas_call(
        last_kernel,
        out_shape=outs,
        in_specs=[any_spec] * len(far) + [vmem] * len(near),
        out_specs=[any_spec] * len(outs),
        scratch_shapes=[pltpu.VMEM(a.shape, a.dtype) for a in far]
        + [pltpu.VMEM(a.shape, WIDE) for a in far[:4]]
        + [pltpu.VMEM(hidden_in.shape, SMALL)] * 2
        + [pltpu.SemaphoreType.DMA((len(far),)), pltpu.SemaphoreType.DMA((32,))],
        compiler_params=pltpu.CompilerParams(vmem_limit_bytes=VMEM_BYTES),
    )(*far, *near)
    flat = {2, 3, 4, 5, 7, 9, 11, 13}
    return tuple(v.reshape(-1) if i in flat else v for i, v in enumerate(results))


def solution(mesh):
    matrix = P(("seq", "fsdp"), "tensor")
    vector = P("tensor")
    return jax.shard_map(
        per_device,
        mesh=mesh,
        in_specs=(
            matrix, matrix, P(), P(), P(), P(),
            matrix, vector, matrix, vector, matrix, vector, matrix, vector,
        ),
        out_specs=(
            matrix, matrix, P(), P(), P(), P(),
            matrix, vector, matrix, vector, matrix, vector, matrix, vector,
        ),
        check_vma=False,
    )
```

```python
import functools
import types

import jax
import jax.numpy as jnp
import numpy as np
from jax import lax
from jax.experimental import pallas as pl
from jax.experimental.pallas import tpu as pltpu
from jax.sharding import PartitionSpec as P

HEAD_DIM = 256
ROT = 64
LANES = 128
STRIP = 256
MESH = pl.DeviceIdType.MESH
VMEM_BYTES = 67_043_328
SMALL, WIDE = jnp.bfloat16, jnp.float32

norm_eps = 1e-05
rope_base = 10000.0

WQ, WP, WU1, WU2, WD1, WD2 = range(6)
P1, D1, D2, Q1, U1, U2 = range(6)


def bits_of(size):
    return [1 << b for b in range(size.bit_length() - 1)]


def bf(value):
    return value.astype(jnp.bfloat16)


def f32(value):
    return value.astype(jnp.float32)


def mm(left, right, left_dim, right_dim):
    return lax.dot_general(
        left, right, (((left_dim,), (right_dim,)), ((), ())), preferred_element_type=jnp.float32
    )


def rotary_tables(tok, blocks):
    half = ROT // 2
    frequency = rope_base ** (-np.arange(half, dtype=np.float64) * 2.0 / ROT)
    lanes = np.zeros(LANES)
    lanes[:half] = frequency
    lanes[half:ROT] = frequency
    inner = np.arange(tok, dtype=np.float64)[:, None] * lanes
    outer = np.arange(blocks, dtype=np.float64)[:, None] * tok * lanes
    pack = lambda a: np.stack([np.cos(a), np.sin(a)]).astype(np.float32)
    return (jnp.asarray(pack(inner)), jnp.asarray(pack(outer)))


def flip(rank, mask, size):
    out = jnp.int32(0)
    for b in range(size.bit_length() - 1):
        digit = lax.rem(lax.div(rank, jnp.int32(1 << b)), jnp.int32(2))
        out = out + ((1 - digit) if mask >> b & 1 else digit) * (1 << b)
    return out


def low_bit(j, size):
    return j & -j if j else size


def line_mask(j):
    mask = 0
    b = 0
    while j >> b:
        if j >> b & 1:
            mask ^= (2 << b) - 1
        b += 1
    return mask


def arrivals(size):
    return sorted(range(1, size), key=lambda j: (-low_bit(j, size), j))


def slot_of(j, bit, size):
    index = 0
    for jj in range(size):
        for bb in bits_of(size):
            if bb < low_bit(jj, size):
                if (jj, bb) == (j, bit):
                    return index
                index += 1
    raise ValueError


def at(index, size):
    return pl.ds(pl.multiple_of(index * size, size), size)


def remote(src, dst, send, recv, peer):
    return pltpu.make_async_remote_copy(
        src_ref=src, dst_ref=dst, send_sem=send, recv_sem=recv, device_id=peer, device_id_type=MESH
    )


def repeat(count, body):
    def step(i, carry):
        body(i)
        return carry

    lax.fori_loop(0, count, step, 0)


def turn(value, cos_part, sin_part):
    half = ROT // 2
    head = value[:, :LANES]
    lane = lax.broadcasted_iota(jnp.int32, head.shape, 1)
    other = jnp.where(
        lane < half, -pltpu.roll(head, LANES - half, 1), pltpu.roll(head, half, 1)
    )
    return jnp.concatenate([head * cos_part + other * sin_part, value[:, LANES:]], axis=1)


def make_core(S, T, F):
    c = types.SimpleNamespace(S=S, T=T, F=F)
    c.z, c.y, c.f = lax.axis_index("seq"), lax.axis_index("tensor"), lax.axis_index("fsdp")
    c.fbits, c.sbits = bits_of(F), bits_of(S)
    sends, busy = [], {}

    def start(copy, key=None):
        copy.start()
        sends.append(copy)
        if key is not None:
            busy.setdefault(key, []).append(copy)

    def free(key):
        done = busy.pop(key, [])
        for copy in done:
            copy.wait_send()
        sends[:] = [s for s in sends if not any(s is copy for copy in done)]

    def finish():
        for copy in sends:
            copy.wait_send()

    def greet():
        barrier = pltpu.get_barrier_semaphore()
        peers = [dict(seq=flip(c.z, k, S)) for k in range(1, S)]
        peers += [dict(tensor=flip(c.y, t, T)) for t in range(1, T)]
        peers += [dict(fsdp=flip(c.f, b, F)) for b in c.fbits]
        for peer in peers:
            pl.semaphore_signal(barrier, inc=1, device_id=peer, device_id_type=MESH)
        pl.semaphore_wait(barrier, len(peers))

    c.start, c.free, c.finish, c.greet = start, free, finish, greet
    return c


def gather_ops(c, e):
    S, T, F, z, y, f = c.S, c.T, c.F, c.z, c.y, c.f
    tok, width = e.hid_in.shape
    rows = e.wq_in.shape[0]
    half = e.wu.shape[1] // 2
    tokens = ((e.hid_in, e.hid), (e.cot_in, e.cot))
    weights = (
        (e.wq_in, e.wq, 0, e.wq.shape[1]),
        (e.wp_in, e.wp, 0, e.wp.shape[1]),
        (e.wu_in, e.wu, 0, half),
        (e.wu_in, e.wu, half, half),
        (e.wd_in, e.wd, 0, half),
        (e.wd_in, e.wd, half, half),
    )
    g = types.SimpleNamespace()

    def tok_sem(a, j, t):
        return (a * S + j) * T + t

    def tok_place(a, j, t):
        return tokens[a][1].at[at(flip(z, line_mask(j), S), tok), at(flip(y, t, T), width)]

    def tok_seq(a, j):
        src = tokens[a][0] if j == 0 else tok_place(a, j, 0)
        dst = tok_place(a, j, 0)
        for b in reversed(c.sbits):
            if b < low_bit(j, S):
                i = tok_sem(a, j + b, 0)
                peer = dict(seq=flip(z, line_mask(b), S))
                c.start(remote(src, dst, e.tok_send.at[i], e.tok_recv.at[i], peer))

    def tok_tensor(a, j):
        src = tokens[a][0] if j == 0 else tok_place(a, j, 0)
        dst = tok_place(a, j, 0)
        for t in range(1, T):
            i = tok_sem(a, j, t)
            peer = dict(tensor=flip(y, t, T))
            c.start(remote(src, dst, e.tok_send.at[i], e.tok_recv.at[i], peer))

    def tok_wait(a, j, t):
        i = tok_sem(a, j, t)
        spot = tok_place(a, j, t)
        peer = dict(tensor=flip(y, 1, T))
        remote(spot, spot, e.tok_send.at[i], e.tok_recv.at[i], peer).wait_recv()

    def tok_own(a):
        return pltpu.make_async_copy(tokens[a][0], tok_place(a, 0, 0), e.own_sem.at[a])

    def tok_direct(a, j):
        tok_wait(a, j, 0)
        tok_seq(a, j)
        tok_tensor(a, j)

    def tok_passed(a):
        for j in arrivals(S):
            if j not in c.sbits:
                tok_wait(a, j, 0)
                tok_seq(a, j)
                tok_tensor(a, j)

    def tok_rest(a):
        tok_own(a).wait()
        for j in range(S):
            for t in range(1, T):
                tok_wait(a, j, t)

    def row_sem(m, k, j):
        return (m * S + k) * F + j

    def row_place(m, k, j):
        _, dst, first, size = weights[m]
        return dst.at[at(flip(z, k, S) * F + flip(f, j, F), rows), first : first + size]

    def row_source(m, zd):
        src, dst, first, size = weights[m]
        return src.at[:, pl.ds(pl.multiple_of(zd * dst.shape[1] + first, LANES), size)]

    def row_seq(m, *peers):
        for k in peers or range(1, S):
            i = row_sem(m, k, 0)
            zd = flip(z, k, S)
            src = row_source(m, zd)
            dst = row_place(m, 0, 0)
            c.start(remote(src, dst, e.row_send.at[i], e.row_recv.at[i], dict(seq=zd)))

    def row_forward(m, k, j):
        dst = row_place(m, k, j)
        src = row_source(m, z) if k == 0 and j == 0 else dst
        for b in reversed(c.fbits):
            if b < low_bit(j, F):
                i = row_sem(m, k, j + b)
                peer = dict(fsdp=flip(f, b, F))
                c.start(remote(src, dst, e.row_send.at[i], e.row_recv.at[i], peer))

    def row_wait(m, k, j):
        i = row_sem(m, k, j)
        spot = row_place(m, k, j)
        peer = dict(seq=flip(z, 1, S))
        remote(spot, spot, e.row_send.at[i], e.row_recv.at[i], peer).wait_recv()

    def row_own(m):
        return pltpu.make_async_copy(row_source(m, z), row_place(m, 0, 0), e.own_sem.at[2 + m])

    def row_arrive(m, *peers):
        for k in peers or range(1, S):
            row_wait(m, k, 0)
            row_forward(m, k, 0)

    def row_relay(m):
        for j in arrivals(F):
            if low_bit(j, F) > 1:
                for k in range(S):
                    row_wait(m, k, j)
                    row_forward(m, k, j)

    def row_rest(m):
        row_own(m).wait()
        for j in arrivals(F):
            if low_bit(j, F) == 1:
                for k in range(S):
                    row_wait(m, k, j)

    def begin_own():
        for a in range(2):
            tok_own(a).start()
        for m in range(6):
            row_own(m).start()

    g.tok_seq, g.tok_tensor, g.tok_direct, g.tok_passed = tok_seq, tok_tensor, tok_direct, tok_passed
    g.tok_rest, g.row_seq, g.row_forward, g.row_arrive = tok_rest, row_seq, row_forward, row_arrive
    g.row_relay, g.row_rest, g.begin_own = row_relay, row_rest, begin_own
    return g


def attention_ops(c, e):
    S, T, F, z, y, f = c.S, c.T, c.F, c.z, c.y, c.f
    tok = e.hid_in.shape[0]
    ntok = e.hid.shape[0]
    scale = HEAD_DIM ** (-0.5)
    chunk = 32
    o = types.SimpleNamespace()

    def norm():
        def norm_chunk(i):
            part = at(i, chunk)
            x = f32(e.hid[part, :])
            mean = jnp.mean(x, axis=-1, keepdims=True)
            centered = x - mean
            inv_std = lax.rsqrt(jnp.mean(centered * centered, axis=-1, keepdims=True) + norm_eps)
            xhat = centered * inv_std
            e.attn_in[part, :] = bf(xhat * e.attn_gain[...] + e.attn_bias[...])
            e.mlp_in[part, :] = bf(xhat * e.mlp_gain[...] + e.mlp_bias[...])
            e.stat[0, part, :] = jnp.broadcast_to(mean, (chunk, LANES))
            e.stat[1, part, :] = jnp.broadcast_to(inv_std, (chunk, LANES))

        repeat(ntok // chunk, norm_chunk)

    def angles(zd):
        block = pl.ds(zd * F + f, 1)
        cos_in, sin_in = e.inner[0], e.inner[1]
        cos_out, sin_out = e.outer[0, block, :], e.outer[1, block, :]
        return (cos_in * cos_out - sin_in * sin_out, sin_in * cos_out + cos_in * sin_out)

    def qkv():
        bias = e.qkv_bias[:, at(z, 3 * HEAD_DIM)]
        for n in range(3):
            columns = slice(n * HEAD_DIM, (n + 1) * HEAD_DIM)
            part = mm(e.attn_in[...], e.wq[:, columns], 1, 0) + bias[:, columns]
            for zd in range(S):
                piece = part[zd * tok : (zd + 1) * tok]
                if n < 2:
                    piece = turn(piece, *angles(zd))
                if n == 0:
                    e.query[zd * tok : (zd + 1) * tok, :] = bf(piece)
                else:
                    spot = at(zd * F + f, tok)
                    e.pair[spot, (n - 1) * HEAD_DIM : n * HEAD_DIM] = bf(piece)

    def pair_place(zd, j):
        return e.pair.at[at(zd * F + flip(f, j, F), tok), :]

    def pair_forward(zd, j):
        spot = pair_place(zd, j)
        for b in reversed(c.fbits):
            if b < low_bit(j, F):
                i = zd * F + j + b
                peer = dict(fsdp=flip(f, b, F))
                c.start(remote(spot, spot, e.pair_send.at[i], e.pair_recv.at[i], peer), "pair")

    def pair_wait(zd, j):
        i = zd * F + j
        spot = pair_place(zd, j)
        peer = dict(fsdp=flip(f, 1, F))
        remote(spot, spot, e.pair_send.at[i], e.pair_recv.at[i], peer).wait_recv()

    def pair_own():
        for zd in range(S):
            pair_forward(zd, 0)

    def pair_relay():
        for j in arrivals(F):
            if low_bit(j, F) > 1:
                for zd in range(S):
                    pair_wait(zd, j)
                    pair_forward(zd, j)

    def pair_rest():
        for j in arrivals(F):
            if low_bit(j, F) == 1:
                for zd in range(S):
                    pair_wait(zd, j)

    n = F * tok

    def row_chunks(b, body):
        count = ntok - b * tok
        size = count // 2 if count > 2 * tok else count
        while size * n > 2 * tok * 512 and size > 32:
            size //= 2

        def step(i):
            first = pl.multiple_of(b * tok + i * size, 32)
            here = pl.ds(first, size)
            scores = mm(e.query[here, :], e.pair[b * n : (b + 1) * n, :HEAD_DIM], 1, 1) * scale
            row = i * size + lax.broadcasted_iota(jnp.int32, scores.shape, 0)
            column = lax.broadcasted_iota(jnp.int32, scores.shape, 1)
            body(here, scores, (column - row <= f * tok) | (row >= tok))

        repeat(count // size, step)

    def wide_rows(value):
        return jnp.broadcast_to(value, (value.shape[0], LANES))

    def forward():
        for b in range(S):
            values = e.pair.at[b * n : (b + 1) * n, HEAD_DIM:]

            def block(here, scores, allowed, b=b, values=values):
                top = jnp.max(jnp.where(allowed, scores, -1e30), axis=-1, keepdims=True)
                if b:
                    old = e.row_info[here, :1]
                    top = jnp.maximum(top, old)
                terms = jnp.where(allowed, jnp.exp(scores - top), 0.0)
                total = jnp.sum(terms, axis=-1, keepdims=True)
                mixed = mm(bf(terms), values[...], 1, 0)
                if b:
                    rescale = jnp.exp(old - top)
                    total = total + e.row_sum[here, :1] * rescale
                    mixed = mixed + e.acc[here, :] * rescale
                e.row_info[here, :] = wide_rows(top)
                e.row_sum[here, :] = wide_rows(total)
                e.acc[here, :] = mixed

            row_chunks(b, block)
            done = slice(b * tok, (b + 1) * tok)
            total = e.row_sum[done, :]
            e.attn[done, :] = bf(e.acc[done, :] / total[:, :1])
            e.row_info[done, :] = e.row_info[done, :] + jnp.log(total)

    def backward():
        e.attn_grad[...] = bf(mm(e.cot[...], e.wp[...], 1, 0))
        delta = jnp.sum(f32(e.attn_grad[...]) * f32(e.attn[...]), axis=-1, keepdims=True)
        e.row_sum[...] = wide_rows(delta)
        for b in range(S):
            keys_here = slice(b * n, (b + 1) * n)

            def block(here, scores, allowed, b=b, keys_here=keys_here):
                weights_here = jnp.where(allowed, jnp.exp(scores - e.row_info[here, :1]), 0.0)
                slopes = mm(e.attn_grad[here, :], e.pair[keys_here, HEAD_DIM:], 1, 1)
                inner_grad = bf(weights_here * (slopes - e.row_sum[here, :1]))
                e.probs[here, keys_here] = bf(weights_here)
                e.score_grad[here, keys_here] = inner_grad
                term = mm(inner_grad, e.pair[keys_here, :HEAD_DIM], 1, 0)
                e.acc[here, :] = e.acc[here, :] + term if b else term

            row_chunks(b, block)
            if b:
                blank = jnp.zeros((b * tok, n), jnp.bfloat16)
                e.probs[: b * tok, keys_here] = blank
                e.score_grad[: b * tok, keys_here] = blank
            done = slice(b * tok, (b + 1) * tok)
            cos_part, sin_part = angles(b)
            e.tg[done, :HEAD_DIM] = bf(turn(e.acc[done, :] * scale, cos_part, -sin_part))

    def part_sum(j):
        def lanes(ref):
            return jnp.concatenate(
                [ref[:, at(zd * F + flip(f, j, F), tok)] for zd in range(S)], axis=1
            )

        total = jnp.concatenate(
            [
                mm(lanes(e.score_grad), e.query[...], 0, 0) * scale,
                mm(lanes(e.probs), e.attn_grad[...], 0, 0),
            ],
            axis=1,
        )
        for b in c.fbits:
            if b < low_bit(j, F):
                i = slot_of(j, b, F)
                spot = e.part_in.at[i]
                peer = dict(fsdp=flip(f, b, F))
                remote(spot, spot, e.part_send.at[i], e.part_recv.at[i], peer).wait_recv()
                total = total + f32(e.part_in[i])
        return total

    def part_stage(bit):
        c.free("pair")
        for j in range(1, F):
            if low_bit(j, F) == bit:
                spot = e.pair.at[(j - 1) * ntok : j * ntok, :]
                e.pair[(j - 1) * ntok : j * ntok, :] = bf(part_sum(j))
                i = slot_of(j - bit, bit, F)
                peer = dict(fsdp=flip(f, bit, F))
                here = e.part_in.at[i]
                c.start(remote(spot, here, e.part_send.at[j - 1], e.part_recv.at[i], peer))

    def part_later():
        for bit in c.fbits[1:]:
            part_stage(bit)

    def part_home():
        total = part_sum(0)
        for zd in range(S):
            here = slice(zd * tok, (zd + 1) * tok)
            cos_part, sin_part = angles(zd)
            key_part = turn(total[here, :HEAD_DIM], cos_part, -sin_part)
            e.tg[here, HEAD_DIM : 2 * HEAD_DIM] = bf(key_part)
            e.tg[here, 2 * HEAD_DIM :] = bf(total[here, HEAD_DIM:])

    def up(first, size):
        cols = e.wu.shape[1]
        for n in range(first // STRIP, (first + size) // STRIP):
            strip = slice(n * STRIP, (n + 1) * STRIP)
            bias = e.up_bias[:, pl.ds(pl.multiple_of(z * cols + n * STRIP, STRIP), STRIP)]
            mid = mm(e.mlp_in[...], e.wu[:, strip], 1, 0) + bias
            cdf = 0.5 * (1.0 + lax.erf(mid * 0.7071067811865476))
            e.active[:, strip] = bf(mid * cdf)
            e.slope[:, strip] = cdf + mid * jnp.exp(-0.5 * mid * mid) * 0.3989422804014327

    o.norm, o.qkv, o.pair_own, o.pair_relay, o.pair_rest = norm, qkv, pair_own, pair_relay, pair_rest
    o.forward, o.backward, o.part_stage, o.part_later = forward, backward, part_stage, part_later
    o.part_home, o.up = part_home, up
    return o


def grad_units(ff):
    half = ff // 2
    return (
        (0, 0, HEAD_DIM),
        (1, 0, half),
        (1, half, half),
        (2, 0, 3 * HEAD_DIM),
        (3, 0, half),
        (3, half, half),
    )


def spread_ops(c, e, turned):
    S, T, F, z, y, f = c.S, c.T, c.F, c.z, c.y, c.f
    tok, width = e.homes[0].shape
    ntok, D = e.wide.shape
    ff = e.active.shape[1]
    rows = e.grads[0].shape[0]
    rights, lefts = (e.attn, e.active, e.tg, e.pre), (e.cot, e.cot, e.attn_in, e.mlp_in)
    units = grad_units(ff)
    n_u = len(units)
    p = types.SimpleNamespace()

    def block_sum(u, j):
        g, first, size = units[u]
        right, left = rights[g].at[:, first : first + size], lefts[g]
        fd = flip(f, j, F)
        if turned:
            block = jnp.concatenate([left[at(zd * F + fd, rows), :] for zd in range(S)], axis=0)
            total = mm(block, right[...], 1, 0)
        else:
            block = jnp.concatenate([left[:, at(zd * F + fd, rows)] for zd in range(S)], axis=1)
            total = mm(block, right[...], 0, 0)
        for bit in c.fbits:
            if bit < low_bit(j, F):
                s = slot_of(j, bit, F)
                i = u * (F - 1) + s
                spot = e.in_b[u].at[s]
                peer = dict(fsdp=flip(f, bit, F))
                remote(spot, spot, e.out_sem.at[i], e.in_sem.at[i], peer).wait_recv()
                total = total + f32(e.in_b[u][s])
        return total

    def fsdp_stage(u, bit):
        for j in range(1, F):
            if low_bit(j, F) == bit:
                key, spot = e.out_spot(u, j)
                c.free(key)
                spot[...] = bf(block_sum(u, j))
                there = slot_of(j - bit, bit, F)
                send = e.out_sem.at[u * (F - 1) + j - 1]
                recv = e.in_sem.at[u * (F - 1) + there]
                peer = dict(fsdp=flip(f, bit, F))
                c.start(remote(spot, e.in_b[u].at[there], send, recv, peer), key)

    def first(u):
        fsdp_stage(u, c.fbits[0])

    def later(u):
        for bit in c.fbits[1:]:
            fsdp_stage(u, bit)

    def grad_place(u, zd):
        g, first_col, size = units[u]
        start_col = zd * rights[g].shape[1] + first_col
        return e.grads[g].at[:, pl.ds(pl.multiple_of(start_col, LANES), size)]

    def own_grad(u):
        src = e.seq_b[u].at[at(z, rows), :]
        return pltpu.make_async_copy(src, grad_place(u, z), e.home_sem.at[u])

    def seq(u):
        e.seq_b[u][...] = bf(block_sum(u, 0))
        own_grad(u).start()

    def seq_send(u, *peers):
        for k in peers or range(1, S):
            peer = flip(z, k, S)
            src, dst = e.seq_b[u].at[at(peer, rows), :], grad_place(u, z)
            i = u * S + k
            c.start(remote(src, dst, e.seq_send.at[i], e.seq_recv.at[i], dict(seq=peer)))

    def seq_wait():
        for u in range(n_u):
            for k in range(1, S):
                peer = flip(z, k, S)
                spot = grad_place(u, peer)
                i = u * S + k
                remote(spot, spot, e.seq_send.at[i], e.seq_recv.at[i], dict(seq=peer)).wait_recv()
            own_grad(u).wait()

    def half_strips(s, t, term):
        for n in range(width // STRIP):
            there = pl.ds(pl.multiple_of(flip(y, t, T) * width + n * STRIP, STRIP), STRIP)
            here = slice(n * STRIP, (n + 1) * STRIP)
            value = term(there)
            if t:
                for zd in range(S):
                    e.y_out[(t - 1) * S + zd, :, here] = bf(value[zd * tok : (zd + 1) * tok])
            elif s == 0:
                e.own_half[:, here] = value
            else:
                e.wide[:, there] = value

    def y_index(s, t, j):
        return (s * max(T - 1, 1) + t - 1) * S + j

    def tensor_send(s):
        for j in [*sorted(range(1, S), key=lambda j: (low_bit(j, S), j)), 0]:
            zd = flip(z, line_mask(j), S)
            for t in range(1, T):
                i = y_index(s, t, j)
                peer = dict(tensor=flip(y, t, T))
                here = e.y_out.at[(t - 1) * S + zd]
                c.start(remote(here, e.y_in.at[i], e.y_send.at[i], e.y_recv.at[i], peer), "y")

    def token_own(s, zd):
        if s == 0:
            return e.own_half.at[at(zd, tok), :]
        return e.wide.at[at(zd, tok), at(y, width)]

    def token_part(s, j):
        total = token_own(s, flip(z, line_mask(j), S))[...]
        for t in range(1, T):
            i = y_index(s, t, j)
            spot = e.y_in.at[i]
            peer = dict(tensor=flip(y, t, T))
            remote(spot, spot, e.y_send.at[i], e.y_recv.at[i], peer).wait_recv()
            total = total + f32(e.y_in[i])
        for bit in c.sbits:
            if bit < low_bit(j, S):
                i = s * (S - 1) + slot_of(j, bit, S)
                spot = e.z_in.at[i]
                peer = dict(seq=flip(z, line_mask(bit), S))
                remote(spot, spot, e.z_send.at[i], e.z_recv.at[i], peer).wait_recv()
                total = total + f32(e.z_in[i])
        return total

    def token_send(s, j):
        bit = low_bit(j, S)
        i = s * (S - 1) + j - 1
        there = s * (S - 1) + slot_of(j - bit, bit, S)
        c.free(("z", j))
        e.z_out[j - 1] = bf(token_part(s, j))
        peer = dict(seq=flip(z, line_mask(bit), S))
        here = e.z_out.at[j - 1]
        copy = remote(here, e.z_in.at[there], e.z_send.at[i], e.z_recv.at[there], peer)
        c.start(copy, ("z", j))

    def token_sends(s):
        for j in sorted(range(1, S), key=lambda j: (low_bit(j, S), j)):
            token_send(s, j)

    def home_copy(s):
        return pltpu.make_async_copy(token_own(s, z), e.homes[s], e.home_sem.at[n_u + s])

    def token_home(s):
        total = token_part(s, 0)
        token_own(s, z)[...] = total
        home_copy(s).start()

    def home_wait():
        for s in range(2):
            home_copy(s).wait()

    n_f = len(c.fbits)
    vec = e.vec

    def vec_copy(b):
        peer = dict(fsdp=flip(f, c.fbits[b], F))
        return remote(vec.at[b], e.vec_in.at[b], e.v_send.at[b], e.v_recv.at[b], peer)

    def vec_start(b):
        c.start(vec_copy(b))

    def vec_sum(b):
        vec_copy(b).wait_recv()
        vec[b + 1] = vec[b] + e.vec_in[b]

    def vec_fsdp():
        for b in range(n_f - 1):
            vec_sum(b)
            vec_start(b + 1)

    def vec_seq_copy(k):
        peer = dict(seq=flip(z, k, S))
        i = n_f + k - 1
        return remote(vec.at[n_f], e.vec_seq.at[k - 1], e.v_send.at[i], e.v_recv.at[i], peer)

    def vec_seq_start():
        vec_sum(n_f - 1)
        for k in range(1, S):
            c.start(vec_seq_copy(k))

    def tree(parts):
        while len(parts) > 1:
            parts = [a + b for a, b in zip(parts[::2], parts[1::2])]
        return parts[0]

    def vec_seq_sum():
        parts = []
        for k in range(S):
            if k:
                vec_seq_copy(k).wait_recv()
            value = vec[n_f] if k == 0 else e.vec_seq[k - 1]
            zd = flip(z, k, S)
            e.qkv_bias_o[:, at(zd, 3 * HEAD_DIM)] = value[4:5, : 3 * HEAD_DIM]
            e.up_bias_o[:, at(zd, ff)] = value[5:6, :ff]
            parts.append(value)
        total = tree(parts)
        e.out_bias_o[...] = total[6:7, :width]
        e.vec_ten[0] = total[:4]
        for t in range(1, T):
            c.start(vec_ten_copy(t))

    def vec_ten_copy(t):
        peer = dict(tensor=flip(y, t, T))
        i = n_f + S - 1 + t - 1
        return remote(e.vec_ten.at[0], e.vec_ten.at[t], e.v_send.at[i], e.v_recv.at[i], peer)

    def vec_ten_sum():
        parts = [e.vec_ten[0]]
        for t in range(1, T):
            vec_ten_copy(t).wait_recv()
            parts.append(e.vec_ten[t])
        e.gain_o[...] = tree(parts)

    def branch():
        def term(column):
            return mm(e.active[...], e.wd[column, :], 1, 1) + mm(e.attn[...], e.wp[column, :], 1, 1)

        for t in range(1, T):
            half_strips(0, t, term)
        tensor_send(0)
        return lambda: half_strips(0, 0, term)

    def hidden_grad():
        vec[0] = jnp.zeros(vec.shape[1:], jnp.float32)
        for n in range(ff // STRIP):
            here = slice(n * STRIP, (n + 1) * STRIP)
            value = mm(e.cot[...], e.wd[:, here], 0 if turned else 1, 0) * e.slope[:, here]
            vec[0, 5:6, here] = jnp.sum(value, axis=0, keepdims=True)
            e.pre[:, here] = bf(value)

    def unit_rows(column):
        mean, inv_std = e.stat[0, :, :1], e.stat[1, :, :1]
        return ((f32(e.hid[:, column]) - mean) * inv_std, inv_std)

    def add_strip(here, value, gain, row):
        xhat, _ = unit_rows(here)
        scaled = value * xhat
        vec[0, row : row + 1, here] = jnp.sum(scaled, axis=0, keepdims=True)
        vec[0, row + 1 : row + 2, here] = jnp.sum(value, axis=0, keepdims=True)
        gain_here = gain[:, here]
        both, scaled = value * gain_here, scaled * gain_here
        lane_parts = range(0, STRIP, LANES)
        e.sums[0] += sum(both[:, i : i + LANES] for i in lane_parts)
        e.sums[1] += sum(scaled[:, i : i + LANES] for i in lane_parts)
        return both

    def mlp_strips():
        def strip(n):
            here = at(n, STRIP)
            e.wide[:, here] = add_strip(here, mm(e.pre[...], e.wu[here, :], 1, 1), e.mlp_gain, 2)

        e.sums[...] = jnp.zeros_like(e.sums)
        repeat(D // STRIP, strip)

    def norm_strips():
        def strip(n):
            here = at(n, STRIP)
            e.wide[:, here] += add_strip(here, mm(e.tg[...], e.wq[here, :], 1, 1), e.attn_gain, 0)

        repeat(D // STRIP, strip)
        for i in range(2):
            mean = jnp.sum(e.sums[i], axis=-1, keepdims=True) / D
            e.sums[i] = jnp.broadcast_to(mean, e.sums.shape[1:])

    def vec_begin():
        vec[0, 4:5, : 3 * HEAD_DIM] = jnp.sum(f32(e.tg[...]), axis=0, keepdims=True)
        vec[0, 6:7, :width] = jnp.sum(f32(e.own_cot()), axis=0, keepdims=True)
        vec_start(0)

    def input_strips():
        def term(column):
            xhat, inv_std = unit_rows(column)
            return inv_std * (e.wide[:, column] - e.sums[0, :, :1] - xhat * e.sums[1, :, :1])

        c.free("y")
        for t in range(1, T):
            half_strips(1, t, term)
        tensor_send(1)
        return lambda: half_strips(1, 0, term)

    p.first, p.later, p.seq, p.seq_send, p.seq_wait = first, later, seq, seq_send, seq_wait
    p.token_send, p.token_sends, p.token_home = token_send, token_sends, token_home
    p.home_wait, p.vec_fsdp = home_wait, vec_fsdp
    p.vec_seq_start, p.vec_seq_sum, p.vec_ten_sum = vec_seq_start, vec_seq_sum, vec_ten_sum
    p.branch, p.hidden_grad, p.mlp_strips = branch, hidden_grad, mlp_strips
    p.norm_strips, p.input_strips, p.vec_begin = norm_strips, input_strips, vec_begin
    return p


def gather_buffers(S, T, F, tok, width, rows, ff):
    ntok, D, keys = S * tok, T * width, S * F * tok
    kept = dict(
        hid=((ntok, D), SMALL),
        cot=((ntok, D), SMALL),
        attn_in=((ntok, D), SMALL),
        mlp_in=((ntok, D), SMALL),
        stat=((2, ntok, LANES), WIDE),
        wq=((D, 3 * HEAD_DIM), SMALL),
        wp=((D, HEAD_DIM), SMALL),
        wu=((D, ff), SMALL),
        wd=((D, ff), SMALL),
        attn=((ntok, HEAD_DIM), SMALL),
        active=((ntok, ff), SMALL),
        tg=((ntok, 3 * HEAD_DIM), SMALL),
    )
    passing = dict(
        query=((ntok, HEAD_DIM), SMALL),
        pair=((keys, 2 * HEAD_DIM), SMALL),
        attn_grad=((ntok, HEAD_DIM), SMALL),
        probs=((ntok, keys), SMALL),
        score_grad=((ntok, keys), SMALL),
        row_info=((ntok, LANES), WIDE),
        row_sum=((ntok, LANES), WIDE),
        acc=((ntok, HEAD_DIM), WIDE),
        part_in=((max(F - 1, 1), ntok, 2 * HEAD_DIM), SMALL),
    )
    sems = dict(
        own_sem=8,
        tok_send=2 * S * T,
        tok_recv=2 * S * T,
        row_send=6 * S * F,
        row_recv=6 * S * F,
        pair_send=S * F,
        pair_recv=S * F,
        part_send=max(F - 1, 1),
        part_recv=max(F - 1, 1),
    )
    return kept, passing, sems


def spread_buffers(S, T, F, tok, width, rows, ff):
    ntok, D = S * tok, T * width
    n_f, n_y, parts = len(bits_of(F)), max(T - 1, 1) * S, max(F - 1, 1)
    held = dict(
        pre=((ntok, ff), SMALL),
        wide=((ntok, D), WIDE),
        own_half=((ntok, width), WIDE),
        sums=((2, ntok, LANES), WIDE),
        vec=((n_f + 1, 8, D), WIDE),
        vec_in=((n_f, 8, D), WIDE),
        vec_seq=((max(S - 1, 1), 8, D), WIDE),
        vec_ten=((T, 4, D), WIDE),
        y_out=((n_y, tok, width), SMALL),
        y_in=((2 * n_y, tok, width), SMALL),
        z_out=((max(S - 1, 1), tok, width), SMALL),
        z_in=((2 * max(S - 1, 1), tok, width), SMALL),
    )
    for u, (_, _, size) in enumerate(grad_units(ff)):
        held[f"in_b{u}"] = ((parts, S * rows, size), SMALL)
        held[f"seq_b{u}"] = ((S * rows, size), SMALL)
    sems = dict(
        home_sem=8,
        out_sem=6 * parts,
        in_sem=6 * parts,
        seq_send=6 * S,
        seq_recv=6 * S,
        y_send=2 * n_y,
        y_recv=2 * n_y,
        z_send=2 * max(S - 1, 1),
        z_recv=2 * max(S - 1, 1),
        v_send=n_f + S + T,
        v_recv=n_f + S + T,
    )
    outs = {f"grad{g}": ((rows, S * n), SMALL) for g, n in enumerate((HEAD_DIM, ff, 3 * HEAD_DIM, ff))}
    outs |= {f"home{s}": ((tok, width), WIDE) for s in range(2)}
    vectors = dict(
        gain_o=((4, D), WIDE),
        qkv_bias_o=((1, 3 * width), WIDE),
        up_bias_o=((1, S * ff), WIDE),
        out_bias_o=((1, width), WIDE),
    )
    return held, sems, outs, vectors


def send_buffers(S, F, rows, ff, units):
    sizes = [size for _, _, size in grad_units(ff)]
    return {f"out_b{u}": ((max(F - 1, 1), S * rows, sizes[u]), SMALL) for u in units}


def gather_lists(e):
    e.in_b = [getattr(e, f"in_b{u}") for u in range(6)]
    e.seq_b = [getattr(e, f"seq_b{u}") for u in range(6)]
    e.grads = [getattr(e, f"grad{g}") for g in range(4)]
    e.homes = [e.home0, e.home1]


def launch(body, sizes, collective, far, near, outs, near_outs, scratch, sems, **lists):
    names = [*far, *near, *outs, *near_outs, *scratch, *sems]

    def kernel(*refs):
        body(types.SimpleNamespace(**dict(zip(names, refs)), **lists), *sizes)

    kernel.__name__ = body.__name__
    any_spec = pl.BlockSpec(memory_space=pl.ANY)
    vmem = pl.BlockSpec(memory_space=pltpu.VMEM)
    results = pl.pallas_call(
        kernel,
        out_shape=[jax.ShapeDtypeStruct(*o) for o in [*outs.values(), *near_outs.values()]],
        in_specs=[any_spec] * len(far) + [vmem] * len(near),
        out_specs=[any_spec] * len(outs) + [vmem] * len(near_outs),
        scratch_shapes=[pltpu.VMEM(*s) for s in scratch.values()]
        + [pltpu.SemaphoreType.DMA((n,)) for n in sems.values()],
        compiler_params=pltpu.CompilerParams(
            collective_id=collective, has_side_effects=True, vmem_limit_bytes=VMEM_BYTES
        ),
    )(*far.values(), *near.values())
    return dict(zip([*outs, *near_outs], results))


def whole_kernel(e, S, T, F):
    c = make_core(S, T, F)
    width = e.hid_in.shape[1]
    tok = e.hid_in.shape[0]
    ff = e.active.shape[1]
    half = ff // 2
    gather_lists(e)
    e.slope = e.wide.at[:, :ff]
    e.row_info, e.row_sum = e.sums.at[0], e.sums.at[1]
    e.acc = e.wide.at[:, ff : ff + HEAD_DIM]
    e.own_cot = lambda: e.cot[at(c.z, tok), at(c.y, width)]
    wide_q = 3 * HEAD_DIM
    lent = [e.probs.at[:, :wide_q], e.probs.at[:, wide_q : 2 * wide_q], e.score_grad.at[:, :wide_q]]

    def out_spot(u, j):
        if u == Q1:
            return (("out", u, j), lent[j - 1])
        shared = {U1: D1, U2: D2}.get(u, u)
        return (("out", shared, j), getattr(e, f"out_b{shared}").at[j - 1])

    e.out_spot = out_spot
    g, o, p = gather_ops(c, e), attention_ops(c, e), spread_ops(c, e, False)
    near, vectors = e.near_names, e.vector_names

    def near_copy(i):
        return pltpu.make_async_copy(getattr(e, near[i] + "_i"), getattr(e, near[i]), e.near_sem.at[i])

    def vec_copy(i):
        return pltpu.make_async_copy(getattr(e, vectors[i]), getattr(e, vectors[i] + "_h"), e.vec_sem.at[i])

    def begin():
        g.begin_own()
        for i in range(len(near)):
            near_copy(i).start()

    def norm():
        for i in range(len(near)):
            near_copy(i).wait()
        o.norm()

    def vec_home():
        p.vec_ten_sum()
        for i in range(len(vectors)):
            vec_copy(i).start()

    c.greet()
    g.row_seq(WU2, 1)
    g.row_forward(WU1, 0, 0)
    g.tok_tensor(1, 0)
    g.row_seq(WQ, 2)
    g.tok_seq(0, 0)
    begin()
    g.tok_tensor(0, 0)
    g.row_forward(WQ, 0, 0)
    g.row_seq(WQ, 1)
    g.row_seq(WQ, 3)
    g.row_seq(WD2, 1)
    g.row_forward(WD1, 0, 0)
    g.row_seq(WP, 3)
    g.row_arrive(WQ, 1)
    g.row_seq(WU2, 2)
    g.row_arrive(WQ, 2)
    g.row_arrive(WD2, 1)
    g.tok_direct(0, 2)
    g.row_forward(WP, 0, 0)
    g.row_arrive(WQ, 3)
    g.row_forward(WU2, 0, 0)
    g.row_seq(WU2, 3)
    g.row_arrive(WU2, 2)
    g.tok_direct(0, 1)
    g.row_seq(WP, 2)
    g.row_relay(WQ)
    g.row_seq(WU1, 1)
    g.row_seq(WU1, 3)
    g.row_seq(WP, 1)
    g.tok_passed(0)
    g.row_arrive(WP, 2)
    g.row_arrive(WU2, 3)
    g.row_rest(WQ)
    g.row_arrive(WU2, 1)
    g.row_forward(WD2, 0, 0)
    g.tok_seq(1, 0)
    g.row_arrive(WU1, 1)
    g.tok_rest(0)
    norm()
    g.row_seq(WU1, 2)
    o.qkv()
    o.pair_own()
    g.row_arrive(WP, 3)
    g.tok_direct(1, 1)
    g.row_relay(WU2)
    g.tok_direct(1, 2)
    g.row_rest(WU2)
    g.row_seq(WD2, 2)
    o.pair_relay()
    g.row_seq(WD1, 3)
    g.row_arrive(WU1, 3)
    g.row_arrive(WU1, 2)
    o.up(half, half)
    g.row_seq(WD1, 1)
    o.pair_rest()
    o.forward()
    g.row_arrive(WP, 1)
    g.row_arrive(WD2, 2)
    g.row_seq(WD1, 2)
    g.row_relay(WU1)
    g.tok_passed(1)
    g.row_arrive(WD1, 3)
    g.row_rest(WU1)
    g.row_arrive(WD1, 1)
    o.up(0, half)
    g.row_relay(WP)
    g.row_seq(WD2, 3)
    g.tok_rest(1)
    p.first(D1)
    g.row_arrive(WD1, 2)
    g.row_rest(WP)
    p.first(D2)
    g.row_arrive(WD2, 3)
    p.later(D1)
    g.row_relay(WD1)
    g.row_rest(WD1)
    g.row_relay(WD2)
    g.row_rest(WD2)
    p.later(D2)
    own_strips = p.branch()
    o.backward()
    p.seq(D1)
    p.seq_send(D1, 2)
    o.part_stage(c.fbits[0])
    p.seq_send(D1, 3)
    p.seq_send(D1, 1)
    p.first(P1)
    p.hidden_grad()
    p.mlp_strips()
    p.later(P1)
    own_strips()
    p.token_send(0, 3)
    o.part_later()
    p.seq(D2)
    p.seq_send(D2, 3)
    p.first(U1)
    p.seq(P1)
    p.seq_send(D2, 2)
    p.seq_send(D2, 1)
    p.first(U2)
    p.later(U2)
    p.seq_send(P1, 2)
    p.token_send(0, 2)
    p.token_send(0, 1)
    o.part_home()
    p.norm_strips()
    p.vec_begin()
    own_terms = p.input_strips()
    p.vec_fsdp()
    p.seq_send(P1, 3)
    p.seq(U2)
    p.seq_send(U2, 2)
    p.vec_seq_start()
    p.later(U1)
    p.seq_send(U2, 1)
    own_terms()
    p.first(Q1)
    p.token_send(1, 3)
    p.seq_send(U2, 3)
    p.vec_seq_sum()
    p.token_home(0)
    p.later(Q1)
    p.seq(U1)
    p.seq_send(U1, 3)
    p.token_send(1, 2)
    p.token_send(1, 1)
    p.seq(Q1)
    vec_home()
    p.seq_send(Q1, 2)
    p.seq_send(U1, 1)
    p.token_home(1)
    p.seq_send(Q1, 1)
    p.seq_send(P1, 1)
    p.seq_send(Q1, 3)
    p.seq_send(U1, 2)
    p.seq_wait()
    p.home_wait()
    for i in range(len(vectors)):
        vec_copy(i).wait()
    c.finish()


def first_kernel(e, S, T, F):
    c = make_core(S, T, F)
    half = e.active.shape[1] // 2
    g, o = gather_ops(c, e), attention_ops(c, e)
    names = e.kept_names

    def out_copy(name):
        i = names.index(name)
        return pltpu.make_async_copy(getattr(e, name), getattr(e, name + "_o"), e.put_sem.at[i])

    c.greet()
    g.tok_seq(0, 0)
    g.tok_tensor(0, 0)
    for m in range(6):
        g.row_forward(m, 0, 0)
    g.begin_own()
    for j in c.sbits:
        g.tok_direct(0, j)
    g.row_seq(WQ)
    g.tok_passed(0)
    g.row_seq(WU1)
    g.tok_tensor(1, 0)
    g.tok_rest(0)
    o.norm()
    g.row_arrive(WQ)
    g.tok_seq(1, 0)
    g.row_relay(WQ)
    g.row_rest(WQ)
    o.qkv()
    o.pair_own()
    g.row_arrive(WU1)
    for m in (WP, WU2, WD1, WD2):
        g.row_seq(m)
    for j in c.sbits:
        g.tok_direct(1, j)
    g.row_relay(WU1)
    o.pair_relay()
    g.tok_passed(1)
    g.row_rest(WU1)
    o.up(0, half)
    g.row_arrive(WP)
    o.pair_rest()
    o.forward()
    g.row_arrive(WU2)
    g.tok_rest(1)
    g.row_relay(WP)
    g.row_rest(WP)
    o.backward()
    o.part_stage(c.fbits[0])
    g.row_relay(WU2)
    g.row_rest(WU2)
    o.up(half, half)
    o.part_later()
    g.row_arrive(WD1)
    g.row_arrive(WD2)
    o.part_home()
    for m in (WD1, WD2):
        g.row_relay(m)
        g.row_rest(m)
    for name in names:
        out_copy(name).start()
    for name in names:
        out_copy(name).wait()
    c.finish()


def second_kernel(e, S, T, F, turned):
    c = make_core(S, T, F)
    gather_lists(e)
    ff = e.active.shape[1]
    e.slope = e.wide.at[:, :ff]
    e.own_cot = lambda: e.own_cot_in[...]
    e.out_spot = lambda u, j: (("out", u, j), getattr(e, f"out_b{u}").at[j - 1])
    e.wd = e.wu = e.wud
    p = spread_ops(c, e, turned)
    names = e.kept_names

    def load(name):
        i = names.index(name)
        return pltpu.make_async_copy(getattr(e, name + "_i"), getattr(e, name), e.load_sem.at[i])

    for name in names:
        if name != "wu":
            load(name).start()
    c.greet()
    for name in names:
        if name != "wu":
            load(name).wait()
    p.first(P1)
    p.first(D1)
    p.first(D2)
    own_strips = p.branch()
    p.later(P1)
    own_strips()
    p.later(D1)
    p.hidden_grad()
    load("wu").start()
    p.seq(P1)
    p.seq_send(P1)
    p.later(D2)
    p.token_sends(0)
    p.first(Q1)
    p.first(U1)
    p.first(U2)
    load("wu").wait()
    p.mlp_strips()
    p.norm_strips()
    p.vec_begin()
    p.seq(D1)
    p.seq_send(D1)
    p.later(Q1)
    own_terms = p.input_strips()
    own_terms()
    p.token_home(0)
    p.seq(D2)
    p.seq_send(D2)
    p.later(U1)
    p.vec_fsdp()
    p.seq(Q1)
    p.seq_send(Q1)
    p.later(U2)
    p.vec_seq_start()
    p.token_sends(1)
    p.seq(U1)
    p.seq_send(U1)
    p.seq(U2)
    p.seq_send(U2)
    p.vec_seq_sum()
    p.vec_ten_sum()
    p.token_home(1)
    p.seq_wait()
    p.home_wait()
    c.finish()


def per_device(
    hidden_in,
    out_cotangent,
    attn_norm_gain,
    attn_norm_bias,
    mlp_norm_gain,
    mlp_norm_bias,
    qkv_weight,
    qkv_bias,
    proj_weight,
    proj_bias,
    up_weight,
    up_bias,
    down_weight,
    down_bias,
):
    S, T, F = [lax.axis_size(a) for a in ("seq", "tensor", "fsdp")]
    tok, width = hidden_in.shape
    rows, ff = qkv_weight.shape[0], up_weight.shape[1] // S
    if width != S * HEAD_DIM or S * F * rows != T * width:
        raise ValueError
    shape = (S, T, F, tok, width, rows, ff)
    inner, outer = rotary_tables(tok, S * F)
    far = dict(
        hid_in=hidden_in,
        cot_in=out_cotangent,
        wq_in=qkv_weight,
        wp_in=proj_weight,
        wu_in=up_weight,
        wd_in=down_weight,
    )
    row = lambda v: v.reshape(1, -1)
    gains = dict(attn_gain=row(attn_norm_gain), mlp_gain=row(mlp_norm_gain))
    near = gains | dict(
        attn_bias=row(attn_norm_bias),
        mlp_bias=row(mlp_norm_bias),
        qkv_bias=row(qkv_bias),
        up_bias=row(up_bias),
        inner=inner,
        outer=outer,
    )
    kept, passing, gather_sems = gather_buffers(*shape)
    held, spread_sems, outs, vectors = spread_buffers(*shape)
    if rows % LANES == 0 and (S, T, F) == (4, 2, 4):
        scratch = kept | passing | held | send_buffers(S, F, rows, ff, (P1, D1, D2)) | vectors
        scratch |= {k: (v.shape, v.dtype) for k, v in near.items()}
        del scratch["row_info"], scratch["row_sum"], scratch["acc"]
        sems = gather_sems | spread_sems | dict(near_sem=len(near), vec_sem=len(vectors))
        far |= {k + "_i": v for k, v in near.items()}
        outs |= {k + "_h": v for k, v in vectors.items()}
        lists = dict(near_names=list(near), vector_names=list(vectors))
        res = launch(whole_kernel, (S, T, F), 0, far, {}, outs, {}, scratch, sems, **lists)
        res |= {k: res[k + "_h"] for k in vectors}
    else:
        slope = dict(slope=((S * tok, ff), WIDE))
        saved = {k + "_o": v for k, v in (kept | slope).items()}
        sems = gather_sems | dict(put_sem=len(saved))
        scratch = kept | slope | passing
        lists = dict(kept_names=[*kept, *slope])
        mid = launch(first_kernel, (S, T, F), 0, far, near, saved, {}, scratch, sems, **lists)
        turned = rows % LANES != 0
        if turned:
            for k in ("cot_o", "attn_in_o", "mlp_in_o"):
                mid[k] = mid[k].T
        ins = {k[:-2] + "_i": v for k, v in mid.items()}
        scratch = {k: (ins[k + "_i"].shape, t) for k, (_, t) in kept.items() if k not in ("wu", "wd")}
        scratch |= dict(wud=kept["wu"]) | held | send_buffers(S, F, rows, ff, range(6))
        near = gains | dict(own_cot_in=out_cotangent)
        sems = spread_sems | dict(load_sem=len(ins))
        res = launch(
            second_kernel, (S, T, F, turned), 1, ins, near, outs, vectors, scratch, sems, **lists
        )
    return finish(res, hidden_in, out_cotangent, row(proj_bias), row(down_bias))


def last_kernel(*refs):
    sources, (gain, qkv_b, up_b, out_b, proj_bias, down_bias), refs = refs[:8], refs[8:14], refs[14:]
    outs, refs = refs[:14], refs[14:]
    held, wide, (hidden, norm, load_sem, out_sem) = refs[:8], refs[8:12], refs[12:]
    loads = []

    def load(src, dst):
        loads.append(pltpu.make_async_copy(src, dst, load_sem.at[len(loads)]))
        loads[-1].start()

    rows = held[0].shape[0]
    step = max(16, rows // 4)
    parts = [slice(r, r + step) for r in range(0, rows, step)]
    for i in range(4):
        for part in parts:
            load(sources[i].at[part, :], held[i].at[part, :])
    for i in range(4, 8):
        load(sources[i], held[i])
    stores = []

    def store(src, dst):
        copy = pltpu.make_async_copy(src, dst, out_sem.at[len(stores)])
        copy.start()
        stores.append(copy)

    for i in range(4):
        store(gain.at[i : i + 1, :], outs[2 + i])
    for i, ref in enumerate((qkv_b, out_b, up_b, out_b)):
        store(ref, outs[7 + 2 * i])
    for i in range(4):
        for r, part in enumerate(parts):
            loads[i * len(parts) + r].wait()
            wide[i][part, :] = f32(held[i][part, :])
            store(wide[i].at[part, :], outs[6 + 2 * i].at[part, :])
    for copy in loads[-4:]:
        copy.wait()
    hidden[...] = bf(f32(held[6][...]) + held[4][...] + proj_bias[...] + down_bias[...])
    norm[...] = bf(f32(held[7][...]) + held[5][...])
    store(hidden, outs[0])
    store(norm, outs[1])
    for copy in stores:
        copy.wait()


def finish(res, hidden_in, out_cotangent, proj_bias, down_bias):
    r = types.SimpleNamespace(**res)
    far = [r.grad2, r.grad0, r.grad3, r.grad1, r.home0, r.home1, hidden_in, out_cotangent]
    near = [r.gain_o, r.qkv_bias_o, r.up_bias_o, r.out_bias_o, proj_bias, down_bias]
    shape = jax.ShapeDtypeStruct
    D = r.gain_o.shape[1]
    qkv_b, up_b, out_b = [shape(v.shape, WIDE) for v in near[1:4]]
    big = [shape(a.shape, WIDE) for a in far[:4]]
    outs = [shape(hidden_in.shape, SMALL)] * 2 + [shape((1, D), WIDE)] * 4
    outs += [big[0], qkv_b, big[1], out_b, big[2], up_b, big[3], out_b]
    any_spec = pl.BlockSpec(memory_space=pl.ANY)
    vmem = pl.BlockSpec(memory_space=pltpu.VMEM)
    results = pl.pallas_call(
        last_kernel,
        out_shape=outs,
        in_specs=[any_spec] * len(far) + [vmem] * len(near),
        out_specs=[any_spec] * len(outs),
        scratch_shapes=[pltpu.VMEM(a.shape, a.dtype) for a in far]
        + [pltpu.VMEM(a.shape, WIDE) for a in far[:4]]
        + [pltpu.VMEM(hidden_in.shape, SMALL)] * 2
        + [pltpu.SemaphoreType.DMA((20,)), pltpu.SemaphoreType.DMA((32,))],
        compiler_params=pltpu.CompilerParams(vmem_limit_bytes=VMEM_BYTES),
    )(*far, *near)
    flat = {2, 3, 4, 5, 7, 9, 11, 13}
    return tuple(v.reshape(-1) if i in flat else v for i, v in enumerate(results))


def solution(mesh):
    matrix = P(("seq", "fsdp"), "tensor")
    vector = P("tensor")
    return jax.shard_map(
        per_device,
        mesh=mesh,
        in_specs=(
            matrix, matrix, P(), P(), P(), P(),
            matrix, vector, matrix, vector, matrix, vector, matrix, vector,
        ),
        out_specs=(
            matrix, matrix, P(), P(), P(), P(),
            matrix, vector, matrix, vector, matrix, vector, matrix, vector,
        ),
        check_vma=False,
    )
```
